256 devices in a mesh: gx: 16 (over x_hi, y, core), gy: 16 (over x_lo, z).
Axes of the slice: x: 4 (x_hi: 2, x_lo: 2; x = x_hi * 2 + x_lo), y: 4, z: 8, core: 2. Of those that a mesh axis runs over, the one named last changes fastest.
Arguments:
- u_old: float32 [3, 512, 512, 256], P(None, 'gx', 'gy'), may hold values from -0.6 to 0.6
- density: float32 [512, 512, 256], P('gx', 'gy'), may hold values from 0.5 to 2
- offsets: float32 [3, 4096, 128], P(None, ('gx', 'gy')), may hold values from 0 to 1
- forces: float32 [3, 4096, 128], P(None, ('gx', 'gy')), may hold values from -60 to 60
- base_x: int32 [4096, 128], P(('gx', 'gy')), may hold values from 0 to 31
- base_y: int32 [4096, 128], P(('gx', 'gy')), may hold values from 0 to 31
- base_z: int32 [4096, 128], P(('gx', 'gy')), may hold values from 0 to 255
- tile_count: int32 [256], P(('gx', 'gy')), may hold values from 1 to 16, as said below
Outputs:
- u_new: float32 [3, 512, 512, 256], P(None, 'gx', 'gy')
- marker_velocity: float32 [3, 4096, 128], P(None, ('gx', 'gy'))
The draws below stay inside these ranges and needn't reach their ends.
Inputs may be any that keep to these rules, and one draw needn't show every extreme that they name: `tile_count`: every draw has a device with exactly 16 live tiles; loads are skewed, with a mean near a quarter of that.
All inputs are finite; a program needn't handle non-finite values.
Results may differ from the reference program's by a relative error of at most 0.000075.
Values sent between devices are 32-bit elements; how exact they have to be, the bound alone decides.
No kernel may reach another device: no remote copies, remote signals or barrier semaphores. Data moves between devices by JAX's collectives and lax.ppermute only.
A program may use at most 64 MiB of HBM per device.

```python
import math
import jax
import jax.numpy as jnp

CX = 32
CY = 32
NZ = 256
TILE = 128
MAXT = 16
NX = 512
NY = 512
TILES = 4096
N_GY = 16
DEVICES = 256


def draw_tile_count(key, part):
    first, second, third = jax.random.split(jax.random.fold_in(key, 17), 3)
    upper = jax.random.randint(first, (DEVICES,), 0, MAXT)
    lower = jax.random.randint(second, (DEVICES,), 0, MAXT)
    counts = 1 + upper * lower // MAXT
    busiest = jax.random.randint(third, (), 0, DEVICES)
    return jnp.where(jnp.arange(DEVICES) == busiest, MAXT, counts).astype(jnp.int32)


def plant(drawn, key, least, top_value):
    index_at = [jax.random.randint(jax.random.fold_in(key, axis), (), 0, length) for axis, length in enumerate(drawn.shape)]
    widest = drawn.shape.index(max(drawn.shape))
    next_to = index_at[:widest] + [(index_at[widest] + 1) % drawn.shape[widest]] + index_at[widest + 1:]
    return drawn.at[tuple(index_at)].set(least).at[tuple(next_to)].set(top_value)


def block_levels(stream_key, dims, shards, least, largest):
    level, own = 1.0, jax.random.fold_in(stream_key, 6)
    for dim, shards_of in shards:
        steps = jnp.exp(jax.random.uniform(jax.random.fold_in(own, dim), (shards_of,), jnp.float32, least / len(shards), largest / len(shards)))
        level = level * jnp.repeat(steps, dims[dim] // shards_of).reshape([-1 if axis == dim else 1 for axis in range(len(dims))])
    return level


def noise(own_key, dims, scale, most, cuts=(), kind=jnp.bfloat16):
    drawn = jax.random.normal(own_key, dims, jnp.float32) * scale
    if len(cuts) > 0:
        drawn = block_levels(own_key, dims, cuts, -0.22, 0.18) * drawn
    return jnp.clip(drawn, min=-most, max=most).astype(kind)


def setup_inputs(seed: int = 0) -> dict:
    key_list = jax.random.split(jax.random.key(seed), 9)
    return {
        "u_old": noise(key_list[0], (3, NX, NY, NZ), 0.1, 0.6, ((1, 16), (2, 16)), jnp.float32),
        "density": jnp.clip(jnp.exp(math.log(2.0) - 1.3862944 * jax.random.uniform(key_list[1], (NX, NY, NZ), jnp.float32) ** block_levels(key_list[1], (NX, NY, NZ), ((0, 16), (1, 16)), -0.2, 0.2)), 0.5, 2.0),
        "offsets": jnp.clip(1.0 * jax.random.uniform(key_list[2], (3, TILES, TILE), jnp.float32) ** block_levels(key_list[2], (3, TILES, TILE), ((1, 256),), -0.2, 0.2), 0.0, 1.0),
        "forces": noise(key_list[3], (3, TILES, TILE), 10.0, 60.0, ((1, 256),), jnp.float32),
        "base_x": plant(jax.random.randint(key_list[4], (TILES, TILE), 0, CX), jax.random.fold_in(key_list[4], 1), 0, CX - 1).astype(jnp.int32),
        "base_y": plant(jax.random.randint(key_list[5], (TILES, TILE), 0, CY), jax.random.fold_in(key_list[5], 1), 0, CY - 1).astype(jnp.int32),
        "base_z": plant(jax.random.randint(key_list[6], (TILES, TILE), 0, NZ), jax.random.fold_in(key_list[6], 1), 0, NZ - 1).astype(jnp.int32),
        "tile_count": draw_tile_count(jax.random.fold_in(key_list[8], 71), 0),
    }


def stencil(frac):
    root = jnp.sqrt(1.0 + 4.0 * frac - 4.0 * frac * frac)
    return [(3.0 - 2.0 * frac - root) / 8.0, (3.0 - 2.0 * frac + root) / 8.0, (1.0 + 2.0 * frac + root) / 8.0, (1.0 + 2.0 * frac - root) / 8.0]

def reference(u_old, density, offsets, forces, base_x, base_y, base_z, tile_count):
    time_step = 0.5
    tiles, width = base_x.shape
    nx, ny, nz = density.shape
    slot = jnp.arange(tiles).astype(jnp.int32)
    device = slot // MAXT
    anchor_x = (device // N_GY * CX)[:, None]
    anchor_y = (device % N_GY * CY)[:, None]
    live = (slot % MAXT < tile_count[device]).astype(jnp.float32)[:, None] * jnp.ones((tiles, width), jnp.float32)
    weight_x = stencil(offsets[0])
    weight_y = stencil(offsets[1])
    weight_z = stencil(offsets[2])
    load = forces * live[None]
    grid = jnp.zeros((3, nx * ny * nz), jnp.float32)
    places = []
    for shift_a in range(4):
        cell_x = (anchor_x + base_x + shift_a - 1) % nx
        for shift_b in range(4):
            cell_y = (anchor_y + base_y + shift_b - 1) % ny
            for shift_c in range(4):
                cell_z = (base_z + shift_c - 1) % nz
                index = ((cell_x * ny + cell_y) * nz + cell_z).astype(jnp.int32)
                weight = weight_x[shift_a] * weight_y[shift_b] * weight_z[shift_c]
                grid = grid.at[:, index.reshape(-1)].add((load * weight[None]).reshape(3, -1))
                places.append((index, weight))
    force_grid = grid.reshape(3, nx, ny, nz)
    u_new = u_old + time_step * force_grid / density[None]
    table = u_new.reshape(3, -1)
    velocity = jnp.zeros((3, tiles, width), jnp.float32)
    for index, weight in places:
        velocity = velocity + table[:, index.reshape(-1)].reshape(3, tiles, width) * weight[None]
    return (u_new, velocity * live[None])
```

```python
import functools

import jax
import jax.numpy as jnp
from jax import lax
from jax.experimental import pallas as pl
from jax.experimental.pallas import tpu as pltpu
from jax.sharding import PartitionSpec as P


CX, CY, ROWS, PLANES = 32, 32, 40, 36
GROUPS = 12
F32, BF16 = jnp.float32, jnp.bfloat16
DIRS = [(1, 0), (-1, 0), (0, 1), (0, -1), (1, 1), (1, -1), (-1, 1), (-1, -1)]
VMEM = pl.BlockSpec(memory_space=pltpu.VMEM)
SMEM = pl.BlockSpec(memory_space=pltpu.SMEM)
ANY = pl.BlockSpec(memory_space=pl.ANY)


def stencil(frac):
    root = jnp.sqrt(1.0 + 4.0 * frac - 4.0 * frac * frac)
    return [
        (3.0 - 2.0 * frac - root) / 8.0,
        (3.0 - 2.0 * frac + root) / 8.0,
        (1.0 + 2.0 * frac + root) / 8.0,
        (1.0 + 2.0 * frac - root) / 8.0,
    ]


def spread_four(rows, targets, weights):
    row = lax.broadcasted_iota(jnp.int32, (rows, targets[0].shape[1]), 0)
    total = jnp.zeros(row.shape, F32)
    for target, weight in zip(targets, weights):
        total = jnp.where(row == target, weight, total)
    return total


def split(value):
    high = value.astype(BF16)
    return high, (value - high.astype(F32)).astype(BF16)


def marker_tables(tile, off_ref, bx_ref, by_ref, bz_ref, wx_ref):
    one = pl.ds(tile, 1)
    base_x, base_y, base_z = bx_ref[one, :], by_ref[one, :], bz_ref[one, :]
    wx_ref[...] = spread_four(PLANES + 4, [base_x + a for a in range(4)], stencil(off_ref[0, one, :]))
    targets = [base_y + b - 1 for b in range(4)]
    targets[0] = jnp.where(targets[0] < 0, ROWS - 1, targets[0])
    wy = spread_four(ROWS, targets, stencil(off_ref[1, one, :]))
    wz = spread_four(256, [(base_z + c - 1) & 255 for c in range(4)], stencil(off_ref[2, one, :]))
    return wy, wz


def pack_kernel(u_ref, rho_ref, xn_ref, xp_ref, yn_ref, yp_ref, c0, c1, c2, c3, slab, sems):
    copies = []
    for c in range(4):
        for h in range(2):
            j, lanes = 2 * c + h, pl.ds(128 * h, 128)
            for n, (dst, x0, planes, y0, rows) in enumerate(
                [
                    (xp_ref, 0, 2, 0, CY),
                    (xn_ref, CX - 1, 1, 0, CY),
                    (slab.at[0], 0, CX, 0, 8),
                    (slab.at[1], 0, CX, CY - 8, 8),
                ]
            ):
                xs, ys = pl.ds(x0, planes), pl.ds(y0, rows)
                src = u_ref.at[c, xs, ys, lanes] if c < 3 else rho_ref.at[xs, ys, lanes]
                copies.append(pltpu.make_async_copy(src, dst.at[j], sems.at[n, j]))
    for copy in copies:
        copy.start()
    for copy in copies:
        copy.wait()
    for j in range(8):
        yp_ref[j, 0] = slab[0, j, :, 0, :]
        yp_ref[j, 1] = slab[0, j, :, 1, :]
        yn_ref[j, 0] = slab[1, j, :, 7, :]
        c0[j, 0:1, :] = xn_ref[j, 0, CY - 1 : CY, :]
        c1[j, 0:2, :] = xn_ref[j, 0, 0:2, :]
        c2[j, 0:1, :] = xp_ref[j, 0, CY - 1 : CY, :]
        c2[j, 1:2, :] = xp_ref[j, 1, CY - 1 : CY, :]
        c3[j, 0:2, :] = xp_ref[j, 0, 0:2, :]
        c3[j, 2:4, :] = xp_ref[j, 1, 0:2, :]


def pack(u_old, density):
    shapes = [(8, 1, CY, 128), (8, 2, CY, 128), (8, 1, CX, 128), (8, 2, CX, 128)] + [(8, 8, 128)] * 4
    return pl.pallas_call(
        pack_kernel,
        out_shape=[jax.ShapeDtypeStruct(s, F32) for s in shapes],
        in_specs=[ANY, ANY],
        out_specs=[VMEM] * 8,
        scratch_shapes=[pltpu.VMEM((2, 8, CX, 8, 128), F32), pltpu.SemaphoreType.DMA((4, 8))],
        name="pack",
    )(u_old, density)


def exchange(pieces):
    nx, ny = lax.axis_size("gx"), lax.axis_size("gy")
    out = []
    for piece, (dx, dy) in zip(pieces, DIRS):
        pairs = [
            (x * ny + y, (x + dx) % nx * ny + (y + dy) % ny) for x in range(nx) for y in range(ny)
        ]
        out.append(lax.ppermute(piece, ("gx", "gy"), pairs))
    return out


def spread_kernel(
    count_ref, off_ref, force_ref, bx_ref, by_ref, bz_ref,
    grid_ref, xn_ref, xp_ref, yn_ref, yp_ref, c0, c1, c2, c3,
    a_ref, b_ref, wx_ref,
):
    count = count_ref[0]
    for j in range(6):
        grid_ref[j] = jnp.zeros((PLANES, ROWS, 128), F32)

    def pair(p, carry):
        for half in range(2):
            tile = 2 * p + half
            wy, wz = marker_tables(tile, off_ref, bx_ref, by_ref, bz_ref, wx_ref)
            live = (tile < count).astype(F32)
            cols = [slice(256 * part + 128 * half, 256 * part + 128 * half + 128) for part in range(3)]
            for c in range(3):
                high, low = split(wz * (force_ref[c, pl.ds(tile, 1), :] * live))
                rows = slice(256 * c, 256 * c + 256)
                b_ref[rows, cols[0]] = high
                b_ref[rows, cols[1]] = high
                b_ref[rows, cols[2]] = low
            for e in range(0, PLANES, 2):
                both = jnp.concatenate([wx_ref[e : e + 1, :] * wy, wx_ref[e + 1 : e + 2, :] * wy], axis=0)
                high, low = split(both)
                rows = slice(ROWS * e, ROWS * e + 2 * ROWS)
                a_ref[rows, cols[0]] = high
                a_ref[rows, cols[1]] = low
                a_ref[rows, cols[2]] = high
        step = 18
        for e in range(0, PLANES, step):
            part = lax.dot_general(
                a_ref[ROWS * e : ROWS * (e + step), :], b_ref[...],
                (((1,), (1,)), ((), ())), preferred_element_type=F32,
            )
            for j in range(6):
                grid_ref[j, e : e + step] += part[:, 128 * j : 128 * j + 128].reshape(step, ROWS, 128)
        return carry

    lax.fori_loop(0, (count + 1) // 2, pair, 0)
    for j in range(6):
        xn_ref[j] = grid_ref[j, 32:35]
        xp_ref[j] = grid_ref[j, 0:3]
        for i, (up, down) in enumerate([(31, 39), (32, 0), (33, 1)]):
            yn_ref[j, i] = grid_ref[j, :, up, :]
            yp_ref[j, i] = grid_ref[j, :, down, :]
            c0[j, i] = grid_ref[j, 32 + i, 24:40, :]
            c2[j, i] = grid_ref[j, i, 24:40, :]
            c1[j, i, 0:8] = grid_ref[j, 32 + i, 0:8, :]
            c1[j, i, 8:16] = grid_ref[j, 32 + i, 32:40, :]
            c3[j, i, 0:8] = grid_ref[j, i, 0:8, :]
            c3[j, i, 8:16] = grid_ref[j, i, 32:40, :]


def spread(count, offsets, forces, base_x, base_y, base_z):
    shapes = (
        [(6, PLANES, ROWS, 128)] + [(6, 3, ROWS, 128)] * 2 + [(6, 3, PLANES, 128)] * 2 + [(6, 3, 16, 128)] * 4
    )
    return pl.pallas_call(
        spread_kernel,
        out_shape=[jax.ShapeDtypeStruct(s, F32) for s in shapes],
        in_specs=[SMEM] + [VMEM] * 5,
        out_specs=[VMEM] * len(shapes),
        scratch_shapes=[
            pltpu.VMEM((PLANES * ROWS, 768), BF16),
            pltpu.VMEM((768, 768), BF16),
            pltpu.VMEM((PLANES + 4, 128), F32),
        ],
        cost_estimate=pl.CostEstimate(flops=14_000_000_000, bytes_accessed=6_000_000, transcendentals=0),
        name="spread",
    )(count, offsets, forces, base_x, base_y, base_z)


def finish_kernel(
    count_ref, off_ref, bx_ref, by_ref, bz_ref, u_ref, rho_ref,
    s0, s1, s2, s3, s4, s5, s6, s7, force_ref, f0, f1, f2, f3, f4, f5, f6, f7,
    out_ref, vel_ref, grid_ref, state, ut_ref, a_ref, wx_ref, sems, out_sem,
):
    count = count_ref[0]
    copies = []
    for c in range(4):
        for h in range(2):
            lanes = pl.ds(128 * h, 128)
            src = u_ref.at[c, :, :, lanes] if c < 3 else rho_ref.at[:, :, lanes]
            copies.append(
                pltpu.make_async_copy(
                    src, state.at[2 * c + h, pl.ds(1, CX), pl.ds(0, CY), :], sems.at[2 * c + h]
                )
            )
    for copy in copies:
        copy.start()
    fetch = pltpu.make_async_copy(force_ref, grid_ref, sems.at[8])
    fetch.start()
    for j in range(8):
        fill = 0.0 if j < 6 else 1.0
        state[j, :, 32:40, :] = jnp.full((PLANES, 8, 128), fill, F32)
        state[j, 35, 0:32, :] = jnp.full((32, 128), fill, F32)
        state[j, 0, 0:32, :] = s0[j, 0]
        state[j, 33, 0:32, :] = s1[j, 0]
        state[j, 34, 0:32, :] = s1[j, 1]
        state[j, 1:33, 39, :] = s2[j, 0]
        state[j, 1:33, 32, :] = s3[j, 0]
        state[j, 1:33, 33, :] = s3[j, 1]
        state[j, 0, 39:40, :] = s4[j, 0:1, :]
        state[j, 0, 32:34, :] = s5[j, 0:2, :]
        state[j, 33, 39:40, :] = s6[j, 0:1, :]
        state[j, 34, 39:40, :] = s6[j, 1:2, :]
        state[j, 33, 32:34, :] = s7[j, 0:2, :]
        state[j, 34, 32:34, :] = s7[j, 2:4, :]
    fetch.wait()
    for j in range(6):
        grid_ref[j, 0:3] += f0[j]
        grid_ref[j, 32:35] += f1[j]
        for i, (up, down) in enumerate([(31, 39), (32, 0), (33, 1)]):
            grid_ref[j, :, down, :] += f2[j, i]
            grid_ref[j, :, up, :] += f3[j, i]
        for i in range(3):
            for e, piece in ((i, f4), (32 + i, f6)):
                grid_ref[j, e, 39:40, :] += piece[j, i, 7:8, :]
                grid_ref[j, e, 0:2, :] += piece[j, i, 8:10, :]
            for e, piece in ((i, f5), (32 + i, f7)):
                grid_ref[j, e, 31:32, :] += piece[j, i, 15:16, :]
                grid_ref[j, e, 32:34, :] += piece[j, i, 0:2, :]
    for copy in copies:
        copy.wait()

    def group(g, carry):
        e = 3 * g
        planes = pl.ds(e, 3)
        for h in range(2):
            half_over = 0.5 / state[6 + h, planes]
            for c in range(3):
                j = 2 * c + h
                value = state[j, planes] + grid_ref[j, planes] * half_over
                state[j, planes] = value
                flat = jnp.concatenate([value.reshape(3 * ROWS, 128), jnp.zeros((8, 128), F32)], axis=0)
                high, low = split(flat.T)
                rows = slice(128 * j, 128 * j + 128)
                ut_ref[rows, pl.ds(pl.multiple_of(128 * g, 128), 128)] = high
                ut_ref[rows, pl.ds(pl.multiple_of(128 * (GROUPS + g), 128), 128)] = low
        return carry

    lax.fori_loop(0, GROUPS, group, 0)
    outs = []
    for c in range(3):
        for h in range(2):
            outs.append(
                pltpu.make_async_copy(
                    state.at[2 * c + h, pl.ds(1, CX), pl.ds(0, CY), :],
                    out_ref.at[c, :, :, pl.ds(128 * h, 128)],
                    out_sem.at[2 * c + h],
                )
            )
    for copy in outs:
        copy.start()

    vel_ref[...] = jnp.zeros(vel_ref.shape, F32)

    def pair(p, carry):
        tables = []
        for half in range(2):
            tile = 2 * p + half
            wy, wz = marker_tables(tile, off_ref, bx_ref, by_ref, bz_ref, wx_ref)
            tables.append(wz)
            lanes = slice(128 * half, 128 * half + 128)
            for g in range(GROUPS):
                three = [wx_ref[e : e + 1, :] * wy for e in range(3 * g, 3 * g + 3)]
                high, low = split(jnp.concatenate(three + [jnp.zeros((8, 128), F32)], axis=0))
                for part, value in enumerate((high, high, low)):
                    row = 128 * (GROUPS * part + g)
                    a_ref[row : row + 128, lanes] = value
        depth = 128 * GROUPS
        picked = jnp.dot(ut_ref[...], a_ref[: 2 * depth, :], preferred_element_type=F32) + jnp.dot(
            ut_ref[:, :depth], a_ref[2 * depth :, :], preferred_element_type=F32
        )
        for half in range(2):
            tile = 2 * p + half
            live = (tile < count).astype(F32)
            for c in range(3):
                part = picked[256 * c : 256 * c + 256, 128 * half : 128 * half + 128]
                vel_ref[c, pl.ds(tile, 1), :] = live * jnp.sum(part * tables[half], axis=0, keepdims=True)
        return carry

    lax.fori_loop(0, (count + 1) // 2, pair, 0)
    for copy in outs:
        copy.wait()


def finish(count, offsets, base_x, base_y, base_z, u_old, density, halos, grid, faces):
    slots = base_x.shape[0]
    return pl.pallas_call(
        finish_kernel,
        out_shape=[jax.ShapeDtypeStruct(u_old.shape, F32), jax.ShapeDtypeStruct((3, slots, 128), F32)],
        in_specs=[SMEM] + [VMEM] * 4 + [ANY, ANY] + [VMEM] * 8 + [ANY] + [VMEM] * 8,
        out_specs=[ANY, VMEM],
        scratch_shapes=[
            pltpu.VMEM((6, PLANES, ROWS, 128), F32),
            pltpu.VMEM((8, PLANES, ROWS, 128), F32),
            pltpu.VMEM((768, 2 * 128 * GROUPS), BF16),
            pltpu.VMEM((3 * 128 * GROUPS, 256), BF16),
            pltpu.VMEM((PLANES + 4, 128), F32),
            pltpu.SemaphoreType.DMA((9,)),
            pltpu.SemaphoreType.DMA((6,)),
        ],
        cost_estimate=pl.CostEstimate(flops=14_000_000_000, bytes_accessed=12_000_000, transcendentals=0),
        name="finish",
    )(count, offsets, base_x, base_y, base_z, u_old, density, *halos, grid, *faces)


def on_device(u_old, density, offsets, forces, base_x, base_y, base_z, tile_count):
    halos = exchange(pack(u_old, density))
    grid, *faces = spread(tile_count, offsets, forces, base_x, base_y, base_z)
    faces = exchange(faces)
    u_new, velocity = finish(
        tile_count, offsets, base_x, base_y, base_z, u_old, density, halos, grid, faces
    )
    return (u_new, velocity)


def solution(mesh):
    in_specs = (
        P(None, "gx", "gy", None),
        P("gx", "gy", None),
        P(None, ("gx", "gy"), None),
        P(None, ("gx", "gy"), None),
        P(("gx", "gy"), None),
        P(("gx", "gy"), None),
        P(("gx", "gy"), None),
        P(("gx", "gy")),
    )
    out_specs = (P(None, "gx", "gy", None), P(None, ("gx", "gy"), None))
    return jax.shard_map(
        on_device, mesh=mesh, in_specs=in_specs, out_specs=out_specs, check_vma=False
    )
```

```python
import jax
import jax.numpy as jnp
from jax import lax
from jax.experimental import pallas as pl
from jax.experimental.pallas import tpu as pltpu
from jax.sharding import PartitionSpec as P


CX, CY, ROWS, PLANES = 32, 32, 40, 36
GROUPS = 12
WINDOW = 9
REACH = 4
TILES = 16
LIST = 8 * TILES
F32, BF16 = jnp.float32, jnp.bfloat16
VMEM = pl.BlockSpec(memory_space=pltpu.VMEM)
SMEM = pl.BlockSpec(memory_space=pltpu.SMEM)
ANY = pl.BlockSpec(memory_space=pl.ANY)


def stencil(frac):
    root = jnp.sqrt(1.0 + 4.0 * frac - 4.0 * frac * frac)
    return [
        (3.0 - 2.0 * frac - root) / 8.0,
        (3.0 - 2.0 * frac + root) / 8.0,
        (1.0 + 2.0 * frac + root) / 8.0,
        (1.0 + 2.0 * frac - root) / 8.0,
    ]


def spread_four(rows, targets, weights):
    row = lax.broadcasted_iota(jnp.int32, (rows, targets[0].shape[1]), 0)
    total = jnp.zeros(row.shape, F32)
    for target, weight in zip(targets, weights):
        total = jnp.where(row == target, weight, total)
    return total


def split(value):
    high = value.astype(BF16)
    return high, (value - high.astype(F32)).astype(BF16)


def split3(value):
    high, rest = value.astype(BF16), value
    parts = [high]
    for _ in range(2):
        rest = rest - parts[-1].astype(F32)
        parts.append(rest.astype(BF16))
    return parts


def x_table(rows, base_x, first, weights):
    return spread_four(rows, [base_x + (a - first) for a in range(4)], weights)


def y_table(base_y, weights):
    targets = []
    for b in range(4):
        y = base_y + (b - 1)
        targets.append(jnp.where((y < -1) | (y > CY + 1), -1, jnp.where(y < 0, ROWS - 1, y)))
    return spread_four(ROWS, targets, weights)


def one_row(base, target, weights):
    total = jnp.zeros(base.shape, F32)
    for shift, weight in enumerate(weights):
        total = jnp.where(base + (shift - 1) == target, weight, total)
    return total


def z_table(base_z, weights):
    return spread_four(256, [(base_z + c - 1) & 255 for c in range(4)], weights)


def payload_of(pay_ref, off_ref, force_ref, bx_ref, by_ref, bz_ref):
    for t in range(TILES):
        lanes = slice(128 * t, 128 * t + 128)
        for c in range(3):
            pay_ref[c : c + 1, lanes] = off_ref[c, t : t + 1, :]
            pay_ref[3 + c : 4 + c, lanes] = force_ref[c, t : t + 1, :]
        pay_ref[6:7, lanes] = bx_ref[t : t + 1, :].astype(F32)
        pay_ref[7:8, lanes] = by_ref[t : t + 1, :].astype(F32)
        pay_ref[14:15, lanes] = bz_ref[t : t + 1, :].astype(F32)
        pay_ref[15:16, lanes] = jnp.ones((1, 128), F32)
    first, second, third = split3(pay_ref[0:8, :])
    row8 = lax.broadcasted_iota(jnp.int32, first.shape, 0)
    second = jnp.where(row8 < 6, second.astype(F32), pay_ref[8:16, :])
    return jnp.concatenate([first.astype(F32), second, third.astype(F32)], axis=0).astype(BF16)


def columns_of(rows, col_ref):
    columns = jnp.concatenate([rows, jnp.zeros((128 - TILES, 128), F32)], axis=0).T
    for t in range(TILES):
        col_ref[128 * t : 128 * t + 128, :] = jnp.broadcast_to(columns[:, t : t + 1], (128, 128))


def gather(payload, col_ref, j, start, list_ref, base):
    lane = lax.broadcasted_iota(jnp.int32, (128 * TILES, 128), 1).astype(F32)
    here = col_ref[...] - (start + 256 * j).astype(F32)
    pick = jnp.concatenate([jnp.where(here == lane + 128.0 * h, 1.0, 0.0).astype(BF16) for h in range(2)], axis=1)
    parts = jnp.dot(payload, pick, preferred_element_type=F32)
    code = parts[6:7] + 64.0 * parts[7:8] + 4096.0 * parts[14:15]
    row = lax.broadcasted_iota(jnp.int32, (8, 256), 0)
    fields = parts[0:8] + parts[8:16] + parts[16:24]
    fields = jnp.where(row < 6, fields, jnp.where(row == 6, code, 0.0))
    rows = pl.multiple_of(base + 16 * j, 8)
    list_ref[pl.ds(rows, 8), :] = fields[:, :128]
    list_ref[pl.ds(rows + 8, 8), :] = fields[:, 128:]
    return parts


def running():
    i0 = lax.broadcasted_iota(jnp.int32, (128, 256), 0)
    i1 = lax.broadcasted_iota(jnp.int32, (128, 256), 1)
    return jnp.where(i0 <= i1, 1.0, 0.0).astype(BF16)


def scalar(row):
    return jnp.max(row).astype(jnp.int32)


def decode(block):
    weights = [stencil(block[c : c + 1]) for c in range(3)]
    code = block[6:7].astype(jnp.int32)
    return weights, [block[3 + c : 4 + c] for c in range(3)], (code & 63, (code >> 6) & 63, code >> 12)


def pair_of(list_ref, j):
    rows = pl.multiple_of(16 * j, 8)
    return jnp.concatenate([list_ref[pl.ds(rows, 8), :], list_ref[pl.ds(rows + 8, 8), :]], axis=1)


def pack_y_kernel(
    count_ref, off_ref, force_ref, bx_ref, by_ref, bz_ref, u_ref, rho_ref, yn_ref, yp_ref,
    slab, pay_ref, col_ref, sems,
):
    copies = []
    for c in range(4):
        for h in range(2):
            j, lanes = 2 * c + h, pl.ds(128 * h, 128)
            for n in range(2):
                ys = pl.ds((CY - 8) * n, 8)
                src = u_ref.at[c, :, ys, lanes] if c < 3 else rho_ref.at[:, ys, lanes]
                copies.append(pltpu.make_async_copy(src, slab.at[n, j], sems.at[n, j]))
    for copy in copies:
        copy.start()
    count = count_ref[0]
    tile = lax.broadcasted_iota(jnp.int32, (TILES, 128), 0)
    y = jnp.where(tile < count, by_ref[...], CY // 2)
    low, high = (y < 3).astype(F32), (y > CY - 4).astype(F32)
    counts = jnp.dot(jnp.concatenate([low, high], axis=0).astype(BF16), running(), preferred_element_type=F32)
    below = lax.broadcasted_iota(jnp.int32, (2 * TILES, 2 * TILES), 0)
    left = lax.broadcasted_iota(jnp.int32, (2 * TILES, 2 * TILES), 1)
    earlier = jnp.where((left < below) & ((left < TILES) == (below < TILES)), 1.0, 0.0).astype(BF16)
    before = jnp.dot(earlier, counts[:, 128:].astype(BF16), preferred_element_type=F32)
    place = counts[:, :128] + before - 1.0
    columns_of(low * (place[:TILES] + 1.0) + high * (place[TILES:] + 4097.0) - 1.0, col_ref)
    payload = payload_of(pay_ref, off_ref, force_ref, bx_ref, by_ref, bz_ref)
    ends = before + counts[:, 128:]
    for n, (ref, base, start) in enumerate(((yp_ref, 16 * CX, 0), (yn_ref, 8 * CX, 4096))):
        end = ends[TILES * n + TILES - 1 : TILES * n + TILES]
        size = scalar(end)

        def chunk(j, carry, ref=ref, base=base, start=start):
            gather(payload, col_ref, j, start, ref, base)
            return carry

        lax.fori_loop(0, jnp.maximum((size + 255) // 256, 1), chunk, 0)
        ref[base + 7 : base + 8, :] = end
    for copy in copies:
        copy.wait()
    for j in range(8):
        for r in range(2):
            yp_ref[(2 * j + r) * CX : (2 * j + r + 1) * CX, :] = slab[0, j, :, r, :]
        yn_ref[j * CX : (j + 1) * CX, :] = slab[1, j, :, 7, :]


def pack_y(count, arrays, u_old, density):
    return pl.pallas_call(
        pack_y_kernel,
        out_shape=[
            jax.ShapeDtypeStruct((8 * CX + LIST, 128), F32),
            jax.ShapeDtypeStruct((16 * CX + LIST, 128), F32),
        ],
        in_specs=[SMEM] + [VMEM] * 5 + [ANY, ANY],
        out_specs=[VMEM] * 2,
        scratch_shapes=[
            pltpu.VMEM((2, 8, CX, 8, 128), F32),
            pltpu.VMEM((16, 128 * TILES), F32),
            pltpu.VMEM((128 * TILES, 128), F32),
            pltpu.SemaphoreType.DMA((2, 8)),
        ],
        name="pack_y",
    )(count, *arrays, u_old, density)


def sort_kernel(
    count_ref, off_ref, force_ref, bx_ref, by_ref, bz_ref, list_ref, pos_ref, span_ref, pay_ref, col_ref
):
    count = count_ref[0]
    key_row = lax.broadcasted_iota(jnp.int32, (CX, 128), 0)
    keys = [jnp.where(t < count, bx_ref[t : t + 1, :], 2 * CX) for t in range(TILES)]
    same = [(key_row == k).astype(F32) for k in keys]
    less = [(k < key_row).astype(F32) for k in keys]
    counts = jnp.dot(jnp.concatenate(same, axis=0).astype(BF16), running(), preferred_element_type=F32)
    smaller = jnp.dot(sum(less).astype(BF16), jnp.ones((128, 128), BF16), preferred_element_type=F32)
    before = smaller
    for t in range(TILES):
        part = counts[CX * t : CX * t + CX]
        pos_ref[t : t + 1, :] = jnp.sum(same[t] * (part[:, :128] + before), axis=0, keepdims=True) - 1.0
        before = before + part[:, 128:]
    columns_of(pos_ref[...], col_ref)
    payload = payload_of(pay_ref, off_ref, force_ref, bx_ref, by_ref, bz_ref)

    def chunk(j, carry):
        parts = gather(payload, col_ref, j, 0, list_ref, 0)
        there = parts[15:16] > 0.5
        span_ref[2 * j] = jnp.min(jnp.where(there, parts[6:7], 255.0)).astype(jnp.int32)
        span_ref[2 * j + 1] = scalar(jnp.where(there, parts[6:7], 0.0))
        return carry

    lax.fori_loop(0, (count + 1) // 2, chunk, 0)
    list_ref[7:8, :] = smaller[3:4]
    list_ref[15:16, :] = smaller[CX - 3 : CX - 2]
    list_ref[23:24, :] = jnp.full((1, 128), (128 * count).astype(F32))


def sort(count, arrays):
    return pl.pallas_call(
        sort_kernel,
        out_shape=[
            jax.ShapeDtypeStruct((LIST, 128), F32),
            jax.ShapeDtypeStruct((TILES, 128), F32),
            jax.ShapeDtypeStruct((TILES,), jnp.int32),
        ],
        in_specs=[SMEM] + [VMEM] * 5,
        out_specs=[VMEM, VMEM, SMEM],
        scratch_shapes=[pltpu.VMEM((16, 128 * TILES), F32), pltpu.VMEM((128 * TILES, 128), F32)],
        cost_estimate=pl.CostEstimate(flops=3_000_000_000, bytes_accessed=400_000, transcendentals=0),
        name="sort",
    )(count, *arrays)


def pack_x_kernel(u_ref, rho_ref, below_ref, above_ref, list_ref, xn_ref, xp_ref, sems):
    copies = []
    for c in range(4):
        for h in range(2):
            j, lanes = 2 * c + h, pl.ds(128 * h, 128)
            for n, (ref, base, x) in enumerate(
                ((xn_ref, ROWS * j, CX - 1), (xp_ref, 2 * ROWS * j, 0), (xp_ref, 2 * ROWS * j + ROWS, 1))
            ):
                src = u_ref.at[c, x, :, lanes] if c < 3 else rho_ref.at[x, :, lanes]
                copies.append(pltpu.make_async_copy(src, ref.at[pl.ds(base, CY)], sems.at[n, j]))
    for copy in copies:
        copy.start()
    for j in range(8):
        fill = jnp.full((8, 128), 0.0 if j < 6 else 1.0, F32)
        for ref, base, x in (
            (xn_ref, ROWS * j, CX - 1), (xp_ref, 2 * ROWS * j, 0), (xp_ref, 2 * ROWS * j + ROWS, 1)
        ):
            ref[base + CY : base + ROWS, :] = fill
            for r in range(2):
                row = (2 * j + r) * CX + x
                ref[base + CY + r : base + CY + r + 1, :] = above_ref[row : row + 1, :]
            ref[base + ROWS - 1 : base + ROWS, :] = below_ref[j * CX + x : j * CX + x + 1, :]
    for ref, base in ((xn_ref, 8 * ROWS), (xp_ref, 16 * ROWS)):
        ref[base : base + LIST, :] = list_ref[...]
        ref[base + LIST : base + 2 * LIST, :] = below_ref[8 * CX :, :]
        ref[base + 2 * LIST : base + 3 * LIST, :] = above_ref[16 * CX :, :]
    for copy in copies:
        copy.wait()


def pack_x(u_old, density, below, above, markers):
    return pl.pallas_call(
        pack_x_kernel,
        out_shape=[
            jax.ShapeDtypeStruct((8 * ROWS + 3 * LIST, 128), F32),
            jax.ShapeDtypeStruct((16 * ROWS + 3 * LIST, 128), F32),
        ],
        in_specs=[ANY, ANY] + [VMEM] * 3,
        out_specs=[VMEM] * 2,
        scratch_shapes=[pltpu.SemaphoreType.DMA((3, 8))],
        name="pack_x",
    )(u_old, density, below, above, markers)


def spread_list(list_ref, chunks, span_ref, grid_ref, a_ref, b_ref, wx_ref):
    def chunk(j, carry):
        (weight_x, weight_y, weight_z), forces, (base_x, base_y, base_z) = decode(pair_of(list_ref, j))
        wy, wz = y_table(base_y, weight_y), z_table(base_z, weight_z)
        for c in range(3):
            high, low = split(wz * forces[c])
            for part, value in enumerate((high, high, low)):
                b_ref[256 * c : 256 * c + 256, 256 * part : 256 * part + 256] = value
        low_x, high_x = span_ref[2 * j], span_ref[2 * j + 1]

        def window(w, carry):
            first = low_x + WINDOW * w
            wx_ref[...] = x_table(16, base_x, first, weight_x)
            flat = jnp.concatenate([wx_ref[e : e + 1, :] * wy for e in range(WINDOW)], axis=0)
            high, low = split(flat)
            for part, value in enumerate((high, low, high)):
                a_ref[:, 256 * part : 256 * part + 256] = value
            sums = lax.dot_general(
                a_ref[...], b_ref[...], (((1,), (1,)), ((), ())), preferred_element_type=F32
            )
            for j in range(6):
                grid_ref[j, pl.ds(first, WINDOW)] += sums[:, 128 * j : 128 * j + 128].reshape(
                    WINDOW, ROWS, 128
                )
            return carry

        lax.fori_loop(0, (high_x + 4 - low_x + WINDOW - 1) // WINDOW, window, 0)
        return carry

    lax.fori_loop(0, chunks, chunk, 0)


def spread_edge(ref, base, first, last, dx, dy, grid_ref):
    def tile(t, carry):
        rows = pl.ds(pl.multiple_of(base + 8 * t, 8), 8)
        (weight_x, weight_y, weight_z), forces, (base_x, base_y, base_z) = decode(ref[rows, :])
        base_x, base_y = base_x + CX * dx, base_y + CY * dy
        wz = z_table(base_z, weight_z)
        if dx == 0:
            table = x_table(ROWS, base_x, 0, weight_x)
            cells = (-1, 0, 1) if dy < 0 else (CY - 1, CY, CY + 1)
            lines = [one_row(base_y, cell, weight_y) for cell in cells]
        else:
            table = y_table(base_y, weight_y)
            cells = (-1, 0, 1) if dx < 0 else (CX - 1, CX, CX + 1)
            lines = [one_row(base_x, cell, weight_x) for cell in cells]
        a_high, a_low = split(jnp.concatenate([table * line for line in lines], axis=0))
        b_high, b_low = split(jnp.concatenate([wz * force for force in forces], axis=0))
        sums = lax.dot_general(
            jnp.concatenate([a_high, a_low, a_high], axis=1),
            jnp.concatenate([b_high, b_high, b_low], axis=1),
            (((1,), (1,)), ((), ())),
            preferred_element_type=F32,
        )
        for j in range(6):
            part = sums[:, 128 * j : 128 * j + 128]
            if dx == 0:
                for i, cell in enumerate(cells):
                    row = cell % ROWS
                    grid_ref[j, 0:PLANES, row, :] += part[ROWS * i : ROWS * i + PLANES]
            else:
                grid_ref[j, cells[0] + 1 : cells[0] + 4] += part.reshape(3, ROWS, 128)
        return carry

    lax.fori_loop(first, last, tile, 0)


def tiles_of(ref, base):
    return (scalar(ref[base + 7 : base + 8, :]) + 127) // 128


def spread_kernel(count_ref, span_ref, list_ref, below_ref, above_ref, grid_ref, a_ref, b_ref, wx_ref):
    for j in range(6):
        grid_ref[j] = jnp.zeros(grid_ref.shape[1:], F32)
    spread_list(list_ref, (count_ref[0] + 1) // 2, span_ref, grid_ref, a_ref, b_ref, wx_ref)
    spread_edge(below_ref, 8 * CX, 0, tiles_of(below_ref, 8 * CX), 0, -1, grid_ref)
    spread_edge(above_ref, 16 * CX, 0, tiles_of(above_ref, 16 * CX), 0, 1, grid_ref)


def spread(count, span, markers, below, above):
    return pl.pallas_call(
        spread_kernel,
        out_shape=jax.ShapeDtypeStruct((6, PLANES + WINDOW, ROWS, 128), F32),
        in_specs=[SMEM, SMEM] + [VMEM] * 3,
        out_specs=VMEM,
        scratch_shapes=[
            pltpu.VMEM((WINDOW * ROWS, 768), BF16),
            pltpu.VMEM((768, 768), BF16),
            pltpu.VMEM((16, 256), F32),
        ],
        cost_estimate=pl.CostEstimate(flops=6_000_000_000, bytes_accessed=6_000_000, transcendentals=0),
        name="spread",
    )(count, span, markers, below, above)


def finish_kernel(
    count_ref, span_ref, list_ref, pos_ref, u_ref, rho_ref, below_ref, above_ref, left_ref, right_ref, force_ref,
    out_ref, vel_ref, grid_ref, state, ut_ref, a_ref, wx_ref, sorted_ref, sems, out_sem,
):
    count = count_ref[0]
    copies = []
    for c in range(4):
        for h in range(2):
            lanes = pl.ds(128 * h, 128)
            src = u_ref.at[c, :, :, lanes] if c < 3 else rho_ref.at[:, :, lanes]
            copies.append(
                pltpu.make_async_copy(
                    src, state.at[2 * c + h, pl.ds(1, CX), pl.ds(0, CY), :], sems.at[2 * c + h]
                )
            )
    for copy in copies:
        copy.start()
    fetch = pltpu.make_async_copy(force_ref.at[:, pl.ds(0, PLANES)], grid_ref, sems.at[8])
    fetch.start()
    for j in range(8):
        fill = 0.0 if j < 6 else 1.0
        state[j, :, 32:40, :] = jnp.full((PLANES, 8, 128), fill, F32)
        state[j, 35, 0:32, :] = jnp.full((32, 128), fill, F32)
        state[j, 0] = left_ref[ROWS * j : ROWS * (j + 1), :]
        state[j, 33] = right_ref[2 * ROWS * j : 2 * ROWS * j + ROWS, :]
        state[j, 34] = right_ref[2 * ROWS * j + ROWS : 2 * ROWS * (j + 1), :]
        state[j, 1:33, 39, :] = below_ref[CX * j : CX * (j + 1), :]
        state[j, 1:33, 32, :] = above_ref[2 * CX * j : 2 * CX * j + CX, :]
        state[j, 1:33, 33, :] = above_ref[2 * CX * j + CX : 2 * CX * (j + 1), :]
    lo, ro = 8 * ROWS, 16 * ROWS
    ends = [
        scalar(left_ref[lo + 15 : lo + 16, :]) // 128, (scalar(left_ref[lo + 23 : lo + 24, :]) + 127) // 128,
        tiles_of(right_ref, ro),
    ] + [tiles_of(ref, base + LIST * i) for ref, base in ((left_ref, lo), (right_ref, ro)) for i in (1, 2)]
    fetch.wait()
    spread_edge(left_ref, lo, ends[0], ends[1], -1, 0, grid_ref)
    spread_edge(right_ref, ro, 0, ends[2], 1, 0, grid_ref)
    spread_edge(left_ref, lo + LIST, 0, ends[3], -1, -1, grid_ref)
    spread_edge(left_ref, lo + 2 * LIST, 0, ends[4], -1, 1, grid_ref)
    spread_edge(right_ref, ro + LIST, 0, ends[5], 1, -1, grid_ref)
    spread_edge(right_ref, ro + 2 * LIST, 0, ends[6], 1, 1, grid_ref)
    for copy in copies:
        copy.wait()

    def group(g, carry):
        e = 3 * g
        planes = pl.ds(e, 3)
        for h in range(2):
            half_over = 0.5 / state[6 + h, planes]
            for c in range(3):
                j = 2 * c + h
                value = state[j, planes] + grid_ref[j, planes] * half_over
                state[j, planes] = value
                flat = jnp.concatenate([value.reshape(3 * ROWS, 128), jnp.zeros((8, 128), F32)], axis=0)
                high, low = split(flat.T)
                rows = slice(128 * j, 128 * j + 128)
                ut_ref[rows, pl.ds(pl.multiple_of(128 * g, 128), 128)] = high
                ut_ref[rows, pl.ds(pl.multiple_of(128 * (GROUPS + REACH + g), 128), 128)] = low
        return carry

    lax.fori_loop(0, GROUPS, group, 0)
    outs = []
    for c in range(3):
        for h in range(2):
            outs.append(
                pltpu.make_async_copy(
                    state.at[2 * c + h, pl.ds(1, CX), pl.ds(0, CY), :],
                    out_ref.at[c, :, :, pl.ds(128 * h, 128)],
                    out_sem.at[2 * c + h],
                )
            )
    for copy in outs:
        copy.start()

    depth = 128 * (GROUPS + REACH)
    for part in range(2):
        start = depth * part + 128 * GROUPS
        ut_ref[:, start : start + 128 * REACH] = jnp.zeros((768, 128 * REACH), BF16)
    sorted_ref[...] = jnp.zeros(sorted_ref.shape, F32)

    def chunk(j, carry):
        lanes = pl.ds(pl.multiple_of(256 * j, 256), 256)
        (weight_x, weight_y, weight_z), _, (base_x, base_y, base_z) = decode(pair_of(list_ref, j))
        wy, wz = y_table(base_y, weight_y), z_table(base_z, weight_z)
        first_group = span_ref[2 * j] // 3
        high_x = span_ref[2 * j + 1]

        def window(w, sums):
            g = first_group + REACH * w
            wx_ref[...] = x_table(16, base_x, 3 * g, weight_x)
            for i in range(REACH):
                three = [wx_ref[e : e + 1, :] * wy for e in range(3 * i, 3 * i + 3)]
                high, low = split(jnp.concatenate(three + [jnp.zeros((8, 256), F32)], axis=0))
                a_ref[128 * i : 128 * i + 128, :] = high
                a_ref[128 * (REACH + i) : 128 * (REACH + i) + 128, :] = low
            wide = 128 * REACH
            ut_high = ut_ref[:, pl.ds(pl.multiple_of(128 * g, 128), wide)]
            ut_low = ut_ref[:, pl.ds(pl.multiple_of(depth + 128 * g, 128), wide)]
            high, low = a_ref[:wide, :], a_ref[wide:, :]
            picked = (
                jnp.dot(ut_high, high, preferred_element_type=F32)
                + jnp.dot(ut_high, low, preferred_element_type=F32)
                + jnp.dot(ut_low, high, preferred_element_type=F32)
            )
            return tuple(
                total + jnp.sum(picked[256 * c : 256 * c + 256] * wz, axis=0, keepdims=True)
                for c, total in enumerate(sums)
            )

        windows = (high_x + 4 - 3 * first_group + 3 * REACH - 1) // (3 * REACH)
        sums = lax.fori_loop(0, windows, window, tuple(jnp.zeros((1, 256), F32) for _ in range(3)))
        for c in range(3):
            sorted_ref[c : c + 1, lanes] = sums[c]
        return carry

    lax.fori_loop(0, (count + 1) // 2, chunk, 0)

    parts = jnp.concatenate([p.astype(F32) for p in split3(sorted_ref[...])], axis=0).astype(BF16)
    place = lax.broadcasted_iota(jnp.int32, (2048, 128), 0).astype(F32)
    vel_ref[...] = jnp.zeros(vel_ref.shape, F32)

    def back(t, carry):
        pick = jnp.concatenate(
            [jnp.where(place == pos_ref[pl.ds(2 * t + h, 1), :], 1.0, 0.0).astype(BF16) for h in range(2)], axis=1
        )
        sums = jnp.dot(parts, pick, preferred_element_type=F32)
        sums = sums[0:8] + sums[8:16] + sums[16:24]
        for h in range(2):
            for c in range(3):
                vel_ref[c, pl.ds(2 * t + h, 1), :] = sums[c : c + 1, 128 * h : 128 * h + 128]
        return carry

    lax.fori_loop(0, (count + 1) // 2, back, 0)
    for copy in outs:
        copy.wait()


def finish(count, span, markers, pos, u_old, density, below, above, left, right, grid):
    slots = pos.shape[0]
    return pl.pallas_call(
        finish_kernel,
        out_shape=[jax.ShapeDtypeStruct(u_old.shape, F32), jax.ShapeDtypeStruct((3, slots, 128), F32)],
        in_specs=[SMEM, SMEM, VMEM, VMEM] + [ANY, ANY] + [VMEM] * 4 + [ANY],
        out_specs=[ANY, VMEM],
        scratch_shapes=[
            pltpu.VMEM((6, PLANES, ROWS, 128), F32),
            pltpu.VMEM((8, PLANES, ROWS, 128), F32),
            pltpu.VMEM((768, 2 * 128 * (GROUPS + REACH)), BF16),
            pltpu.VMEM((2 * 128 * REACH, 256), BF16),
            pltpu.VMEM((16, 256), F32),
            pltpu.VMEM((8, 128 * slots), F32),
            pltpu.SemaphoreType.DMA((9,)),
            pltpu.SemaphoreType.DMA((6,)),
        ],
        cost_estimate=pl.CostEstimate(flops=6_000_000_000, bytes_accessed=12_000_000, transcendentals=0),
        name="finish",
    )(count, span, markers, pos, u_old, density, below, above, left, right, grid)


def shift(value, axis, steps):
    count = lax.axis_size(axis)
    return lax.ppermute(value, axis, [(i, (i + steps) % count) for i in range(count)])


def on_device(u_old, density, offsets, forces, base_x, base_y, base_z, tile_count):
    arrays = (offsets, forces, base_x, base_y, base_z)
    to_next, to_previous = pack_y(tile_count, arrays, u_old, density)
    below = shift(to_next, "gy", 1)
    above = shift(to_previous, "gy", -1)
    markers, pos, span = sort(tile_count, arrays)
    to_next, to_previous = pack_x(u_old, density, below, above, markers)
    left = shift(to_next, "gx", 1)
    right = shift(to_previous, "gx", -1)
    grid = spread(tile_count, span, markers, below, above)
    return finish(tile_count, span, markers, pos, u_old, density, below, above, left, right, grid)


def solution(mesh):
    in_specs = (
        P(None, "gx", "gy", None),
        P("gx", "gy", None),
        P(None, ("gx", "gy"), None),
        P(None, ("gx", "gy"), None),
        P(("gx", "gy"), None),
        P(("gx", "gy"), None),
        P(("gx", "gy"), None),
        P(("gx", "gy")),
    )
    out_specs = (P(None, "gx", "gy", None), P(None, ("gx", "gy"), None))
    return jax.shard_map(
        on_device, mesh=mesh, in_specs=in_specs, out_specs=out_specs, check_vma=False
    )
```

```python
import jax
import jax.numpy as jnp
from jax import lax
from jax.experimental import pallas as pl
from jax.experimental.pallas import tpu as pltpu
from jax.sharding import PartitionSpec as P


CX, CY, ROWS, PLANES = 32, 32, 40, 36
GROUPS = 12
WINDOW = 9
TALL = 368
REACH = 4
TILES = 16
LIST = 8 * TILES
F32, BF16 = jnp.float32, jnp.bfloat16
VMEM = pl.BlockSpec(memory_space=pltpu.VMEM)
SMEM = pl.BlockSpec(memory_space=pltpu.SMEM)
HBM = pl.BlockSpec(memory_space=pltpu.MemorySpace.HBM)
MIB = 2**20


def stencil(frac):
    root = jnp.sqrt(1.0 + 4.0 * frac - 4.0 * frac * frac)
    return [
        (3.0 - 2.0 * frac - root) / 8.0,
        (3.0 - 2.0 * frac + root) / 8.0,
        (1.0 + 2.0 * frac + root) / 8.0,
        (1.0 + 2.0 * frac - root) / 8.0,
    ]


def spread_four(rows, targets, weights):
    row = lax.broadcasted_iota(jnp.int32, (rows, targets[0].shape[1]), 0)
    total = jnp.zeros(row.shape, F32)
    for target, weight in zip(targets, weights):
        total = jnp.where(row == target, weight, total)
    return total


def split(value):
    high = value.astype(BF16)
    return high, (value - high.astype(F32)).astype(BF16)


def split3(value):
    high, rest = value.astype(BF16), value
    parts = [high]
    for _ in range(2):
        rest = rest - parts[-1].astype(F32)
        parts.append(rest.astype(BF16))
    return parts


def x_table(rows, base_x, first, weights):
    return spread_four(rows, [base_x + (a - first) for a in range(4)], weights)


def y_table(base_y, weights):
    targets = []
    for b in range(4):
        y = base_y + (b - 1)
        targets.append(jnp.where((y < -1) | (y > CY + 1), -1, jnp.where(y < 0, ROWS - 1, y)))
    return spread_four(ROWS, targets, weights)


def one_row(base, target, weights):
    total = jnp.zeros(base.shape, F32)
    for shift, weight in enumerate(weights):
        total = jnp.where(base + (shift - 1) == target, weight, total)
    return total


def z_table(base_z, weights):
    return spread_four(256, [(base_z + c - 1) & 255 for c in range(4)], weights)


def fill_payload(pay_ref, off_ref, force_ref, bx_ref, by_ref, bz_ref):
    for t in range(TILES):
        lanes = slice(128 * t, 128 * t + 128)
        for c in range(3):
            pay_ref[c : c + 1, lanes] = off_ref[c, t : t + 1, :]
            pay_ref[3 + c : 4 + c, lanes] = force_ref[c, t : t + 1, :]
        pay_ref[6:7, lanes] = bx_ref[t : t + 1, :].astype(F32)
        pay_ref[7:8, lanes] = by_ref[t : t + 1, :].astype(F32)
        pay_ref[14:15, lanes] = bz_ref[t : t + 1, :].astype(F32)
        pay_ref[15:16, lanes] = jnp.ones((1, 128), F32)


def payload_of(pay_ref):
    first, second, third = split3(pay_ref[0:8, :])
    row8 = lax.broadcasted_iota(jnp.int32, first.shape, 0)
    second = jnp.where(row8 < 6, second.astype(F32), pay_ref[8:16, :])
    return jnp.concatenate([first.astype(F32), second, third.astype(F32)], axis=0).astype(BF16)


def columns_of(rows, col_ref):
    columns = jnp.concatenate([rows, jnp.zeros((128 - TILES, 128), F32)], axis=0).T
    for t in range(TILES):
        col_ref[128 * t : 128 * t + 128, :] = jnp.broadcast_to(columns[:, t : t + 1], (128, 128))


def gather(payload, col_ref, j, start, list_ref, base):
    lane = lax.broadcasted_iota(jnp.int32, (128 * TILES, 128), 1).astype(F32)
    here = col_ref[...] - (start + 256 * j).astype(F32)
    pick = jnp.concatenate([jnp.where(here == lane + 128.0 * h, 1.0, 0.0).astype(BF16) for h in range(2)], axis=1)
    parts = jnp.dot(payload, pick, preferred_element_type=F32)
    code = parts[6:7] + 64.0 * parts[7:8] + 4096.0 * parts[14:15]
    row = lax.broadcasted_iota(jnp.int32, (8, 256), 0)
    fields = parts[0:8] + parts[8:16] + parts[16:24]
    fields = jnp.where(row < 6, fields, jnp.where(row == 6, code, 0.0))
    rows = pl.multiple_of(base + 16 * j, 8)
    list_ref[pl.ds(rows, 8), :] = fields[:, :128]
    list_ref[pl.ds(rows + 8, 8), :] = fields[:, 128:]
    return parts


def running():
    i0 = lax.broadcasted_iota(jnp.int32, (128, 256), 0)
    i1 = lax.broadcasted_iota(jnp.int32, (128, 256), 1)
    return jnp.where(i0 <= i1, 1.0, 0.0).astype(BF16)


def scalar(row):
    return jnp.max(row).astype(jnp.int32)


def decode(block):
    weights = [stencil(block[c : c + 1]) for c in range(3)]
    code = block[6:7].astype(jnp.int32)
    return weights, [block[3 + c : 4 + c] for c in range(3)], (code & 63, (code >> 6) & 63, code >> 12)


def pair_of(list_ref, j):
    rows = pl.multiple_of(16 * j, 8)
    return jnp.concatenate([list_ref[pl.ds(rows, 8), :], list_ref[pl.ds(rows + 8, 8), :]], axis=1)


def pack_y_kernel(
    count_ref, off_hbm, force_hbm, bx_hbm, by_hbm, bz_hbm, u_ref, rho_ref, yn_ref, yp_ref, pay_ref,
    off_ref, force_ref, bx_ref, by_ref, bz_ref, slab, col_ref, sems,
):
    loads = [
        pltpu.make_async_copy(src, dst, sems.at[2, n])
        for n, (src, dst) in enumerate(
            zip((by_hbm, bx_hbm, bz_hbm, off_hbm, force_hbm), (by_ref, bx_ref, bz_ref, off_ref, force_ref))
        )
    ]
    for load in loads:
        load.start()
    copies = []
    for c in range(4):
        for h in range(2):
            j, lanes = 2 * c + h, pl.ds(128 * h, 128)
            for n in range(2):
                ys = pl.ds((CY - 8) * n, 8)
                src = u_ref.at[c, :, ys, lanes] if c < 3 else rho_ref.at[:, ys, lanes]
                copies.append(pltpu.make_async_copy(src, slab.at[n, j], sems.at[n, j]))
    for copy in copies:
        copy.start()
    count = count_ref[0]
    for load in loads:
        load.wait()
    tile = lax.broadcasted_iota(jnp.int32, (TILES, 128), 0)
    y = jnp.where(tile < count, by_ref[...], CY // 2)
    low, high = (y < 3).astype(F32), (y > CY - 4).astype(F32)
    counts = jnp.dot(jnp.concatenate([low, high], axis=0).astype(BF16), running(), preferred_element_type=F32)
    below = lax.broadcasted_iota(jnp.int32, (2 * TILES, 2 * TILES), 0)
    left = lax.broadcasted_iota(jnp.int32, (2 * TILES, 2 * TILES), 1)
    earlier = jnp.where((left < below) & ((left < TILES) == (below < TILES)), 1.0, 0.0).astype(BF16)
    before = jnp.dot(earlier, counts[:, 128:].astype(BF16), preferred_element_type=F32)
    place = counts[:, :128] + before - 1.0
    columns_of(low * (place[:TILES] + 1.0) + high * (place[TILES:] + 4097.0) - 1.0, col_ref)
    fill_payload(pay_ref, off_ref, force_ref, bx_ref, by_ref, bz_ref)
    payload = payload_of(pay_ref)
    ends = before + counts[:, 128:]
    for n, (ref, base, start) in enumerate(((yp_ref, 16 * CX, 0), (yn_ref, 8 * CX, 4096))):
        end = ends[TILES * n + TILES - 1 : TILES * n + TILES]
        size = scalar(end)

        def chunk(j, carry, ref=ref, base=base, start=start):
            gather(payload, col_ref, j, start, ref, base)
            return carry

        lax.fori_loop(0, jnp.maximum((size + 255) // 256, 1), chunk, 0)
        ref[base + 7 : base + 8, :] = end
    for copy in copies:
        copy.wait()
    for j in range(8):
        for r in range(2):
            yp_ref[(2 * j + r) * CX : (2 * j + r + 1) * CX, :] = slab[0, j, :, r, :]
        yn_ref[j * CX : (j + 1) * CX, :] = slab[1, j, :, 7, :]


def pack_y(count, arrays, u_old, density):
    return pl.pallas_call(
        pack_y_kernel,
        out_shape=[
            jax.ShapeDtypeStruct((8 * CX + LIST, 128), F32),
            jax.ShapeDtypeStruct((16 * CX + LIST, 128), F32),
            jax.ShapeDtypeStruct((16, 128 * TILES), F32),
        ],
        in_specs=[SMEM] + [HBM] * 7,
        out_specs=[VMEM] * 3,
        scratch_shapes=[
            pltpu.VMEM((3, TILES, 128), F32),
            pltpu.VMEM((3, TILES, 128), F32),
            pltpu.VMEM((TILES, 128), jnp.int32),
            pltpu.VMEM((TILES, 128), jnp.int32),
            pltpu.VMEM((TILES, 128), jnp.int32),
            pltpu.VMEM((2, 8, CX, 8, 128), F32),
            pltpu.VMEM((128 * TILES, 128), F32),
            pltpu.SemaphoreType.DMA((3, 8)),
        ],
        name="pack_y",
    )(count, *arrays, u_old, density)


def sort_kernel(count_ref, pay_ref, list_ref, pos_ref, span_ref, col_ref):
    count = count_ref[0]
    list_ref[...] = jnp.zeros(list_ref.shape, F32)
    key_row = lax.broadcasted_iota(jnp.int32, (CX, 128), 0)
    keys = [
        jnp.where(t < count, pay_ref[6:7, 128 * t : 128 * t + 128].astype(jnp.int32), 2 * CX) for t in range(TILES)
    ]
    same = [(key_row == k).astype(F32) for k in keys]
    less = [(k < key_row).astype(F32) for k in keys]
    counts = jnp.dot(jnp.concatenate(same, axis=0).astype(BF16), running(), preferred_element_type=F32)
    smaller = jnp.dot(sum(less).astype(BF16), jnp.ones((128, 128), BF16), preferred_element_type=F32)
    before = smaller
    for t in range(TILES):
        part = counts[CX * t : CX * t + CX]
        pos_ref[t : t + 1, :] = jnp.sum(same[t] * (part[:, :128] + before), axis=0, keepdims=True) - 1.0
        before = before + part[:, 128:]
    columns_of(pos_ref[...], col_ref)
    payload = payload_of(pay_ref)

    def chunks(p, carry):
        for j in (2 * p, 2 * p + 1):
            parts = gather(payload, col_ref, j, 0, list_ref, 0)
            there = parts[15:16] > 0.5
            span_ref[2 * j] = jnp.min(jnp.where(there, parts[6:7], CX - 1.0)).astype(jnp.int32)
            span_ref[2 * j + 1] = scalar(jnp.where(there, parts[6:7], 0.0))
        return carry

    lax.fori_loop(0, (count + 3) // 4, chunks, 0)
    list_ref[7:8, :] = smaller[3:4]
    list_ref[15:16, :] = smaller[CX - 3 : CX - 2]
    list_ref[23:24, :] = jnp.full((1, 128), (128 * count).astype(F32))


def sort(count, payload):
    return pl.pallas_call(
        sort_kernel,
        out_shape=[
            jax.ShapeDtypeStruct((LIST, 128), F32),
            jax.ShapeDtypeStruct((TILES, 128), F32),
            jax.ShapeDtypeStruct((TILES,), jnp.int32),
        ],
        in_specs=[SMEM, VMEM],
        out_specs=[VMEM, VMEM, SMEM],
        compiler_params=pltpu.CompilerParams(vmem_limit_bytes=8 * MIB),
        scratch_shapes=[pltpu.VMEM((128 * TILES, 128), F32)],
        cost_estimate=pl.CostEstimate(flops=3_000_000_000, bytes_accessed=400_000, transcendentals=0),
        name="sort",
    )(count, payload)


def pack_x_kernel(u_ref, rho_ref, below_ref, above_ref, list_ref, xn_ref, xp_ref, sems):
    copies = []
    for c in range(4):
        for h in range(2):
            j, lanes = 2 * c + h, pl.ds(128 * h, 128)
            for n, (ref, base, x) in enumerate(
                ((xn_ref, ROWS * j, CX - 1), (xp_ref, 2 * ROWS * j, 0), (xp_ref, 2 * ROWS * j + ROWS, 1))
            ):
                src = u_ref.at[c, x, :, lanes] if c < 3 else rho_ref.at[x, :, lanes]
                copies.append(pltpu.make_async_copy(src, ref.at[pl.ds(base, CY)], sems.at[n, j]))
    for copy in copies:
        copy.start()
    for j in range(8):
        fill = jnp.full((8, 128), 0.0 if j < 6 else 1.0, F32)
        for ref, base, x in (
            (xn_ref, ROWS * j, CX - 1), (xp_ref, 2 * ROWS * j, 0), (xp_ref, 2 * ROWS * j + ROWS, 1)
        ):
            ref[base + CY : base + ROWS, :] = fill
            for r in range(2):
                row = (2 * j + r) * CX + x
                ref[base + CY + r : base + CY + r + 1, :] = above_ref[row : row + 1, :]
            ref[base + ROWS - 1 : base + ROWS, :] = below_ref[j * CX + x : j * CX + x + 1, :]
    for ref, base in ((xn_ref, 8 * ROWS), (xp_ref, 16 * ROWS)):
        ref[base : base + LIST, :] = list_ref[...]
        ref[base + LIST : base + 2 * LIST, :] = below_ref[8 * CX :, :]
        ref[base + 2 * LIST : base + 3 * LIST, :] = above_ref[16 * CX :, :]
    for copy in copies:
        copy.wait()


def pack_x(u_old, density, below, above, markers):
    return pl.pallas_call(
        pack_x_kernel,
        out_shape=[
            jax.ShapeDtypeStruct((8 * ROWS + 3 * LIST, 128), F32),
            jax.ShapeDtypeStruct((16 * ROWS + 3 * LIST, 128), F32),
        ],
        in_specs=[HBM, HBM] + [VMEM] * 3,
        out_specs=[VMEM] * 2,
        compiler_params=pltpu.CompilerParams(vmem_limit_bytes=8 * MIB),
        scratch_shapes=[pltpu.SemaphoreType.DMA((3, 8))],
        name="pack_x",
    )(u_old, density, below, above, markers)


def spread_list(list_ref, pairs, span_ref, grid_ref, a_ref, b_ref, wx_ref):
    def tables(j, k):
        (weight_x, weight_y, weight_z), forces, (base_x, base_y, base_z) = decode(pair_of(list_ref, j))
        wy, wz = y_table(base_y, weight_y), z_table(base_z, weight_z)
        for c in range(3):
            high, low = split(wz * forces[c])
            b_ref[k, 0, 256 * c : 256 * c + 256, :] = high
            b_ref[k, 1, 256 * c : 256 * c + 256, :] = low
        return weight_x, base_x, wy

    def window(first, weight_x, base_x, wy, k):
        wx_ref[k] = x_table(16, base_x, first, weight_x)
        rows = [wx_ref[k, e : e + 1, :] * wy for e in range(WINDOW)]
        high, low = split(jnp.concatenate(rows + [jnp.zeros((TALL - WINDOW * ROWS, 256), F32)], axis=0))
        a_ref[k, :TALL, :] = high
        a_ref[k, TALL:, :] = low
        across = (((1,), (1,)), ((), ()))
        both = lax.dot_general(a_ref[k], b_ref[k, 0], across, preferred_element_type=F32)
        rest = lax.dot_general(a_ref[k, :TALL, :], b_ref[k, 1], across, preferred_element_type=F32)
        sums = (both[:TALL] + rest + both[TALL:])[: WINDOW * ROWS]
        for j in range(6):
            grid_ref[j, pl.ds(first, WINDOW)] += sums[:, 128 * j : 128 * j + 128].reshape(
                WINDOW, ROWS, 128
            )

    def two(p, carry):
        both = [(tables(2 * p + k, k), k) for k in range(2)]
        for table, k in both:
            window(span_ref[2 * (2 * p + k)], *table, k)
        for table, k in both:
            low_x, high_x = span_ref[2 * (2 * p + k)], span_ref[2 * (2 * p + k) + 1]

            def more(w, carry, table=table, k=k, low_x=low_x):
                window(low_x + WINDOW * w, *table, k)
                return carry

            lax.fori_loop(1, (high_x + 4 - low_x + WINDOW - 1) // WINDOW, more, 0)
        return carry

    lax.fori_loop(0, pairs, two, 0)


def spread_edges(edges, grid_ref):
    for edge in edges:
        edge_tile(*edge[:3], *edge[4:], grid_ref)
    for edge in edges:
        lax.fori_loop(
            edge[2] + 1, edge[3], lambda t, carry, e=edge: edge_tile(*e[:2], t, *e[4:], grid_ref) or carry, 0
        )


def edge_tile(ref, base, t, dx, dy, grid_ref):
    rows = pl.ds(pl.multiple_of(base + 8 * t, 8), 8)
    (weight_x, weight_y, weight_z), forces, (base_x, base_y, base_z) = decode(ref[rows, :])
    base_x, base_y = base_x + CX * dx, base_y + CY * dy
    wz = z_table(base_z, weight_z)
    if dx == 0:
        table = x_table(ROWS, base_x, 0, weight_x)
        cells = (-1, 0, 1) if dy < 0 else (CY - 1, CY, CY + 1)
        lines = [one_row(base_y, cell, weight_y) for cell in cells]
    else:
        table = y_table(base_y, weight_y)
        cells = (-1, 0, 1) if dx < 0 else (CX - 1, CX, CX + 1)
        lines = [one_row(base_x, cell, weight_x) for cell in cells]
    a_high, a_low = split(jnp.concatenate([table * line for line in lines], axis=0))
    b_high, b_low = split(jnp.concatenate([wz * force for force in forces], axis=0))
    sums = lax.dot_general(
        jnp.concatenate([a_high, a_low, a_high], axis=1),
        jnp.concatenate([b_high, b_high, b_low], axis=1),
        (((1,), (1,)), ((), ())),
        preferred_element_type=F32,
    )
    for j in range(6):
        part = sums[:, 128 * j : 128 * j + 128]
        if dx == 0:
            for i, cell in enumerate(cells):
                row = cell % ROWS
                grid_ref[j, 0:PLANES, row, :] += part[ROWS * i : ROWS * i + PLANES]
        else:
            grid_ref[j, cells[0] + 1 : cells[0] + 4] += part.reshape(3, ROWS, 128)


def tiles_of(ref, base):
    return (scalar(ref[base + 7 : base + 8, :]) + 127) // 128


def spread_kernel(count_ref, span_ref, list_ref, below_ref, above_ref, grid_ref, a_ref, b_ref, wx_ref):
    for j in range(6):
        grid_ref[j] = jnp.zeros(grid_ref.shape[1:], F32)
    spread_list(list_ref, (count_ref[0] + 3) // 4, span_ref, grid_ref, a_ref, b_ref, wx_ref)
    spread_edges(
        [
            (below_ref, 8 * CX, 0, tiles_of(below_ref, 8 * CX), 0, -1),
            (above_ref, 16 * CX, 0, tiles_of(above_ref, 16 * CX), 0, 1),
        ],
        grid_ref,
    )


def spread(count, span, markers, below, above):
    return pl.pallas_call(
        spread_kernel,
        out_shape=jax.ShapeDtypeStruct((6, PLANES + WINDOW, ROWS, 128), F32),
        in_specs=[SMEM, SMEM] + [VMEM] * 3,
        out_specs=VMEM,
        compiler_params=pltpu.CompilerParams(vmem_limit_bytes=16 * MIB),
        scratch_shapes=[
            pltpu.VMEM((2, 2 * TALL, 256), BF16),
            pltpu.VMEM((2, 2, 768, 256), BF16),
            pltpu.VMEM((2, 16, 256), F32),
        ],
        cost_estimate=pl.CostEstimate(flops=6_000_000_000, bytes_accessed=6_000_000, transcendentals=0),
        name="spread",
    )(count, span, markers, below, above)


def finish_kernel(
    count_ref, span_ref, list_ref, pos_ref, u_ref, rho_ref, below_ref, above_ref, left_ref, right_ref, force_ref,
    out_ref, vel_ref, grid_ref, state, ut_ref, a_ref, wx_ref, sorted_ref, sems, out_sem,
):
    count = count_ref[0]
    copies = []
    for c in range(4):
        for h in range(2):
            lanes = pl.ds(128 * h, 128)
            src = u_ref.at[c, :, :, lanes] if c < 3 else rho_ref.at[:, :, lanes]
            copies.append(
                pltpu.make_async_copy(
                    src, state.at[2 * c + h, pl.ds(1, CX), pl.ds(0, CY), :], sems.at[2 * c + h]
                )
            )
    for copy in copies:
        copy.start()
    for j in range(8):
        fill = 0.0 if j < 6 else 1.0
        state[j, :, 32:40, :] = jnp.full((PLANES, 8, 128), fill, F32)
        state[j, 35, 0:32, :] = jnp.full((32, 128), fill, F32)
        state[j, 0] = left_ref[ROWS * j : ROWS * (j + 1), :]
        state[j, 33] = right_ref[2 * ROWS * j : 2 * ROWS * j + ROWS, :]
        state[j, 34] = right_ref[2 * ROWS * j + ROWS : 2 * ROWS * (j + 1), :]
        state[j, 1:33, 39, :] = below_ref[CX * j : CX * (j + 1), :]
        state[j, 1:33, 32, :] = above_ref[2 * CX * j : 2 * CX * j + CX, :]
        state[j, 1:33, 33, :] = above_ref[2 * CX * j + CX : 2 * CX * (j + 1), :]
    lo, ro = 8 * ROWS, 16 * ROWS
    ends = [
        scalar(left_ref[lo + 15 : lo + 16, :]) // 128, (scalar(left_ref[lo + 23 : lo + 24, :]) + 127) // 128,
        tiles_of(right_ref, ro),
    ] + [tiles_of(ref, base + LIST * i) for ref, base in ((left_ref, lo), (right_ref, ro)) for i in (1, 2)]
    spread_edges(
        [
            (left_ref, lo, jnp.minimum(ends[0], TILES - 1), ends[1], -1, 0),
            (right_ref, ro, 0, ends[2], 1, 0),
            (left_ref, lo + LIST, 0, ends[3], -1, -1),
            (left_ref, lo + 2 * LIST, 0, ends[4], -1, 1),
            (right_ref, ro + LIST, 0, ends[5], 1, -1),
            (right_ref, ro + 2 * LIST, 0, ends[6], 1, 1),
        ],
        grid_ref,
    )
    for copy in copies:
        copy.wait()

    def group(g, carry):
        e = 3 * g
        planes = pl.ds(e, 3)
        for h in range(2):
            half_over = 0.5 / state[6 + h, planes]
            for c in range(3):
                j = 2 * c + h
                value = state[j, planes] + grid_ref[j, planes] * half_over
                state[j, planes] = value
                flat = jnp.concatenate([value.reshape(3 * ROWS, 128), jnp.zeros((8, 128), F32)], axis=0)
                high, low = split(flat.T)
                rows = slice(128 * j, 128 * j + 128)
                ut_ref[rows, pl.ds(pl.multiple_of(128 * g, 128), 128)] = high
                ut_ref[rows, pl.ds(pl.multiple_of(128 * (GROUPS + REACH + g), 128), 128)] = low
        return carry

    lax.fori_loop(0, GROUPS, group, 0)
    outs = []
    for c in range(3):
        for h in range(2):
            outs.append(
                pltpu.make_async_copy(
                    state.at[2 * c + h, pl.ds(1, CX), pl.ds(0, CY), :],
                    out_ref.at[c, :, :, pl.ds(128 * h, 128)],
                    out_sem.at[2 * c + h],
                )
            )
    for copy in outs:
        copy.start()

    depth = 128 * (GROUPS + REACH)
    for part in range(2):
        start = depth * part + 128 * GROUPS
        ut_ref[:, start : start + 128 * REACH] = jnp.zeros((768, 128 * REACH), BF16)
    sorted_ref[...] = jnp.zeros(sorted_ref.shape, F32)

    wide = 128 * REACH

    def tables(j):
        (weight_x, weight_y, weight_z), _, (base_x, base_y, base_z) = decode(pair_of(list_ref, j))
        return weight_x, base_x, y_table(base_y, weight_y), z_table(base_z, weight_z)

    def window(g, weight_x, base_x, wy, wz, k):
        wx_ref[k] = x_table(16, base_x, 3 * g, weight_x)
        for i in range(REACH):
            three = [wx_ref[k, e : e + 1, :] * wy for e in range(3 * i, 3 * i + 3)]
            high, low = split(jnp.concatenate(three + [jnp.zeros((8, 256), F32)], axis=0))
            a_ref[k, 128 * i : 128 * i + 128, :] = high
            a_ref[k, 128 * (REACH + i) : 128 * (REACH + i) + 128, :] = low
        ut_high = ut_ref[:, pl.ds(pl.multiple_of(128 * g, 128), wide)]
        ut_low = ut_ref[:, pl.ds(pl.multiple_of(depth + 128 * g, 128), wide)]
        high, low = a_ref[k, :wide, :], a_ref[k, wide:, :]
        picked = (
            jnp.dot(ut_high, high, preferred_element_type=F32)
            + jnp.dot(ut_high, low, preferred_element_type=F32)
            + jnp.dot(ut_low, high, preferred_element_type=F32)
        )
        return [jnp.sum(picked[256 * c : 256 * c + 256] * wz, axis=0, keepdims=True) for c in range(3)]

    def two(p, carry):
        both = [(tables(2 * p + k), k) for k in range(2)]
        for table, k in both:
            j = 2 * p + k
            lanes = pl.ds(pl.multiple_of(256 * j, 256), 256)
            for c, value in enumerate(window(span_ref[2 * j] // 3, *table, k)):
                sorted_ref[c : c + 1, lanes] = value
        for table, k in both:
            j = 2 * p + k
            lanes = pl.ds(pl.multiple_of(256 * j, 256), 256)
            first, high_x = span_ref[2 * j] // 3, span_ref[2 * j + 1]

            def more(w, carry, table=table, k=k, lanes=lanes, first=first):
                for c, value in enumerate(window(first + REACH * w, *table, k)):
                    sorted_ref[c : c + 1, lanes] += value
                return carry

            lax.fori_loop(1, (high_x + 4 - 3 * first + 3 * REACH - 1) // (3 * REACH), more, 0)
        return carry

    lax.fori_loop(0, (count + 3) // 4, two, 0)

    parts = jnp.concatenate([p.astype(F32) for p in split3(sorted_ref[...])], axis=0).astype(BF16)
    place = lax.broadcasted_iota(jnp.int32, (2048, 128), 0).astype(F32)
    vel_ref[...] = jnp.zeros(vel_ref.shape, F32)

    def back(p, carry):
        for t in (4 * p, 4 * p + 2):
            pick = jnp.concatenate(
                [jnp.where(place == pos_ref[pl.ds(t + h, 1), :], 1.0, 0.0).astype(BF16) for h in range(2)], axis=1
            )
            sums = jnp.dot(parts, pick, preferred_element_type=F32)
            sums = sums[0:8] + sums[8:16] + sums[16:24]
            for h in range(2):
                for c in range(3):
                    vel_ref[c, pl.ds(t + h, 1), :] = sums[c : c + 1, 128 * h : 128 * h + 128]
        return carry

    lax.fori_loop(0, (count + 3) // 4, back, 0)
    for copy in outs:
        copy.wait()


def finish(count, span, markers, pos, u_old, density, below, above, left, right, grid):
    slots = pos.shape[0]
    return pl.pallas_call(
        finish_kernel,
        out_shape=[
            jax.ShapeDtypeStruct(u_old.shape, F32),
            jax.ShapeDtypeStruct((3, slots, 128), F32),
            jax.ShapeDtypeStruct(grid.shape, F32),
        ],
        input_output_aliases={10: 2},
        in_specs=[SMEM, SMEM, VMEM, VMEM] + [HBM, HBM] + [VMEM] * 5,
        out_specs=[HBM, VMEM, VMEM],
        compiler_params=pltpu.CompilerParams(vmem_limit_bytes=36 * MIB),
        scratch_shapes=[
            pltpu.VMEM((8, PLANES, ROWS, 128), F32),
            pltpu.VMEM((768, 2 * 128 * (GROUPS + REACH)), BF16),
            pltpu.VMEM((2, 2 * 128 * REACH, 256), BF16),
            pltpu.VMEM((2, 16, 256), F32),
            pltpu.VMEM((8, 128 * slots), F32),
            pltpu.SemaphoreType.DMA((9,)),
            pltpu.SemaphoreType.DMA((6,)),
        ],
        cost_estimate=pl.CostEstimate(flops=6_000_000_000, bytes_accessed=12_000_000, transcendentals=0),
        name="finish",
    )(count, span, markers, pos, u_old, density, below, above, left, right, grid)[:2]


def shift(value, axis, steps):
    count = lax.axis_size(axis)
    return lax.ppermute(value, axis, [(i, (i + steps) % count) for i in range(count)])


def on_device(u_old, density, offsets, forces, base_x, base_y, base_z, tile_count):
    arrays = (offsets, forces, base_x, base_y, base_z)
    to_next, to_previous, payload = pack_y(tile_count, arrays, u_old, density)
    below = shift(to_next, "gy", 1)
    above = shift(to_previous, "gy", -1)
    markers, pos, span = sort(tile_count, payload)
    to_next, to_previous = pack_x(u_old, density, below, above, markers)
    left = shift(to_next, "gx", 1)
    right = shift(to_previous, "gx", -1)
    grid = spread(tile_count, span, markers, below, above)
    return finish(tile_count, span, markers, pos, u_old, density, below, above, left, right, grid)[:2]


def solution(mesh):
    in_specs = (
        P(None, "gx", "gy", None),
        P("gx", "gy", None),
        P(None, ("gx", "gy"), None),
        P(None, ("gx", "gy"), None),
        P(("gx", "gy"), None),
        P(("gx", "gy"), None),
        P(("gx", "gy"), None),
        P(("gx", "gy")),
    )
    out_specs = (P(None, "gx", "gy", None), P(None, ("gx", "gy"), None))
    return jax.shard_map(
        on_device, mesh=mesh, in_specs=in_specs, out_specs=out_specs, check_vma=False
    )
```

```python
import jax
import jax.numpy as jnp
from jax import lax
from jax.experimental import pallas as pl
from jax.experimental.pallas import tpu as pltpu
from jax.sharding import PartitionSpec as P


CX, CY, ROWS, PLANES = 32, 32, 40, 36
GROUPS = 12
WINDOW = 9
TALL = 368
REACH = 4
TILES = 16
LIST = 8 * TILES
F32, BF16 = jnp.float32, jnp.bfloat16
VMEM = pl.BlockSpec(memory_space=pltpu.VMEM)
SMEM = pl.BlockSpec(memory_space=pltpu.SMEM)
HBM = pl.BlockSpec(memory_space=pltpu.MemorySpace.HBM)
MIB = 2**20


def stencil(frac):
    root = jnp.sqrt(1.0 + 4.0 * frac - 4.0 * frac * frac)
    return [
        (3.0 - 2.0 * frac - root) / 8.0,
        (3.0 - 2.0 * frac + root) / 8.0,
        (1.0 + 2.0 * frac + root) / 8.0,
        (1.0 + 2.0 * frac - root) / 8.0,
    ]


def spread_four(rows, targets, weights):
    row = lax.broadcasted_iota(jnp.int32, (rows, targets[0].shape[1]), 0)
    total = jnp.zeros(row.shape, F32)
    for target, weight in zip(targets, weights):
        total = jnp.where(row == target, weight, total)
    return total


def split(value):
    high = value.astype(BF16)
    return high, (value - high.astype(F32)).astype(BF16)


def split3(value):
    high, rest = value.astype(BF16), value
    parts = [high]
    for _ in range(2):
        rest = rest - parts[-1].astype(F32)
        parts.append(rest.astype(BF16))
    return parts


def x_table(rows, base_x, first, weights):
    return spread_four(rows, [base_x + (a - first) for a in range(4)], weights)


def y_table(base_y, weights):
    targets = []
    for b in range(4):
        y = base_y + (b - 1)
        targets.append(jnp.where((y < -1) | (y > CY + 1), -1, jnp.where(y < 0, ROWS - 1, y)))
    return spread_four(ROWS, targets, weights)


def one_row(base, target, weights):
    total = jnp.zeros(base.shape, F32)
    for shift, weight in enumerate(weights):
        total = jnp.where(base + (shift - 1) == target, weight, total)
    return total


def z_table(base_z, weights):
    return spread_four(256, [(base_z + c - 1) & 255 for c in range(4)], weights)


def fill_payload(pay_ref, off_ref, force_ref, bx_ref, by_ref, bz_ref):
    for t in range(TILES):
        lanes = slice(128 * t, 128 * t + 128)
        for c in range(3):
            pay_ref[c : c + 1, lanes] = off_ref[c, t : t + 1, :]
            pay_ref[3 + c : 4 + c, lanes] = force_ref[c, t : t + 1, :]
        pay_ref[6:7, lanes] = bx_ref[t : t + 1, :].astype(F32)
        pay_ref[7:8, lanes] = by_ref[t : t + 1, :].astype(F32)
        pay_ref[14:15, lanes] = bz_ref[t : t + 1, :].astype(F32)
        pay_ref[15:16, lanes] = jnp.ones((1, 128), F32)


def payload_of(pay_ref):
    first, second, third = split3(pay_ref[0:8, :])
    row8 = lax.broadcasted_iota(jnp.int32, first.shape, 0)
    second = jnp.where(row8 < 6, second.astype(F32), pay_ref[8:16, :])
    return jnp.concatenate([first.astype(F32), second, third.astype(F32)], axis=0).astype(BF16)


def columns_of(rows, col_ref):
    columns = jnp.concatenate([rows, jnp.zeros((128 - TILES, 128), F32)], axis=0).T
    for t in range(TILES):
        col_ref[128 * t : 128 * t + 128, :] = jnp.broadcast_to(columns[:, t : t + 1], (128, 128))


def gather(payload, col_ref, j, start, list_ref, base):
    lane = lax.broadcasted_iota(jnp.int32, (128 * TILES, 128), 1).astype(F32)
    here = col_ref[...] - (start + 256 * j).astype(F32)
    pick = jnp.concatenate([jnp.where(here == lane + 128.0 * h, 1.0, 0.0).astype(BF16) for h in range(2)], axis=1)
    parts = jnp.dot(payload, pick, preferred_element_type=F32)
    code = parts[6:7] + 64.0 * parts[7:8] + 4096.0 * parts[14:15]
    row = lax.broadcasted_iota(jnp.int32, (8, 256), 0)
    fields = parts[0:8] + parts[8:16] + parts[16:24]
    fields = jnp.where(row < 6, fields, jnp.where(row == 6, code, 0.0))
    rows = pl.multiple_of(base + 16 * j, 8)
    list_ref[pl.ds(rows, 8), :] = fields[:, :128]
    list_ref[pl.ds(rows + 8, 8), :] = fields[:, 128:]
    return parts


def running():
    i0 = lax.broadcasted_iota(jnp.int32, (128, 256), 0)
    i1 = lax.broadcasted_iota(jnp.int32, (128, 256), 1)
    return jnp.where(i0 <= i1, 1.0, 0.0).astype(BF16)


def scalar(row):
    return jnp.max(row).astype(jnp.int32)


def decode(block):
    weights = [stencil(block[c : c + 1]) for c in range(3)]
    code = block[6:7].astype(jnp.int32)
    return weights, [block[3 + c : 4 + c] for c in range(3)], (code & 63, (code >> 6) & 63, code >> 12)


def pair_of(list_ref, j):
    rows = pl.multiple_of(16 * j, 8)
    return jnp.concatenate([list_ref[pl.ds(rows, 8), :], list_ref[pl.ds(rows + 8, 8), :]], axis=1)


def pack_y_kernel(
    count_ref, off_hbm, force_hbm, bx_hbm, by_hbm, bz_hbm, u_ref, rho_ref, yn_ref, yp_ref, pay_ref,
    off_ref, force_ref, bx_ref, by_ref, bz_ref, slab, col_ref, sems,
):
    loads = [
        pltpu.make_async_copy(src, dst, sems.at[2, n])
        for n, (src, dst) in enumerate(
            zip((by_hbm, bx_hbm, bz_hbm, off_hbm, force_hbm), (by_ref, bx_ref, bz_ref, off_ref, force_ref))
        )
    ]
    for load in loads:
        load.start()
    copies = []
    for c in range(4):
        for h in range(2):
            j, lanes = 2 * c + h, pl.ds(128 * h, 128)
            for n in range(2):
                ys = pl.ds((CY - 8) * n, 8)
                src = u_ref.at[c, :, ys, lanes] if c < 3 else rho_ref.at[:, ys, lanes]
                copies.append(pltpu.make_async_copy(src, slab.at[n, j], sems.at[n, j]))
    for copy in copies:
        copy.start()
    count = count_ref[0]
    for load in loads:
        load.wait()
    tile = lax.broadcasted_iota(jnp.int32, (TILES, 128), 0)
    y = jnp.where(tile < count, by_ref[...], CY // 2)
    low, high = (y < 3).astype(F32), (y > CY - 4).astype(F32)
    counts = jnp.dot(jnp.concatenate([low, high], axis=0).astype(BF16), running(), preferred_element_type=F32)
    below = lax.broadcasted_iota(jnp.int32, (2 * TILES, 2 * TILES), 0)
    left = lax.broadcasted_iota(jnp.int32, (2 * TILES, 2 * TILES), 1)
    earlier = jnp.where((left < below) & ((left < TILES) == (below < TILES)), 1.0, 0.0).astype(BF16)
    before = jnp.dot(earlier, counts[:, 128:].astype(BF16), preferred_element_type=F32)
    place = counts[:, :128] + before - 1.0
    columns_of(low * (place[:TILES] + 1.0) + high * (place[TILES:] + 4097.0) - 1.0, col_ref)
    fill_payload(pay_ref, off_ref, force_ref, bx_ref, by_ref, bz_ref)
    payload = payload_of(pay_ref)
    ends = before + counts[:, 128:]
    for n, (ref, base, start) in enumerate(((yp_ref, 16 * CX, 0), (yn_ref, 8 * CX, 4096))):
        end = ends[TILES * n + TILES - 1 : TILES * n + TILES]
        size = scalar(end)

        def chunk(j, carry, ref=ref, base=base, start=start):
            gather(payload, col_ref, j, start, ref, base)
            return carry

        lax.fori_loop(0, jnp.maximum((size + 255) // 256, 1), chunk, 0)
        ref[base + 7 : base + 8, :] = end
    for copy in copies:
        copy.wait()
    for j in range(8):
        for r in range(2):
            yp_ref[(2 * j + r) * CX : (2 * j + r + 1) * CX, :] = slab[0, j, :, r, :]
        yn_ref[j * CX : (j + 1) * CX, :] = slab[1, j, :, 7, :]


def pack_y(count, arrays, u_old, density):
    return pl.pallas_call(
        pack_y_kernel,
        out_shape=[
            jax.ShapeDtypeStruct((8 * CX + LIST, 128), F32),
            jax.ShapeDtypeStruct((16 * CX + LIST, 128), F32),
            jax.ShapeDtypeStruct((16, 128 * TILES), F32),
        ],
        in_specs=[SMEM] + [HBM] * 7,
        out_specs=[VMEM] * 3,
        scratch_shapes=[
            pltpu.VMEM((3, TILES, 128), F32),
            pltpu.VMEM((3, TILES, 128), F32),
            pltpu.VMEM((TILES, 128), jnp.int32),
            pltpu.VMEM((TILES, 128), jnp.int32),
            pltpu.VMEM((TILES, 128), jnp.int32),
            pltpu.VMEM((2, 8, CX, 8, 128), F32),
            pltpu.VMEM((128 * TILES, 128), F32),
            pltpu.SemaphoreType.DMA((3, 8)),
        ],
        name="pack_y",
    )(count, *arrays, u_old, density)


def sort_kernel(count_ref, pay_ref, list_ref, pos_ref, span_ref, col_ref):
    count = count_ref[0]
    list_ref[...] = jnp.zeros(list_ref.shape, F32)
    key_row = lax.broadcasted_iota(jnp.int32, (CX, 128), 0)
    keys = [
        jnp.where(t < count, pay_ref[6:7, 128 * t : 128 * t + 128].astype(jnp.int32), 2 * CX) for t in range(TILES)
    ]
    same = [(key_row == k).astype(F32) for k in keys]
    less = [(k < key_row).astype(F32) for k in keys]
    counts = jnp.dot(jnp.concatenate(same, axis=0).astype(BF16), running(), preferred_element_type=F32)
    smaller = jnp.dot(sum(less).astype(BF16), jnp.ones((128, 128), BF16), preferred_element_type=F32)
    before = smaller
    for t in range(TILES):
        part = counts[CX * t : CX * t + CX]
        pos_ref[t : t + 1, :] = jnp.sum(same[t] * (part[:, :128] + before), axis=0, keepdims=True) - 1.0
        before = before + part[:, 128:]
    columns_of(pos_ref[...], col_ref)
    payload = payload_of(pay_ref)

    def chunks(p, carry):
        for j in (2 * p, 2 * p + 1):
            parts = gather(payload, col_ref, j, 0, list_ref, 0)
            there = parts[15:16] > 0.5
            span_ref[2 * j] = jnp.min(jnp.where(there, parts[6:7], CX - 1.0)).astype(jnp.int32)
            span_ref[2 * j + 1] = scalar(jnp.where(there, parts[6:7], 0.0))
        return carry

    lax.fori_loop(0, (count + 3) // 4, chunks, 0)
    list_ref[7:8, :] = smaller[3:4]
    list_ref[15:16, :] = smaller[CX - 3 : CX - 2]
    list_ref[23:24, :] = jnp.full((1, 128), (128 * count).astype(F32))


def sort(count, payload):
    return pl.pallas_call(
        sort_kernel,
        out_shape=[
            jax.ShapeDtypeStruct((LIST, 128), F32),
            jax.ShapeDtypeStruct((TILES, 128), F32),
            jax.ShapeDtypeStruct((TILES,), jnp.int32),
        ],
        in_specs=[SMEM, VMEM],
        out_specs=[VMEM, VMEM, SMEM],
        compiler_params=pltpu.CompilerParams(vmem_limit_bytes=8 * MIB),
        scratch_shapes=[pltpu.VMEM((128 * TILES, 128), F32)],
        cost_estimate=pl.CostEstimate(flops=3_000_000_000, bytes_accessed=400_000, transcendentals=0),
        name="sort",
    )(count, payload)


def pack_x_kernel(u_ref, rho_ref, below_ref, above_ref, list_ref, xn_ref, xp_ref, sems):
    copies = []
    for c in range(4):
        for h in range(2):
            j, lanes = 2 * c + h, pl.ds(128 * h, 128)
            for n, (ref, base, x) in enumerate(
                ((xn_ref, ROWS * j, CX - 1), (xp_ref, 2 * ROWS * j, 0), (xp_ref, 2 * ROWS * j + ROWS, 1))
            ):
                src = u_ref.at[c, x, :, lanes] if c < 3 else rho_ref.at[x, :, lanes]
                copies.append(pltpu.make_async_copy(src, ref.at[pl.ds(base, CY)], sems.at[n, j]))
    for copy in copies:
        copy.start()
    for j in range(8):
        fill = jnp.full((8, 128), 0.0 if j < 6 else 1.0, F32)
        for ref, base, x in (
            (xn_ref, ROWS * j, CX - 1), (xp_ref, 2 * ROWS * j, 0), (xp_ref, 2 * ROWS * j + ROWS, 1)
        ):
            ref[base + CY : base + ROWS, :] = fill
            for r in range(2):
                row = (2 * j + r) * CX + x
                ref[base + CY + r : base + CY + r + 1, :] = above_ref[row : row + 1, :]
            ref[base + ROWS - 1 : base + ROWS, :] = below_ref[j * CX + x : j * CX + x + 1, :]
    for ref, base in ((xn_ref, 8 * ROWS), (xp_ref, 16 * ROWS)):
        ref[base : base + LIST, :] = list_ref[...]
        ref[base + LIST : base + 2 * LIST, :] = below_ref[8 * CX :, :]
        ref[base + 2 * LIST : base + 3 * LIST, :] = above_ref[16 * CX :, :]
    for copy in copies:
        copy.wait()


def pack_x(u_old, density, below, above, markers):
    return pl.pallas_call(
        pack_x_kernel,
        out_shape=[
            jax.ShapeDtypeStruct((8 * ROWS + 3 * LIST, 128), F32),
            jax.ShapeDtypeStruct((16 * ROWS + 3 * LIST, 128), F32),
        ],
        in_specs=[HBM, HBM] + [VMEM] * 3,
        out_specs=[VMEM] * 2,
        compiler_params=pltpu.CompilerParams(vmem_limit_bytes=8 * MIB),
        scratch_shapes=[pltpu.SemaphoreType.DMA((3, 8))],
        name="pack_x",
    )(u_old, density, below, above, markers)


def spread_list(list_ref, pairs, span_ref, grid_ref, a_ref, b_ref, wx_ref):
    def tables(j, k):
        (weight_x, weight_y, weight_z), forces, (base_x, base_y, base_z) = decode(pair_of(list_ref, j))
        wy, wz = y_table(base_y, weight_y), z_table(base_z, weight_z)
        for c in range(3):
            high, low = split(wz * forces[c])
            b_ref[k, 0, 256 * c : 256 * c + 256, :] = high
            b_ref[k, 1, 256 * c : 256 * c + 256, :] = low
        return weight_x, base_x, wy

    def window(first, weight_x, base_x, wy, k):
        wx_ref[k] = x_table(16, base_x, first, weight_x)
        rows = [wx_ref[k, e : e + 1, :] * wy for e in range(WINDOW)]
        high, low = split(jnp.concatenate(rows + [jnp.zeros((TALL - WINDOW * ROWS, 256), F32)], axis=0))
        a_ref[k, :TALL, :] = high
        a_ref[k, TALL:, :] = low
        across = (((1,), (1,)), ((), ()))
        both = lax.dot_general(a_ref[k], b_ref[k, 0], across, preferred_element_type=F32)
        rest = lax.dot_general(a_ref[k, :TALL, :], b_ref[k, 1], across, preferred_element_type=F32)
        sums = (both[:TALL] + rest + both[TALL:])[: WINDOW * ROWS]
        for j in range(6):
            grid_ref[j, pl.ds(first, WINDOW)] += sums[:, 128 * j : 128 * j + 128].reshape(
                WINDOW, ROWS, 128
            )

    def two(p, carry):
        both = [(tables(2 * p + k, k), k) for k in range(2)]
        for table, k in both:
            window(span_ref[2 * (2 * p + k)], *table, k)
        for table, k in both:
            low_x, high_x = span_ref[2 * (2 * p + k)], span_ref[2 * (2 * p + k) + 1]

            def more(w, carry, table=table, k=k, low_x=low_x):
                window(low_x + WINDOW * w, *table, k)
                return carry

            lax.fori_loop(1, (high_x + 4 - low_x + WINDOW - 1) // WINDOW, more, 0)
        return carry

    lax.fori_loop(0, pairs, two, 0)


def spread_edges(edges, grid_ref):
    for edge in edges:
        edge_tile(*edge[:3], *edge[4:], grid_ref)
    for edge in edges:
        lax.fori_loop(
            edge[2] + 1, edge[3], lambda t, carry, e=edge: edge_tile(*e[:2], t, *e[4:], grid_ref) or carry, 0
        )


def edge_tile(ref, base, t, dx, dy, grid_ref):
    rows = pl.ds(pl.multiple_of(base + 8 * t, 8), 8)
    (weight_x, weight_y, weight_z), forces, (base_x, base_y, base_z) = decode(ref[rows, :])
    base_x, base_y = base_x + CX * dx, base_y + CY * dy
    wz = z_table(base_z, weight_z)
    if dx == 0:
        table = x_table(ROWS, base_x, 0, weight_x)
        cells = (-1, 0, 1) if dy < 0 else (CY - 1, CY, CY + 1)
        lines = [one_row(base_y, cell, weight_y) for cell in cells]
    else:
        table = y_table(base_y, weight_y)
        cells = (-1, 0, 1) if dx < 0 else (CX - 1, CX, CX + 1)
        lines = [one_row(base_x, cell, weight_x) for cell in cells]
    a_high, a_low = split(jnp.concatenate([table * line for line in lines], axis=0))
    b_high, b_low = split(jnp.concatenate([wz * force for force in forces], axis=0))
    sums = lax.dot_general(
        jnp.concatenate([a_high, a_low, a_high], axis=1),
        jnp.concatenate([b_high, b_high, b_low], axis=1),
        (((1,), (1,)), ((), ())),
        preferred_element_type=F32,
    )
    for j in range(6):
        part = sums[:, 128 * j : 128 * j + 128]
        if dx == 0:
            for i, cell in enumerate(cells):
                row = cell % ROWS
                grid_ref[j, 0:PLANES, row, :] += part[ROWS * i : ROWS * i + PLANES]
        else:
            grid_ref[j, cells[0] + 1 : cells[0] + 4] += part.reshape(3, ROWS, 128)


def tiles_of(ref, base):
    return (scalar(ref[base + 7 : base + 8, :]) + 127) // 128


def spread_kernel(count_ref, span_ref, list_ref, grid_ref, a_ref, b_ref, wx_ref):
    for j in range(6):
        grid_ref[j] = jnp.zeros(grid_ref.shape[1:], F32)
    spread_list(list_ref, (count_ref[0] + 3) // 4, span_ref, grid_ref, a_ref, b_ref, wx_ref)


def spread(count, span, markers):
    return pl.pallas_call(
        spread_kernel,
        out_shape=jax.ShapeDtypeStruct((6, PLANES + WINDOW, ROWS, 128), F32),
        in_specs=[SMEM, SMEM, VMEM],
        out_specs=VMEM,
        compiler_params=pltpu.CompilerParams(vmem_limit_bytes=16 * MIB),
        scratch_shapes=[
            pltpu.VMEM((2, 2 * TALL, 256), BF16),
            pltpu.VMEM((2, 2, 768, 256), BF16),
            pltpu.VMEM((2, 16, 256), F32),
        ],
        cost_estimate=pl.CostEstimate(flops=6_000_000_000, bytes_accessed=6_000_000, transcendentals=0),
        name="spread",
    )(count, span, markers)


DEPTH = 128 * (GROUPS + REACH)


def advance(g, old, grid_ref, fresh_ref, ut_ref, owned):
    planes = pl.ds(3 * g, 3)
    for h in range(2):
        half_over = 0.5 / old(6 + h)
        for c in range(3):
            j = 2 * c + h
            value = old(j) + grid_ref[j, planes] * half_over
            for i, x in owned:
                fresh_ref[j, x] = value[i, :CY]
            flat = jnp.concatenate([value.reshape(3 * ROWS, 128), jnp.zeros((8, 128), F32)], axis=0)
            high, low = split(flat.T)
            rows = slice(128 * j, 128 * j + 128)
            ut_ref[rows, pl.ds(pl.multiple_of(128 * g, 128), 128)] = high
            ut_ref[rows, pl.ds(pl.multiple_of(DEPTH + 128 * g, 128), 128)] = low


def own_plane(u_ref, rho_ref, rim_ref, j, e):
    lanes = slice(128 * (j % 2), 128 * (j % 2) + 128)
    inner = u_ref[j // 2, e - 1, :, lanes] if j < 6 else rho_ref[e - 1, :, lanes]
    return jnp.concatenate([inner, rim_ref[j, e]], axis=0)


def middle_kernel(u_ref, rho_ref, below_ref, above_ref, grid_in, grid_ref, fresh_ref, ut_ref, rim_ref):
    spread_edges(
        [
            (below_ref, 8 * CX, 0, tiles_of(below_ref, 8 * CX), 0, -1),
            (above_ref, 16 * CX, 0, tiles_of(above_ref, 16 * CX), 0, 1),
        ],
        grid_ref,
    )
    for j in range(8):
        rim_ref[j] = jnp.full((PLANES, 8, 128), 0.0 if j < 6 else 1.0, F32)
        rim_ref[j, 1:33, 7, :] = below_ref[CX * j : CX * (j + 1), :]
        rim_ref[j, 1:33, 0, :] = above_ref[2 * CX * j : 2 * CX * j + CX, :]
        rim_ref[j, 1:33, 1, :] = above_ref[2 * CX * j + CX : 2 * CX * (j + 1), :]
    for part in range(2):
        start = DEPTH * part + 128 * GROUPS
        ut_ref[:, start : start + 128 * REACH] = jnp.zeros((768, 128 * REACH), BF16)

    def group(g, carry):
        def old(j):
            return jnp.stack([own_plane(u_ref, rho_ref, rim_ref, j, 3 * g + i) for i in range(3)])

        advance(g, old, grid_ref, fresh_ref, ut_ref, [(i, 3 * g + i - 1) for i in range(3)])
        return carry

    lax.fori_loop(1, 10, group, 0)


def middle(u_old, density, below, above, grid):
    return pl.pallas_call(
        middle_kernel,
        out_shape=[
            jax.ShapeDtypeStruct(grid.shape, F32),
            jax.ShapeDtypeStruct((6, CX, CY, 128), F32),
            jax.ShapeDtypeStruct((768, 2 * DEPTH), BF16),
            jax.ShapeDtypeStruct((8, PLANES, 8, 128), F32),
        ],
        in_specs=[VMEM] * 5,
        out_specs=[VMEM] * 4,
        input_output_aliases={4: 0},
        compiler_params=pltpu.CompilerParams(vmem_limit_bytes=24 * MIB),
        cost_estimate=pl.CostEstimate(flops=6_000_000_000, bytes_accessed=6_000_000, transcendentals=0),
        name="middle",
    )(u_old, density, below, above, grid)


def finish_kernel(
    count_ref, span_ref, list_ref, pos_ref, u_ref, rho_ref, rim_ref, left_ref, right_ref, grid_in, fresh_in, ut_in,
    out_ref, vel_ref, grid_ref, fresh_ref, ut_ref, a_ref, wx_ref, sorted_ref, out_sem,
):
    count = count_ref[0]
    lo, ro = 8 * ROWS, 16 * ROWS
    ends = [
        scalar(left_ref[lo + 15 : lo + 16, :]) // 128, (scalar(left_ref[lo + 23 : lo + 24, :]) + 127) // 128,
        tiles_of(right_ref, ro),
    ] + [tiles_of(ref, base + LIST * i) for ref, base in ((left_ref, lo), (right_ref, ro)) for i in (1, 2)]
    spread_edges(
        [
            (left_ref, lo, jnp.minimum(ends[0], TILES - 1), ends[1], -1, 0),
            (right_ref, ro, 0, ends[2], 1, 0),
            (left_ref, lo + LIST, 0, ends[3], -1, -1),
            (left_ref, lo + 2 * LIST, 0, ends[4], -1, 1),
            (right_ref, ro + LIST, 0, ends[5], 1, -1),
            (right_ref, ro + 2 * LIST, 0, ends[6], 1, 1),
        ],
        grid_ref,
    )

    def plane(j, e):
        if e == 0:
            return left_ref[ROWS * j : ROWS * (j + 1), :]
        if e in (33, 34):
            return right_ref[ROWS * (2 * j + e - 33) : ROWS * (2 * j + e - 32), :]
        if e == 35:
            return jnp.full((ROWS, 128), 0.0 if j < 6 else 1.0, F32)
        return own_plane(u_ref, rho_ref, rim_ref, j, e)

    for g in (0, 10, 11):
        advance(
            g, lambda j, g=g: jnp.stack([plane(j, 3 * g + i) for i in range(3)]), grid_ref, fresh_ref, ut_ref,
            [(i, 3 * g + i - 1) for i in range(3) if 1 <= 3 * g + i <= CX],
        )
    outs = []
    for c in range(3):
        for h in range(2):
            outs.append(
                pltpu.make_async_copy(
                    fresh_ref.at[2 * c + h], out_ref.at[c, :, :, pl.ds(128 * h, 128)], out_sem.at[2 * c + h]
                )
            )
    for copy in outs:
        copy.start()
    sorted_ref[...] = jnp.zeros(sorted_ref.shape, F32)
    wide = 128 * REACH

    def tables(j):
        (weight_x, weight_y, weight_z), _, (base_x, base_y, base_z) = decode(pair_of(list_ref, j))
        return weight_x, base_x, y_table(base_y, weight_y), z_table(base_z, weight_z)

    def window(g, weight_x, base_x, wy, wz, k):
        wx_ref[k] = x_table(16, base_x, 3 * g, weight_x)
        for i in range(REACH):
            three = [wx_ref[k, e : e + 1, :] * wy for e in range(3 * i, 3 * i + 3)]
            high, low = split(jnp.concatenate(three + [jnp.zeros((8, 256), F32)], axis=0))
            a_ref[k, 128 * i : 128 * i + 128, :] = high
            a_ref[k, 128 * (REACH + i) : 128 * (REACH + i) + 128, :] = low
        ut_high = ut_ref[:, pl.ds(pl.multiple_of(128 * g, 128), wide)]
        ut_low = ut_ref[:, pl.ds(pl.multiple_of(DEPTH + 128 * g, 128), wide)]
        high, low = a_ref[k, :wide, :], a_ref[k, wide:, :]
        picked = (
            jnp.dot(ut_high, high, preferred_element_type=F32)
            + jnp.dot(ut_high, low, preferred_element_type=F32)
            + jnp.dot(ut_low, high, preferred_element_type=F32)
        )
        return [jnp.sum(picked[256 * c : 256 * c + 256] * wz, axis=0, keepdims=True) for c in range(3)]

    def two(p, carry):
        both = [(tables(2 * p + k), k) for k in range(2)]
        for table, k in both:
            j = 2 * p + k
            lanes = pl.ds(pl.multiple_of(256 * j, 256), 256)
            for c, value in enumerate(window(span_ref[2 * j] // 3, *table, k)):
                sorted_ref[c : c + 1, lanes] = value
        for table, k in both:
            j = 2 * p + k
            lanes = pl.ds(pl.multiple_of(256 * j, 256), 256)
            first, high_x = span_ref[2 * j] // 3, span_ref[2 * j + 1]

            def more(w, carry, table=table, k=k, lanes=lanes, first=first):
                for c, value in enumerate(window(first + REACH * w, *table, k)):
                    sorted_ref[c : c + 1, lanes] += value
                return carry

            lax.fori_loop(1, (high_x + 4 - 3 * first + 3 * REACH - 1) // (3 * REACH), more, 0)
        return carry

    lax.fori_loop(0, (count + 3) // 4, two, 0)

    parts = jnp.concatenate([p.astype(F32) for p in split3(sorted_ref[...])], axis=0).astype(BF16)
    place = lax.broadcasted_iota(jnp.int32, (2048, 128), 0).astype(F32)
    vel_ref[...] = jnp.zeros(vel_ref.shape, F32)

    def back(p, carry):
        for t in (4 * p, 4 * p + 2):
            pick = jnp.concatenate(
                [jnp.where(place == pos_ref[pl.ds(t + h, 1), :], 1.0, 0.0).astype(BF16) for h in range(2)], axis=1
            )
            sums = jnp.dot(parts, pick, preferred_element_type=F32)
            sums = sums[0:8] + sums[8:16] + sums[16:24]
            for h in range(2):
                for c in range(3):
                    vel_ref[c, pl.ds(t + h, 1), :] = sums[c : c + 1, 128 * h : 128 * h + 128]
        return carry

    lax.fori_loop(0, (count + 3) // 4, back, 0)
    for copy in outs:
        copy.wait()


def finish(count, span, markers, pos, u_old, density, rim, left, right, grid, fresh, ut):
    slots = pos.shape[0]
    return pl.pallas_call(
        finish_kernel,
        out_shape=[
            jax.ShapeDtypeStruct(u_old.shape, F32),
            jax.ShapeDtypeStruct((3, slots, 128), F32),
            jax.ShapeDtypeStruct(grid.shape, F32),
            jax.ShapeDtypeStruct(fresh.shape, F32),
            jax.ShapeDtypeStruct(ut.shape, BF16),
        ],
        in_specs=[SMEM, SMEM] + [VMEM] * 10,
        out_specs=[HBM] + [VMEM] * 4,
        input_output_aliases={9: 2, 10: 3, 11: 4},
        compiler_params=pltpu.CompilerParams(vmem_limit_bytes=24 * MIB),
        scratch_shapes=[
            pltpu.VMEM((2, 2 * 128 * REACH, 256), BF16),
            pltpu.VMEM((2, 16, 256), F32),
            pltpu.VMEM((8, 128 * slots), F32),
            pltpu.SemaphoreType.DMA((6,)),
        ],
        cost_estimate=pl.CostEstimate(flops=6_000_000_000, bytes_accessed=12_000_000, transcendentals=0),
        name="finish",
    )(count, span, markers, pos, u_old, density, rim, left, right, grid, fresh, ut)[:2]


def shift(value, axis, steps):
    count = lax.axis_size(axis)
    return lax.ppermute(value, axis, [(i, (i + steps) % count) for i in range(count)])


def on_device(u_old, density, offsets, forces, base_x, base_y, base_z, tile_count):
    arrays = (offsets, forces, base_x, base_y, base_z)
    to_next, to_previous, payload = pack_y(tile_count, arrays, u_old, density)
    below = shift(to_next, "gy", 1)
    above = shift(to_previous, "gy", -1)
    markers, pos, span = sort(tile_count, payload)
    grid = spread(tile_count, span, markers)
    to_next, to_previous = pack_x(u_old, density, below, above, markers)
    left = shift(to_next, "gx", 1)
    right = shift(to_previous, "gx", -1)
    grid, fresh, ut, rim = middle(u_old, density, below, above, grid)
    return finish(tile_count, span, markers, pos, u_old, density, rim, left, right, grid, fresh, ut)


def solution(mesh):
    in_specs = (
        P(None, "gx", "gy", None),
        P("gx", "gy", None),
        P(None, ("gx", "gy"), None),
        P(None, ("gx", "gy"), None),
        P(("gx", "gy"), None),
        P(("gx", "gy"), None),
        P(("gx", "gy"), None),
        P(("gx", "gy")),
    )
    out_specs = (P(None, "gx", "gy", None), P(None, ("gx", "gy"), None))
    return jax.shard_map(
        on_device, mesh=mesh, in_specs=in_specs, out_specs=out_specs, check_vma=False
    )
```

```python
import jax
import jax.numpy as jnp
from jax import lax
from jax.experimental import pallas as pl
from jax.experimental.pallas import tpu as pltpu
from jax.sharding import PartitionSpec as P


CX, CY, ROWS, PLANES = 32, 32, 40, 36
GROUPS = 12
WINDOW = 9
TALL = 368
REACH = 4
TILES = 16
DEEP, COUNTS = 8 * TILES, 9 * TILES
LIST = 9 * TILES + 8
PATCH = 6 * 24
F32, BF16 = jnp.float32, jnp.bfloat16
VMEM = pl.BlockSpec(memory_space=pltpu.VMEM)
SMEM = pl.BlockSpec(memory_space=pltpu.SMEM)
HBM = pl.BlockSpec(memory_space=pltpu.MemorySpace.HBM)
MIB = 2**20


def stencil(frac):
    root = jnp.sqrt(1.0 + 4.0 * frac - 4.0 * frac * frac)
    return [
        (3.0 - 2.0 * frac - root) / 8.0,
        (3.0 - 2.0 * frac + root) / 8.0,
        (1.0 + 2.0 * frac + root) / 8.0,
        (1.0 + 2.0 * frac - root) / 8.0,
    ]


def spread_four(rows, targets, weights):
    row = lax.broadcasted_iota(jnp.int32, (rows, targets[0].shape[1]), 0)
    total = jnp.zeros(row.shape, F32)
    for target, weight in zip(targets, weights):
        total = jnp.where(row == target, weight, total)
    return total


def split(value):
    high = value.astype(BF16)
    return high, (value - high.astype(F32)).astype(BF16)


def split3(value):
    high, rest = value.astype(BF16), value
    parts = [high]
    for _ in range(2):
        rest = rest - parts[-1].astype(F32)
        parts.append(rest.astype(BF16))
    return parts


def x_table(rows, base_x, first, weights):
    return spread_four(rows, [base_x + (a - first) for a in range(4)], weights)


def y_table(base_y, weights):
    targets = []
    for b in range(4):
        y = base_y + (b - 1)
        targets.append(jnp.where((y < -1) | (y > CY + 1), -1, jnp.where(y < 0, ROWS - 1, y)))
    return spread_four(ROWS, targets, weights)


def one_row(base, target, weights):
    total = jnp.zeros(base.shape, F32)
    for shift, weight in enumerate(weights):
        total = jnp.where(base + (shift - 1) == target, weight, total)
    return total


def z_table(base_z, weights):
    return spread_four(256, [(base_z + c - 1) & 255 for c in range(4)], weights)


def fill_payload(pay_ref, off_ref, force_ref, bx_ref, by_ref, bz_ref):
    for t in range(TILES):
        lanes = slice(128 * t, 128 * t + 128)
        for c in range(3):
            pay_ref[c : c + 1, lanes] = off_ref[c, t : t + 1, :]
            pay_ref[3 + c : 4 + c, lanes] = force_ref[c, t : t + 1, :]
        pay_ref[6:7, lanes] = bx_ref[t : t + 1, :].astype(F32)
        pay_ref[7:8, lanes] = by_ref[t : t + 1, :].astype(F32)
        pay_ref[14:15, lanes] = bz_ref[t : t + 1, :].astype(F32)
        pay_ref[15:16, lanes] = jnp.ones((1, 128), F32)


def payload_of(pay_ref):
    first, second, third = split3(pay_ref[0:8, :])
    row8 = lax.broadcasted_iota(jnp.int32, first.shape, 0)
    second = jnp.where(row8 < 6, second.astype(F32), pay_ref[8:16, :])
    return jnp.concatenate([first.astype(F32), second, third.astype(F32)], axis=0).astype(BF16)


def columns_of(rows, col_ref):
    columns = jnp.concatenate([rows, jnp.zeros((128 - TILES, 128), F32)], axis=0).T
    for t in range(TILES):
        col_ref[128 * t : 128 * t + 128, :] = jnp.broadcast_to(columns[:, t : t + 1], (128, 128))


def gather(payload, col_ref, j, start, list_ref, base):
    lane = lax.broadcasted_iota(jnp.int32, (128 * TILES, 128), 1).astype(F32)
    here = col_ref[...] - (start + 256 * j).astype(F32)
    pick = jnp.concatenate([jnp.where(here == lane + 128.0 * h, 1.0, 0.0).astype(BF16) for h in range(2)], axis=1)
    parts = jnp.dot(payload, pick, preferred_element_type=F32)
    row = lax.broadcasted_iota(jnp.int32, (8, 256), 0)
    fields = jnp.where(row < 6, parts[0:8] + parts[8:16] + parts[16:24], parts[0:8])
    for h in range(2):
        lanes = slice(128 * h, 128 * h + 128)
        list_ref[pl.ds(pl.multiple_of(base + 16 * j, 8) + 8 * h, 8), :] = fields[:, lanes]
        list_ref[pl.ds(base + DEEP + 2 * j + h, 1), :] = parts[14:15, lanes]
    return parts


def running():
    i0 = lax.broadcasted_iota(jnp.int32, (128, 256), 0)
    i1 = lax.broadcasted_iota(jnp.int32, (128, 256), 1)
    return jnp.where(i0 <= i1, 1.0, 0.0).astype(BF16)


def scalar(row):
    return jnp.max(row).astype(jnp.int32)


def decode(block, deep):
    weights = [stencil(block[c : c + 1]) for c in range(3)]
    bases = [row.astype(jnp.int32) for row in (block[6:7], block[7:8], deep)]
    return weights, [block[3 + c : 4 + c] for c in range(3)], bases


def chunk_of(list_ref, j):
    rows = pl.multiple_of(16 * j, 8)
    block = jnp.concatenate([list_ref[pl.ds(rows, 8), :], list_ref[pl.ds(rows + 8, 8), :]], axis=1)
    deep = jnp.concatenate([list_ref[pl.ds(DEEP + 2 * j + h, 1), :] for h in range(2)], axis=1)
    return decode(block, deep)


def pack_y_kernel(
    count_ref, off_hbm, force_hbm, bx_hbm, by_hbm, bz_hbm, u_ref, rho_ref, yn_ref, yp_ref, pay_ref,
    off_ref, force_ref, bx_ref, by_ref, bz_ref, slab, col_ref, sems,
):
    loads = [
        pltpu.make_async_copy(src, dst, sems.at[2, n])
        for n, (src, dst) in enumerate(
            zip((by_hbm, bx_hbm, bz_hbm, off_hbm, force_hbm), (by_ref, bx_ref, bz_ref, off_ref, force_ref))
        )
    ]
    for load in loads:
        load.start()
    copies = []
    for c in range(4):
        for h in range(2):
            j, lanes = 2 * c + h, pl.ds(128 * h, 128)
            for n in range(2):
                ys = pl.ds((CY - 8) * n, 8)
                src = u_ref.at[c, :, ys, lanes] if c < 3 else rho_ref.at[:, ys, lanes]
                copies.append(pltpu.make_async_copy(src, slab.at[n, j], sems.at[n, j]))
    for copy in copies:
        copy.start()
    count = count_ref[0]
    for load in loads:
        load.wait()
    tile = lax.broadcasted_iota(jnp.int32, (TILES, 128), 0)
    y = jnp.where(tile < count, by_ref[...], CY // 2)
    low, high = (y < 3).astype(F32), (y > CY - 4).astype(F32)
    counts = jnp.dot(jnp.concatenate([low, high], axis=0).astype(BF16), running(), preferred_element_type=F32)
    below = lax.broadcasted_iota(jnp.int32, (2 * TILES, 2 * TILES), 0)
    left = lax.broadcasted_iota(jnp.int32, (2 * TILES, 2 * TILES), 1)
    earlier = jnp.where((left < below) & ((left < TILES) == (below < TILES)), 1.0, 0.0).astype(BF16)
    before = jnp.dot(earlier, counts[:, 128:].astype(BF16), preferred_element_type=F32)
    place = counts[:, :128] + before - 1.0
    columns_of(low * (place[:TILES] + 1.0) + high * (place[TILES:] + 4097.0) - 1.0, col_ref)
    fill_payload(pay_ref, off_ref, force_ref, bx_ref, by_ref, bz_ref)
    payload = payload_of(pay_ref)
    ends = before + counts[:, 128:]
    for n, (ref, base, start) in enumerate(((yp_ref, 16 * CX, 0), (yn_ref, 8 * CX, 4096))):
        end = ends[TILES * n + TILES - 1 : TILES * n + TILES]
        size = scalar(end)

        def chunk(j, carry, ref=ref, base=base, start=start):
            gather(payload, col_ref, j, start, ref, base)
            return carry

        lax.fori_loop(0, jnp.maximum((size + 255) // 256, 1), chunk, 0)
        ref[base + COUNTS : base + COUNTS + 1, :] = end
    for copy in copies:
        copy.wait()
    for j in range(8):
        for r in range(2):
            yp_ref[(2 * j + r) * CX : (2 * j + r + 1) * CX, :] = slab[0, j, :, r, :]
        yn_ref[j * CX : (j + 1) * CX, :] = slab[1, j, :, 7, :]


def pack_y(count, arrays, u_old, density):
    return pl.pallas_call(
        pack_y_kernel,
        out_shape=[
            jax.ShapeDtypeStruct((8 * CX + LIST, 128), F32),
            jax.ShapeDtypeStruct((16 * CX + LIST, 128), F32),
            jax.ShapeDtypeStruct((16, 128 * TILES), F32),
        ],
        in_specs=[SMEM] + [HBM] * 7,
        out_specs=[VMEM] * 3,
        scratch_shapes=[
            pltpu.VMEM((3, TILES, 128), F32),
            pltpu.VMEM((3, TILES, 128), F32),
            pltpu.VMEM((TILES, 128), jnp.int32),
            pltpu.VMEM((TILES, 128), jnp.int32),
            pltpu.VMEM((TILES, 128), jnp.int32),
            pltpu.VMEM((2, 8, CX, 8, 128), F32),
            pltpu.VMEM((128 * TILES, 128), F32),
            pltpu.SemaphoreType.DMA((3, 8)),
        ],
        name="pack_y",
    )(count, *arrays, u_old, density)


def sort_kernel(count_ref, pay_ref, list_ref, pos_ref, span_ref, col_ref):
    count = count_ref[0]
    list_ref[...] = jnp.zeros(list_ref.shape, F32)
    key_row = lax.broadcasted_iota(jnp.int32, (CX, 128), 0)
    keys = [
        jnp.where(t < count, pay_ref[6:7, 128 * t : 128 * t + 128].astype(jnp.int32), 2 * CX) for t in range(TILES)
    ]
    same = [(key_row == k).astype(F32) for k in keys]
    less = [(k < key_row).astype(F32) for k in keys]
    counts = jnp.dot(jnp.concatenate(same, axis=0).astype(BF16), running(), preferred_element_type=F32)
    smaller = jnp.dot(sum(less).astype(BF16), jnp.ones((128, 128), BF16), preferred_element_type=F32)
    before = smaller
    for t in range(TILES):
        part = counts[CX * t : CX * t + CX]
        pos_ref[t : t + 1, :] = jnp.sum(same[t] * (part[:, :128] + before), axis=0, keepdims=True) - 1.0
        before = before + part[:, 128:]
    columns_of(pos_ref[...], col_ref)
    payload = payload_of(pay_ref)

    def chunks(p, carry):
        for j in (2 * p, 2 * p + 1):
            parts = gather(payload, col_ref, j, 0, list_ref, 0)
            there = parts[15:16] > 0.5
            span_ref[2 * j] = jnp.min(jnp.where(there, parts[6:7], CX - 1.0)).astype(jnp.int32)
            span_ref[2 * j + 1] = scalar(jnp.where(there, parts[6:7], 0.0))
        return carry

    lax.fori_loop(0, (count + 3) // 4, chunks, 0)
    list_ref[COUNTS : COUNTS + 1, :] = smaller[3:4]
    list_ref[COUNTS + 1 : COUNTS + 2, :] = smaller[CX - 3 : CX - 2]
    list_ref[COUNTS + 2 : COUNTS + 3, :] = jnp.full((1, 128), (128 * count).astype(F32))


def sort(count, payload):
    return pl.pallas_call(
        sort_kernel,
        out_shape=[
            jax.ShapeDtypeStruct((LIST, 128), F32),
            jax.ShapeDtypeStruct((TILES, 128), F32),
            jax.ShapeDtypeStruct((TILES,), jnp.int32),
        ],
        in_specs=[SMEM, VMEM],
        out_specs=[VMEM, VMEM, SMEM],
        compiler_params=pltpu.CompilerParams(vmem_limit_bytes=8 * MIB),
        scratch_shapes=[pltpu.VMEM((128 * TILES, 128), F32)],
        cost_estimate=pl.CostEstimate(flops=3_000_000_000, bytes_accessed=400_000, transcendentals=0),
        name="sort",
    )(count, payload)


def spread_list(list_ref, begin, end, span_ref, grid_ref, a_ref, b_ref, wx_ref):
    def tables(j, k):
        (weight_x, weight_y, weight_z), forces, (base_x, base_y, base_z) = chunk_of(list_ref, j)
        wy, wz = y_table(base_y, weight_y), z_table(base_z, weight_z)
        for c in range(3):
            high, low = split(wz * forces[c])
            b_ref[k, 0, 256 * c : 256 * c + 256, :] = high
            b_ref[k, 1, 256 * c : 256 * c + 256, :] = low
        return weight_x, base_x, wy

    def window(first, weight_x, base_x, wy, k):
        wx_ref[k] = x_table(16, base_x, first, weight_x)
        rows = [wx_ref[k, e : e + 1, :] * wy for e in range(WINDOW)]
        high, low = split(jnp.concatenate(rows + [jnp.zeros((TALL - WINDOW * ROWS, 256), F32)], axis=0))
        a_ref[k, :TALL, :] = high
        a_ref[k, TALL:, :] = low
        across = (((1,), (1,)), ((), ()))
        both = lax.dot_general(a_ref[k], b_ref[k, 0], across, preferred_element_type=F32)
        rest = lax.dot_general(a_ref[k, :TALL, :], b_ref[k, 1], across, preferred_element_type=F32)
        sums = (both[:TALL] + rest + both[TALL:])[: WINDOW * ROWS]
        for j in range(6):
            grid_ref[j, pl.ds(first, WINDOW)] += sums[:, 128 * j : 128 * j + 128].reshape(
                WINDOW, ROWS, 128
            )

    def two(p, carry):
        both = [(tables(2 * p + k, k), k) for k in range(2)]
        for table, k in both:
            window(span_ref[2 * (2 * p + k)], *table, k)
        for table, k in both:
            low_x, high_x = span_ref[2 * (2 * p + k)], span_ref[2 * (2 * p + k) + 1]

            def more(w, carry, table=table, k=k, low_x=low_x):
                window(low_x + WINDOW * w, *table, k)
                return carry

            lax.fori_loop(1, (high_x + 4 - low_x + WINDOW - 1) // WINDOW, more, 0)
        return carry

    lax.fori_loop(begin, end, two, 0)


def spread_edges(edges, grid_ref, patches=None):
    for edge in edges:
        edge_tile(*edge[:3], *edge[4:], grid_ref, patches)
    for edge in edges:

        def more(t, carry, edge=edge):
            edge_tile(*edge[:2], t, *edge[4:], grid_ref, patches)
            return carry

        lax.fori_loop(edge[2] + 1, edge[3], more, 0)


def edge_tile(ref, base, t, dx, dy, grid_ref, patches):
    rows = pl.ds(pl.multiple_of(base + 8 * t, 8), 8)
    (weight_x, weight_y, weight_z), forces, (base_x, base_y, base_z) = decode(
        ref[rows, :], ref[pl.ds(base + DEEP + t, 1), :]
    )
    base_x, base_y = base_x + CX * dx, base_y + CY * dy
    wz = z_table(base_z, weight_z)
    if dx == 0:
        table = x_table(ROWS, base_x, 0, weight_x)
        cells = (-1, 0, 1) if dy < 0 else (CY - 1, CY, CY + 1)
        lines = [one_row(base_y, cell, weight_y) for cell in cells]
    else:
        table = y_table(base_y, weight_y)
        cells = (-1, 0, 1) if dx < 0 else (CX - 1, CX, CX + 1)
        lines = [one_row(base_x, cell, weight_x) for cell in cells]
    a_high, a_low = split(jnp.concatenate([table * line for line in lines], axis=0))
    b_high, b_low = split(jnp.concatenate([wz * force for force in forces], axis=0))
    sums = lax.dot_general(
        jnp.concatenate([a_high, a_low, a_high], axis=1),
        jnp.concatenate([b_high, b_high, b_low], axis=1),
        (((1,), (1,)), ((), ())),
        preferred_element_type=F32,
    )
    for j in range(6):
        part = sums[:, 128 * j : 128 * j + 128]
        if dx == 0:
            for i, cell in enumerate(cells):
                row = cell % ROWS
                grid_ref[j, 0:PLANES, row, :] += part[ROWS * i : ROWS * i + PLANES]
                for (patch, at), e in zip(patches, (32, 0)):
                    at = at + patch_row(j, dy, i)
                    patch[at : at + 3, :] += part[ROWS * i + e : ROWS * i + e + 3]
        else:
            grid_ref[j, cells[0] + 1 : cells[0] + 4] += part.reshape(3, ROWS, 128)


def tiles_of(ref, base):
    return (scalar(ref[base + COUNTS : base + COUNTS + 1, :]) + 127) // 128


def patch_row(j, dy, i):
    return 24 * j + (9 if dy > 0 else 0) + 3 * i


def spread_kernel(count_ref, span_ref, list_ref, grid_ref, a_ref, b_ref, wx_ref):
    for j in range(6):
        grid_ref[j] = jnp.zeros(grid_ref.shape[1:], F32)
    spread_list(list_ref, 0, (count_ref[0] + 3) // 8, span_ref, grid_ref, a_ref, b_ref, wx_ref)


def spread(count, span, markers):
    return pl.pallas_call(
        spread_kernel,
        out_shape=jax.ShapeDtypeStruct((6, PLANES + WINDOW, ROWS, 128), F32),
        in_specs=[SMEM, SMEM, VMEM],
        out_specs=VMEM,
        compiler_params=pltpu.CompilerParams(vmem_limit_bytes=16 * MIB),
        scratch_shapes=[
            pltpu.VMEM((2, 2 * TALL, 256), BF16),
            pltpu.VMEM((2, 2, 768, 256), BF16),
            pltpu.VMEM((2, 16, 256), F32),
        ],
        cost_estimate=pl.CostEstimate(flops=6_000_000_000, bytes_accessed=6_000_000, transcendentals=0),
        name="spread",
    )(count, span, markers)


def pack_x_kernel(u_ref, rho_ref, below_ref, above_ref, list_ref, grid_in, xn_ref, xp_ref, grid_ref, sems):
    copies = []
    for c in range(4):
        for h in range(2):
            j, lanes = 2 * c + h, pl.ds(128 * h, 128)
            for n, (ref, base, x) in enumerate(
                ((xn_ref, ROWS * j, CX - 1), (xp_ref, 2 * ROWS * j, 0), (xp_ref, 2 * ROWS * j + ROWS, 1))
            ):
                src = u_ref.at[c, x, :, lanes] if c < 3 else rho_ref.at[x, :, lanes]
                copies.append(pltpu.make_async_copy(src, ref.at[pl.ds(base, CY)], sems.at[n, j]))
    for copy in copies:
        copy.start()
    for j in range(8):
        fill = jnp.full((8, 128), 0.0 if j < 6 else 1.0, F32)
        for ref, base, x in (
            (xn_ref, ROWS * j, CX - 1), (xp_ref, 2 * ROWS * j, 0), (xp_ref, 2 * ROWS * j + ROWS, 1)
        ):
            ref[base + CY : base + ROWS, :] = fill
            for r in range(2):
                row = (2 * j + r) * CX + x
                ref[base + CY + r : base + CY + r + 1, :] = above_ref[row : row + 1, :]
            ref[base + ROWS - 1 : base + ROWS, :] = below_ref[j * CX + x : j * CX + x + 1, :]
    patches = []
    for ref, base in ((xn_ref, 8 * ROWS), (xp_ref, 16 * ROWS)):
        ref[base : base + LIST, :] = list_ref[:LIST, :]
        ref[base + LIST : base + LIST + PATCH, :] = jnp.zeros((PATCH, 128), F32)
        patches.append((ref, base + LIST))
    spread_edges(
        [
            (below_ref, 8 * CX, 0, tiles_of(below_ref, 8 * CX), 0, -1),
            (above_ref, 16 * CX, 0, tiles_of(above_ref, 16 * CX), 0, 1),
        ],
        grid_ref,
        patches,
    )
    for copy in copies:
        copy.wait()


def pack_x(u_old, density, below, above, markers, grid):
    return pl.pallas_call(
        pack_x_kernel,
        out_shape=[
            jax.ShapeDtypeStruct((8 * ROWS + LIST + PATCH, 128), F32),
            jax.ShapeDtypeStruct((16 * ROWS + LIST + PATCH, 128), F32),
            jax.ShapeDtypeStruct(grid.shape, F32),
        ],
        in_specs=[HBM, HBM] + [VMEM] * 4,
        out_specs=[VMEM] * 3,
        input_output_aliases={5: 2},
        compiler_params=pltpu.CompilerParams(vmem_limit_bytes=16 * MIB),
        scratch_shapes=[pltpu.SemaphoreType.DMA((3, 8))],
        name="pack_x",
    )(u_old, density, below, above, markers, grid)


def chunk_order(span_ref, chunks, early, order_ref):
    def look(j, n):
        inside = (span_ref[2 * j] >= 3) & (span_ref[2 * j + 1] <= 28)
        order_ref[n] = j
        return n + (inside == early).astype(jnp.int32)

    n = lax.fori_loop(0, chunks, look, 0)
    order_ref[n] = TILES // 2
    return n


def interpolate(list_ref, span_ref, order_ref, n, ut_ref, a_ref, wx_ref, sorted_ref):
    wide = 128 * REACH

    def tables(j):
        (weight_x, weight_y, weight_z), _, (base_x, base_y, base_z) = chunk_of(list_ref, j)
        return weight_x, base_x, y_table(base_y, weight_y), z_table(base_z, weight_z)

    def window(g, weight_x, base_x, wy, wz, k):
        wx_ref[k] = x_table(16, base_x, 3 * g, weight_x)
        for i in range(REACH):
            three = [wx_ref[k, e : e + 1, :] * wy for e in range(3 * i, 3 * i + 3)]
            high, low = split(jnp.concatenate(three + [jnp.zeros((8, 256), F32)], axis=0))
            a_ref[k, 128 * i : 128 * i + 128, :] = high
            a_ref[k, 128 * (REACH + i) : 128 * (REACH + i) + 128, :] = low
        ut_high = ut_ref[:, pl.ds(pl.multiple_of(128 * g, 128), wide)]
        ut_low = ut_ref[:, pl.ds(pl.multiple_of(DEPTH + 128 * g, 128), wide)]
        high, low = a_ref[k, :wide, :], a_ref[k, wide:, :]
        picked = (
            jnp.dot(ut_high, high, preferred_element_type=F32)
            + jnp.dot(ut_high, low, preferred_element_type=F32)
            + jnp.dot(ut_low, high, preferred_element_type=F32)
        )
        return [jnp.sum(picked[256 * c : 256 * c + 256] * wz, axis=0, keepdims=True) for c in range(3)]

    def two(p, carry):
        chunks = [order_ref[2 * p + k] for k in range(2)]
        both = [(j, tables(j), k) for k, j in enumerate(chunks)]
        for j, table, k in both:
            lanes = pl.ds(pl.multiple_of(256 * j, 256), 256)
            first = jnp.where(j < TILES // 2, span_ref[jnp.minimum(2 * j, TILES - 2)] // 3, 0)
            for c, value in enumerate(window(first, *table, k)):
                sorted_ref[c : c + 1, lanes] = value
        for j, table, k in both:
            lanes = pl.ds(pl.multiple_of(256 * j, 256), 256)
            at = jnp.minimum(2 * j, TILES - 2)
            first, high_x = span_ref[at] // 3, jnp.where(j < TILES // 2, span_ref[at + 1], 0)

            def more(w, carry, table=table, k=k, lanes=lanes, first=first):
                for c, value in enumerate(window(first + REACH * w, *table, k)):
                    sorted_ref[c : c + 1, lanes] += value
                return carry

            lax.fori_loop(1, (high_x + 4 - 3 * first + 3 * REACH - 1) // (3 * REACH), more, 0)
        return carry

    lax.fori_loop(0, (n + 1) // 2, two, 0)


DEPTH = 128 * (GROUPS + REACH)


def advance(g, old, grid_ref, fresh_ref, ut_ref, owned):
    planes = pl.ds(3 * g, 3)
    for h in range(2):
        half_over = 0.5 / old(6 + h)
        for c in range(3):
            j = 2 * c + h
            value = old(j) + grid_ref[j, planes] * half_over
            for i, x in owned:
                fresh_ref[j, x] = value[i, :CY]
            flat = jnp.concatenate([value.reshape(3 * ROWS, 128), jnp.zeros((8, 128), F32)], axis=0)
            high, low = split(flat.T)
            rows = slice(128 * j, 128 * j + 128)
            ut_ref[rows, pl.ds(pl.multiple_of(128 * g, 128), 128)] = high
            ut_ref[rows, pl.ds(pl.multiple_of(DEPTH + 128 * g, 128), 128)] = low


def own_plane(u_ref, rho_ref, rim_ref, j, e):
    lanes = slice(128 * (j % 2), 128 * (j % 2) + 128)
    inner = u_ref[j // 2, e - 1, :, lanes] if j < 6 else rho_ref[e - 1, :, lanes]
    return jnp.concatenate([inner, rim_ref[j, e]], axis=0)


def middle_kernel(
    count_ref, span_ref, list_ref, u_ref, rho_ref, below_ref, above_ref, grid_in,
    grid_ref, fresh_ref, ut_ref, rim_ref, sorted_ref,
    spread_a, spread_b, spread_wx, a_ref, wx_ref, order_ref,
):
    count = count_ref[0]
    spread_list(
        list_ref, (count + 3) // 8, (count + 3) // 4, span_ref, grid_ref, spread_a, spread_b, spread_wx
    )
    for j in range(8):
        rim_ref[j] = jnp.full((PLANES, 8, 128), 0.0 if j < 6 else 1.0, F32)
        rim_ref[j, 1:33, 7, :] = below_ref[CX * j : CX * (j + 1), :]
        rim_ref[j, 1:33, 0, :] = above_ref[2 * CX * j : 2 * CX * j + CX, :]
        rim_ref[j, 1:33, 1, :] = above_ref[2 * CX * j + CX : 2 * CX * (j + 1), :]
    for part in range(2):
        for g, groups in ((0, 1), (11, 1 + REACH)):
            start = DEPTH * part + 128 * g
            ut_ref[:, start : start + 128 * groups] = jnp.zeros((768, 128 * groups), BF16)
    sorted_ref[...] = jnp.zeros(sorted_ref.shape, F32)

    def group(g, carry):
        def old(j):
            return jnp.stack([own_plane(u_ref, rho_ref, rim_ref, j, 3 * g + i) for i in range(3)])

        advance(g, old, grid_ref, fresh_ref, ut_ref, [(i, 3 * g + i - 1) for i in range(3)])
        return carry

    lax.fori_loop(1, 11, group, 0)
    n = chunk_order(span_ref, (count + 1) // 2, True, order_ref)
    interpolate(list_ref, span_ref, order_ref, n, ut_ref, a_ref, wx_ref, sorted_ref)


def middle(count, span, markers, u_old, density, below, above, grid):
    return pl.pallas_call(
        middle_kernel,
        out_shape=[
            jax.ShapeDtypeStruct(grid.shape, F32),
            jax.ShapeDtypeStruct((6, CX, CY, 128), F32),
            jax.ShapeDtypeStruct((768, 2 * DEPTH), BF16),
            jax.ShapeDtypeStruct((8, PLANES, 8, 128), F32),
            jax.ShapeDtypeStruct((8, 128 * TILES + 256), F32),
        ],
        in_specs=[SMEM, SMEM] + [VMEM] * 6,
        out_specs=[VMEM] * 5,
        input_output_aliases={7: 0},
        compiler_params=pltpu.CompilerParams(vmem_limit_bytes=24 * MIB),
        scratch_shapes=[
            pltpu.VMEM((2, 2 * TALL, 256), BF16),
            pltpu.VMEM((2, 2, 768, 256), BF16),
            pltpu.VMEM((2, 16, 256), F32),
            pltpu.VMEM((2, 2 * 128 * REACH, 256), BF16),
            pltpu.VMEM((2, 16, 256), F32),
            pltpu.SMEM((TILES,), jnp.int32),
        ],
        cost_estimate=pl.CostEstimate(flops=6_000_000_000, bytes_accessed=6_000_000, transcendentals=0),
        name="middle",
    )(count, span, markers, u_old, density, below, above, grid)


def finish_kernel(
    count_ref, span_ref, list_ref, pos_ref, u_ref, rho_ref, rim_ref, left_ref, right_ref,
    grid_in, fresh_in, ut_in, sorted_in,
    out_ref, vel_ref, grid_ref, fresh_ref, ut_ref, sorted_ref, a_ref, wx_ref, order_ref, out_sem,
):
    count = count_ref[0]
    lo, ro = 8 * ROWS, 16 * ROWS
    high = [scalar(left_ref[lo + COUNTS + n : lo + COUNTS + n + 1, :]) for n in (1, 2)]
    spread_edges(
        [
            (left_ref, lo, jnp.minimum(high[0] // 128, TILES - 1), (high[1] + 127) // 128, -1, 0),
            (right_ref, ro, 0, tiles_of(right_ref, ro), 1, 0),
        ],
        grid_ref,
    )
    for j in range(6):
        for ref, base, e in ((left_ref, lo + LIST, 0), (right_ref, ro + LIST, 32)):
            for dy, first in ((-1, -1), (1, CY - 1)):
                for i in range(3):
                    at = base + patch_row(j, dy, i)
                    grid_ref[j, e : e + 3, (first + i) % ROWS, :] += ref[at : at + 3, :]

    def plane(j, e):
        if e == 0:
            return left_ref[ROWS * j : ROWS * (j + 1), :]
        if e in (33, 34):
            return right_ref[ROWS * (2 * j + e - 33) : ROWS * (2 * j + e - 32), :]
        if e == 35:
            return jnp.full((ROWS, 128), 0.0 if j < 6 else 1.0, F32)
        return own_plane(u_ref, rho_ref, rim_ref, j, e)

    for g in (0, 10, 11):
        advance(
            g, lambda j, g=g: jnp.stack([plane(j, 3 * g + i) for i in range(3)]), grid_ref, fresh_ref, ut_ref,
            [(i, 3 * g + i - 1) for i in range(3) if 1 <= 3 * g + i <= CX],
        )
    outs = []
    for c in range(3):
        for h in range(2):
            outs.append(
                pltpu.make_async_copy(
                    fresh_ref.at[2 * c + h], out_ref.at[c, :, :, pl.ds(128 * h, 128)], out_sem.at[2 * c + h]
                )
            )
    for copy in outs:
        copy.start()
    n = chunk_order(span_ref, (count + 1) // 2, False, order_ref)
    interpolate(list_ref, span_ref, order_ref, n, ut_ref, a_ref, wx_ref, sorted_ref)

    parts = jnp.concatenate([p.astype(F32) for p in split3(sorted_ref[:, : 128 * TILES])], axis=0).astype(BF16)
    place = lax.broadcasted_iota(jnp.int32, (2048, 128), 0).astype(F32)
    vel_ref[...] = jnp.zeros(vel_ref.shape, F32)

    def back(p, carry):
        for t in (4 * p, 4 * p + 2):
            pick = jnp.concatenate(
                [jnp.where(place == pos_ref[pl.ds(t + h, 1), :], 1.0, 0.0).astype(BF16) for h in range(2)], axis=1
            )
            sums = jnp.dot(parts, pick, preferred_element_type=F32)
            sums = sums[0:8] + sums[8:16] + sums[16:24]
            for h in range(2):
                for c in range(3):
                    vel_ref[c, pl.ds(t + h, 1), :] = sums[c : c + 1, 128 * h : 128 * h + 128]
        return carry

    lax.fori_loop(0, (count + 3) // 4, back, 0)
    for copy in outs:
        copy.wait()


def finish(count, span, markers, pos, u_old, density, rim, left, right, grid, fresh, ut, sorted_list):
    slots = pos.shape[0]
    return pl.pallas_call(
        finish_kernel,
        out_shape=[
            jax.ShapeDtypeStruct(u_old.shape, F32),
            jax.ShapeDtypeStruct((3, slots, 128), F32),
            jax.ShapeDtypeStruct(grid.shape, F32),
            jax.ShapeDtypeStruct(fresh.shape, F32),
            jax.ShapeDtypeStruct(ut.shape, BF16),
            jax.ShapeDtypeStruct(sorted_list.shape, F32),
        ],
        in_specs=[SMEM, SMEM] + [VMEM] * 11,
        out_specs=[HBM] + [VMEM] * 5,
        input_output_aliases={9: 2, 10: 3, 11: 4, 12: 5},
        compiler_params=pltpu.CompilerParams(vmem_limit_bytes=24 * MIB),
        scratch_shapes=[
            pltpu.VMEM((2, 2 * 128 * REACH, 256), BF16),
            pltpu.VMEM((2, 16, 256), F32),
            pltpu.SMEM((TILES,), jnp.int32),
            pltpu.SemaphoreType.DMA((6,)),
        ],
        cost_estimate=pl.CostEstimate(flops=6_000_000_000, bytes_accessed=12_000_000, transcendentals=0),
        name="finish",
    )(count, span, markers, pos, u_old, density, rim, left, right, grid, fresh, ut, sorted_list)[:2]


def shift(value, axis, steps):
    count = lax.axis_size(axis)
    return lax.ppermute(value, axis, [(i, (i + steps) % count) for i in range(count)])


def on_device(u_old, density, offsets, forces, base_x, base_y, base_z, tile_count):
    arrays = (offsets, forces, base_x, base_y, base_z)
    to_next, to_previous, payload = pack_y(tile_count, arrays, u_old, density)
    below = shift(to_next, "gy", 1)
    above = shift(to_previous, "gy", -1)
    markers, pos, span = sort(tile_count, payload)
    grid = spread(tile_count, span, markers)
    to_next, to_previous, grid = pack_x(u_old, density, below, above, markers, grid)
    left = shift(to_next, "gx", 1)
    right = shift(to_previous, "gx", -1)
    grid, fresh, ut, rim, sorted_list = middle(
        tile_count, span, markers, u_old, density, below, above, grid
    )
    return finish(
        tile_count, span, markers, pos, u_old, density, rim, left, right, grid, fresh, ut, sorted_list
    )


def solution(mesh):
    in_specs = (
        P(None, "gx", "gy", None),
        P("gx", "gy", None),
        P(None, ("gx", "gy"), None),
        P(None, ("gx", "gy"), None),
        P(("gx", "gy"), None),
        P(("gx", "gy"), None),
        P(("gx", "gy"), None),
        P(("gx", "gy")),
    )
    out_specs = (P(None, "gx", "gy", None), P(None, ("gx", "gy"), None))
    return jax.shard_map(
        on_device, mesh=mesh, in_specs=in_specs, out_specs=out_specs, check_vma=False
    )
```

```python
import jax
import jax.numpy as jnp
from jax import lax
from jax.experimental import pallas as pl
from jax.experimental.pallas import tpu as pltpu
from jax.sharding import PartitionSpec as P


CX, CY, ROWS, PLANES = 32, 32, 40, 36
GROUPS = 12
WINDOW = 9
TALL = 368
REACH = 4
TILES = 16
DEEP, COUNTS = 8 * TILES, 9 * TILES
LIST = 9 * TILES + 8
PATCH = 6 * 24
F32, BF16 = jnp.float32, jnp.bfloat16
VMEM = pl.BlockSpec(memory_space=pltpu.VMEM)
SMEM = pl.BlockSpec(memory_space=pltpu.SMEM)
HBM = pl.BlockSpec(memory_space=pltpu.MemorySpace.HBM)
MIB = 2**20


def stencil(frac):
    root = jnp.sqrt(1.0 + 4.0 * frac - 4.0 * frac * frac)
    return [
        (3.0 - 2.0 * frac - root) / 8.0,
        (3.0 - 2.0 * frac + root) / 8.0,
        (1.0 + 2.0 * frac + root) / 8.0,
        (1.0 + 2.0 * frac - root) / 8.0,
    ]


def spread_four(rows, targets, weights):
    row = lax.broadcasted_iota(jnp.int32, (rows, targets[0].shape[1]), 0)
    total = jnp.zeros(row.shape, F32)
    for target, weight in zip(targets, weights):
        total = jnp.where(row == target, weight, total)
    return total


def split(value):
    high = value.astype(BF16)
    return high, (value - high.astype(F32)).astype(BF16)


def split3(value):
    high, rest = value.astype(BF16), value
    parts = [high]
    for _ in range(2):
        rest = rest - parts[-1].astype(F32)
        parts.append(rest.astype(BF16))
    return parts


def x_table(rows, base_x, first, weights):
    return spread_four(rows, [base_x + (a - first) for a in range(4)], weights)


def y_table(base_y, weights):
    targets = []
    for b in range(4):
        y = base_y + (b - 1)
        targets.append(jnp.where((y < -1) | (y > CY + 1), -1, jnp.where(y < 0, ROWS - 1, y)))
    return spread_four(ROWS, targets, weights)


def one_row(base, target, weights):
    total = jnp.zeros(base.shape, F32)
    for shift, weight in enumerate(weights):
        total = jnp.where(base + (shift - 1) == target, weight, total)
    return total


def z_table(base_z, weights):
    return spread_four(256, [(base_z + c - 1) & 255 for c in range(4)], weights)


def fill_payload(pay_ref, off_ref, force_ref, bx_ref, by_ref, bz_ref):
    for t in range(TILES):
        lanes = slice(128 * t, 128 * t + 128)
        for c in range(3):
            pay_ref[c : c + 1, lanes] = off_ref[c, t : t + 1, :]
            pay_ref[3 + c : 4 + c, lanes] = force_ref[c, t : t + 1, :]
        pay_ref[6:7, lanes] = bx_ref[t : t + 1, :].astype(F32)
        pay_ref[7:8, lanes] = by_ref[t : t + 1, :].astype(F32)
        pay_ref[14:15, lanes] = bz_ref[t : t + 1, :].astype(F32)
        pay_ref[15:16, lanes] = jnp.ones((1, 128), F32)


def payload_of(pay_ref):
    first, second, third = split3(pay_ref[0:8, :])
    row8 = lax.broadcasted_iota(jnp.int32, first.shape, 0)
    second = jnp.where(row8 < 6, second.astype(F32), pay_ref[8:16, :])
    return jnp.concatenate([first.astype(F32), second, third.astype(F32)], axis=0).astype(BF16)


def columns_of(rows, col_ref):
    columns = jnp.concatenate([rows, jnp.zeros((128 - TILES, 128), F32)], axis=0).T
    for t in range(TILES):
        col_ref[128 * t : 128 * t + 128, :] = jnp.broadcast_to(columns[:, t : t + 1], (128, 128))


def gather(payload, col_ref, j, start, list_ref, base):
    lane = lax.broadcasted_iota(jnp.int32, (128 * TILES, 128), 1).astype(F32)
    here = col_ref[...] - (start + 256 * j).astype(F32)
    pick = jnp.concatenate([jnp.where(here == lane + 128.0 * h, 1.0, 0.0).astype(BF16) for h in range(2)], axis=1)
    parts = jnp.dot(payload, pick, preferred_element_type=F32)
    row = lax.broadcasted_iota(jnp.int32, (8, 256), 0)
    fields = jnp.where(row < 6, parts[0:8] + parts[8:16] + parts[16:24], parts[0:8])
    for h in range(2):
        lanes = slice(128 * h, 128 * h + 128)
        list_ref[pl.ds(pl.multiple_of(base + 16 * j, 8) + 8 * h, 8), :] = fields[:, lanes]
        list_ref[pl.ds(base + DEEP + 2 * j + h, 1), :] = parts[14:15, lanes]
    return parts


def running():
    i0 = lax.broadcasted_iota(jnp.int32, (128, 256), 0)
    i1 = lax.broadcasted_iota(jnp.int32, (128, 256), 1)
    return jnp.where(i0 <= i1, 1.0, 0.0).astype(BF16)


def scalar(row):
    return jnp.max(row).astype(jnp.int32)


def decode(block, deep):
    weights = [stencil(block[c : c + 1]) for c in range(3)]
    bases = [row.astype(jnp.int32) for row in (block[6:7], block[7:8], deep)]
    return weights, [block[3 + c : 4 + c] for c in range(3)], bases


def chunk_of(list_ref, j):
    rows = pl.multiple_of(16 * j, 8)
    block = jnp.concatenate([list_ref[pl.ds(rows, 8), :], list_ref[pl.ds(rows + 8, 8), :]], axis=1)
    deep = jnp.concatenate([list_ref[pl.ds(DEEP + 2 * j + h, 1), :] for h in range(2)], axis=1)
    return decode(block, deep)


def pack_y_kernel(
    count_ref, off_hbm, force_hbm, bx_hbm, by_hbm, bz_hbm, u_ref, rho_ref, yn_ref, yp_ref, pay_ref,
    off_ref, force_ref, bx_ref, by_ref, bz_ref, slab, col_ref, sems,
):
    loads = [
        pltpu.make_async_copy(src, dst, sems.at[2, n])
        for n, (src, dst) in enumerate(
            zip((by_hbm, bx_hbm, bz_hbm, off_hbm, force_hbm), (by_ref, bx_ref, bz_ref, off_ref, force_ref))
        )
    ]
    for load in loads:
        load.start()
    copies = []
    for c in range(4):
        for h in range(2):
            j, lanes = 2 * c + h, pl.ds(128 * h, 128)
            for n in range(2):
                ys = pl.ds((CY - 8) * n, 8)
                src = u_ref.at[c, :, ys, lanes] if c < 3 else rho_ref.at[:, ys, lanes]
                copies.append(pltpu.make_async_copy(src, slab.at[n, j], sems.at[n, j]))
    for copy in copies:
        copy.start()
    count = count_ref[0]
    for load in loads:
        load.wait()
    tile = lax.broadcasted_iota(jnp.int32, (TILES, 128), 0)
    y = jnp.where(tile < count, by_ref[...], CY // 2)
    low, high = (y < 3).astype(F32), (y > CY - 4).astype(F32)
    counts = jnp.dot(jnp.concatenate([low, high], axis=0).astype(BF16), running(), preferred_element_type=F32)
    below = lax.broadcasted_iota(jnp.int32, (2 * TILES, 2 * TILES), 0)
    left = lax.broadcasted_iota(jnp.int32, (2 * TILES, 2 * TILES), 1)
    earlier = jnp.where((left < below) & ((left < TILES) == (below < TILES)), 1.0, 0.0).astype(BF16)
    before = jnp.dot(earlier, counts[:, 128:].astype(BF16), preferred_element_type=F32)
    place = counts[:, :128] + before - 1.0
    columns_of(low * (place[:TILES] + 1.0) + high * (place[TILES:] + 4097.0) - 1.0, col_ref)
    fill_payload(pay_ref, off_ref, force_ref, bx_ref, by_ref, bz_ref)
    payload = payload_of(pay_ref)
    ends = before + counts[:, 128:]
    for n, (ref, base, start) in enumerate(((yp_ref, 16 * CX, 0), (yn_ref, 8 * CX, 4096))):
        end = ends[TILES * n + TILES - 1 : TILES * n + TILES]
        size = scalar(end)

        def chunk(j, carry, ref=ref, base=base, start=start):
            gather(payload, col_ref, j, start, ref, base)
            return carry

        lax.fori_loop(0, jnp.maximum((size + 255) // 256, 1), chunk, 0)
        ref[base + COUNTS : base + COUNTS + 1, :] = end
    for copy in copies:
        copy.wait()
    for j in range(8):
        for r in range(2):
            yp_ref[(2 * j + r) * CX : (2 * j + r + 1) * CX, :] = slab[0, j, :, r, :]
        yn_ref[j * CX : (j + 1) * CX, :] = slab[1, j, :, 7, :]


def pack_y(count, arrays, u_old, density):
    return pl.pallas_call(
        pack_y_kernel,
        out_shape=[
            jax.ShapeDtypeStruct((8 * CX + LIST, 128), F32),
            jax.ShapeDtypeStruct((16 * CX + LIST, 128), F32),
            jax.ShapeDtypeStruct((16, 128 * TILES), F32),
        ],
        in_specs=[SMEM] + [HBM] * 7,
        out_specs=[VMEM] * 3,
        scratch_shapes=[
            pltpu.VMEM((3, TILES, 128), F32),
            pltpu.VMEM((3, TILES, 128), F32),
            pltpu.VMEM((TILES, 128), jnp.int32),
            pltpu.VMEM((TILES, 128), jnp.int32),
            pltpu.VMEM((TILES, 128), jnp.int32),
            pltpu.VMEM((2, 8, CX, 8, 128), F32),
            pltpu.VMEM((128 * TILES, 128), F32),
            pltpu.SemaphoreType.DMA((3, 8)),
        ],
        name="pack_y",
    )(count, *arrays, u_old, density)


def sort_kernel(count_ref, pay_ref, list_ref, pos_ref, span_ref, col_ref):
    count = count_ref[0]
    list_ref[...] = jnp.zeros(list_ref.shape, F32)
    key_row = lax.broadcasted_iota(jnp.int32, (CX, 128), 0)
    keys = [
        jnp.where(t < count, pay_ref[6:7, 128 * t : 128 * t + 128].astype(jnp.int32), 2 * CX) for t in range(TILES)
    ]
    same = [(key_row == k).astype(F32) for k in keys]
    less = [(k < key_row).astype(F32) for k in keys]
    counts = jnp.dot(jnp.concatenate(same, axis=0).astype(BF16), running(), preferred_element_type=F32)
    smaller = jnp.dot(sum(less).astype(BF16), jnp.ones((128, 128), BF16), preferred_element_type=F32)
    before = smaller
    for t in range(TILES):
        part = counts[CX * t : CX * t + CX]
        pos_ref[t : t + 1, :] = jnp.sum(same[t] * (part[:, :128] + before), axis=0, keepdims=True) - 1.0
        before = before + part[:, 128:]
    columns_of(pos_ref[...], col_ref)
    payload = payload_of(pay_ref)

    def chunks(p, carry):
        for j in (2 * p, 2 * p + 1):
            parts = gather(payload, col_ref, j, 0, list_ref, 0)
            there = parts[15:16] > 0.5
            span_ref[2 * j] = jnp.min(jnp.where(there, parts[6:7], CX - 1.0)).astype(jnp.int32)
            span_ref[2 * j + 1] = scalar(jnp.where(there, parts[6:7], 0.0))
        return carry

    lax.fori_loop(0, (count + 3) // 4, chunks, 0)
    list_ref[COUNTS : COUNTS + 1, :] = smaller[3:4]
    list_ref[COUNTS + 1 : COUNTS + 2, :] = smaller[CX - 3 : CX - 2]
    list_ref[COUNTS + 2 : COUNTS + 3, :] = jnp.full((1, 128), (128 * count).astype(F32))


def sort(count, payload):
    return pl.pallas_call(
        sort_kernel,
        out_shape=[
            jax.ShapeDtypeStruct((LIST, 128), F32),
            jax.ShapeDtypeStruct((TILES, 128), F32),
            jax.ShapeDtypeStruct((TILES,), jnp.int32),
        ],
        in_specs=[SMEM, VMEM],
        out_specs=[VMEM, VMEM, SMEM],
        compiler_params=pltpu.CompilerParams(vmem_limit_bytes=8 * MIB),
        scratch_shapes=[pltpu.VMEM((128 * TILES, 128), F32)],
        cost_estimate=pl.CostEstimate(flops=3_000_000_000, bytes_accessed=400_000, transcendentals=0),
        name="sort",
    )(count, payload)


def spread_list(list_ref, pairs, span_ref, grid_ref, a_ref, b_ref, wx_ref):
    def tables(j, k):
        (weight_x, weight_y, weight_z), forces, (base_x, base_y, base_z) = chunk_of(list_ref, j)
        wy, wz = y_table(base_y, weight_y), z_table(base_z, weight_z)
        for c in range(3):
            high, low = split(wz * forces[c])
            b_ref[k, 0, 256 * c : 256 * c + 256, :] = high
            b_ref[k, 1, 256 * c : 256 * c + 256, :] = low
        return weight_x, base_x, wy

    def window(first, weight_x, base_x, wy, k):
        wx_ref[k] = x_table(16, base_x, first, weight_x)
        rows = [wx_ref[k, e : e + 1, :] * wy for e in range(WINDOW)]
        high, low = split(jnp.concatenate(rows + [jnp.zeros((TALL - WINDOW * ROWS, 256), F32)], axis=0))
        a_ref[k, :TALL, :] = high
        a_ref[k, TALL:, :] = low
        across = (((1,), (1,)), ((), ()))
        both = lax.dot_general(a_ref[k], b_ref[k, 0], across, preferred_element_type=F32)
        rest = lax.dot_general(a_ref[k, :TALL, :], b_ref[k, 1], across, preferred_element_type=F32)
        sums = (both[:TALL] + rest + both[TALL:])[: WINDOW * ROWS]
        for j in range(6):
            grid_ref[j, pl.ds(first, WINDOW)] += sums[:, 128 * j : 128 * j + 128].reshape(
                WINDOW, ROWS, 128
            )

    def two(p, carry):
        both = [(tables(2 * p + k, k), k) for k in range(2)]
        for table, k in both:
            window(span_ref[2 * (2 * p + k)], *table, k)
        for table, k in both:
            low_x, high_x = span_ref[2 * (2 * p + k)], span_ref[2 * (2 * p + k) + 1]

            def more(w, carry, table=table, k=k, low_x=low_x):
                window(low_x + WINDOW * w, *table, k)
                return carry

            lax.fori_loop(1, (high_x + 4 - low_x + WINDOW - 1) // WINDOW, more, 0)
        return carry

    lax.fori_loop(0, pairs, two, 0)


def spread_edges(edges, grid_ref, patches=None):
    for edge in edges:
        edge_tile(*edge[:3], *edge[4:], grid_ref, patches)
    for edge in edges:

        def more(t, carry, edge=edge):
            edge_tile(*edge[:2], t, *edge[4:], grid_ref, patches)
            return carry

        lax.fori_loop(edge[2] + 1, edge[3], more, 0)


def edge_tile(ref, base, t, dx, dy, grid_ref, patches):
    rows = pl.ds(pl.multiple_of(base + 8 * t, 8), 8)
    (weight_x, weight_y, weight_z), forces, (base_x, base_y, base_z) = decode(
        ref[rows, :], ref[pl.ds(base + DEEP + t, 1), :]
    )
    base_x, base_y = base_x + CX * dx, base_y + CY * dy
    wz = z_table(base_z, weight_z)
    if dx == 0:
        table = x_table(ROWS, base_x, 0, weight_x)
        cells = (-1, 0, 1) if dy < 0 else (CY - 1, CY, CY + 1)
        lines = [one_row(base_y, cell, weight_y) for cell in cells]
    else:
        table = y_table(base_y, weight_y)
        cells = (-1, 0, 1) if dx < 0 else (CX - 1, CX, CX + 1)
        lines = [one_row(base_x, cell, weight_x) for cell in cells]
    a_high, a_low = split(jnp.concatenate([table * line for line in lines], axis=0))
    b_high, b_low = split(jnp.concatenate([wz * force for force in forces], axis=0))
    sums = lax.dot_general(
        jnp.concatenate([a_high, a_low, a_high], axis=1),
        jnp.concatenate([b_high, b_high, b_low], axis=1),
        (((1,), (1,)), ((), ())),
        preferred_element_type=F32,
    )
    for j in range(6):
        part = sums[:, 128 * j : 128 * j + 128]
        if dx == 0:
            for i, cell in enumerate(cells):
                row = cell % ROWS
                grid_ref[j, 0:PLANES, row, :] += part[ROWS * i : ROWS * i + PLANES]
                for (patch, at), e in zip(patches, (32, 0)):
                    at = at + patch_row(j, dy, i)
                    patch[at : at + 3, :] += part[ROWS * i + e : ROWS * i + e + 3]
        else:
            grid_ref[j, cells[0] + 1 : cells[0] + 4] += part.reshape(3, ROWS, 128)


def tiles_of(ref, base):
    return (scalar(ref[base + COUNTS : base + COUNTS + 1, :]) + 127) // 128


def patch_row(j, dy, i):
    return 24 * j + (9 if dy > 0 else 0) + 3 * i


def spread_kernel(count_ref, span_ref, list_ref, grid_ref, a_ref, b_ref, wx_ref):
    for j in range(6):
        grid_ref[j] = jnp.zeros(grid_ref.shape[1:], F32)
    spread_list(list_ref, (count_ref[0] + 3) // 4, span_ref, grid_ref, a_ref, b_ref, wx_ref)


def spread(count, span, markers):
    return pl.pallas_call(
        spread_kernel,
        out_shape=jax.ShapeDtypeStruct((6, PLANES + WINDOW, ROWS, 128), F32),
        in_specs=[SMEM, SMEM, VMEM],
        out_specs=VMEM,
        compiler_params=pltpu.CompilerParams(vmem_limit_bytes=16 * MIB),
        scratch_shapes=[
            pltpu.VMEM((2, 2 * TALL, 256), BF16),
            pltpu.VMEM((2, 2, 768, 256), BF16),
            pltpu.VMEM((2, 16, 256), F32),
        ],
        cost_estimate=pl.CostEstimate(flops=6_000_000_000, bytes_accessed=6_000_000, transcendentals=0),
        name="spread",
    )(count, span, markers)


def pack_x_kernel(u_ref, rho_ref, below_ref, above_ref, list_ref, grid_in, xn_ref, xp_ref, grid_ref, sems):
    copies = []
    for c in range(4):
        for h in range(2):
            j, lanes = 2 * c + h, pl.ds(128 * h, 128)
            for n, (ref, base, x) in enumerate(
                ((xn_ref, ROWS * j, CX - 1), (xp_ref, 2 * ROWS * j, 0), (xp_ref, 2 * ROWS * j + ROWS, 1))
            ):
                src = u_ref.at[c, x, :, lanes] if c < 3 else rho_ref.at[x, :, lanes]
                copies.append(pltpu.make_async_copy(src, ref.at[pl.ds(base, CY)], sems.at[n, j]))
    for copy in copies:
        copy.start()
    for j in range(8):
        fill = jnp.full((8, 128), 0.0 if j < 6 else 1.0, F32)
        for ref, base, x in (
            (xn_ref, ROWS * j, CX - 1), (xp_ref, 2 * ROWS * j, 0), (xp_ref, 2 * ROWS * j + ROWS, 1)
        ):
            ref[base + CY : base + ROWS, :] = fill
            for r in range(2):
                row = (2 * j + r) * CX + x
                ref[base + CY + r : base + CY + r + 1, :] = above_ref[row : row + 1, :]
            ref[base + ROWS - 1 : base + ROWS, :] = below_ref[j * CX + x : j * CX + x + 1, :]
    patches = []
    for ref, base in ((xn_ref, 8 * ROWS), (xp_ref, 16 * ROWS)):
        ref[base : base + LIST, :] = list_ref[:LIST, :]
        ref[base + LIST : base + LIST + PATCH, :] = jnp.zeros((PATCH, 128), F32)
        patches.append((ref, base + LIST))
    spread_edges(
        [
            (below_ref, 8 * CX, 0, tiles_of(below_ref, 8 * CX), 0, -1),
            (above_ref, 16 * CX, 0, tiles_of(above_ref, 16 * CX), 0, 1),
        ],
        grid_ref,
        patches,
    )
    for copy in copies:
        copy.wait()


def pack_x(u_old, density, below, above, markers, grid):
    return pl.pallas_call(
        pack_x_kernel,
        out_shape=[
            jax.ShapeDtypeStruct((8 * ROWS + LIST + PATCH, 128), F32),
            jax.ShapeDtypeStruct((16 * ROWS + LIST + PATCH, 128), F32),
            jax.ShapeDtypeStruct(grid.shape, F32),
        ],
        in_specs=[HBM, HBM] + [VMEM] * 4,
        out_specs=[VMEM] * 3,
        input_output_aliases={5: 2},
        compiler_params=pltpu.CompilerParams(vmem_limit_bytes=16 * MIB),
        scratch_shapes=[pltpu.SemaphoreType.DMA((3, 8))],
        name="pack_x",
    )(u_old, density, below, above, markers, grid)


OUTER = (0, 10, 11)


def outer_chunks(span_ref, chunks, order_ref):
    def look(j, n):
        order_ref[n] = j
        return n + ((span_ref[2 * j] < 3) | (span_ref[2 * j + 1] > 28)).astype(jnp.int32)

    n = lax.fori_loop(0, chunks, look, 0)
    order_ref[n] = TILES // 2
    return n


def interpolate(list_ref, span_ref, order_ref, n, ut_ref, a_ref, wx_ref, sorted_ref):
    outer = order_ref is not None
    reach = len(OUTER) if outer else REACH
    wide = 128 * reach

    def tables(j):
        (weight_x, weight_y, weight_z), _, (base_x, base_y, base_z) = chunk_of(list_ref, j)
        return weight_x, base_x, y_table(base_y, weight_y), z_table(base_z, weight_z)

    def window(g, weight_x, base_x, wy, wz, k):
        wx_ref[k] = x_table(wx_ref.shape[1], base_x, 3 * g, weight_x)
        for i in range(reach):
            at = 3 * (OUTER[i] if outer else i)
            three = [wx_ref[k, e : e + 1, :] * wy for e in range(at, at + 3)]
            high, low = split(jnp.concatenate(three + [jnp.zeros((8, 256), F32)], axis=0))
            a_ref[k, 128 * i : 128 * i + 128, :] = high
            a_ref[k, wide + 128 * i : wide + 128 * i + 128, :] = low
        if outer:
            ut_high, ut_low = ut_ref[:, :wide], ut_ref[:, wide:]
        else:
            ut_high = ut_ref[:, pl.ds(pl.multiple_of(128 * g, 128), wide)]
            ut_low = ut_ref[:, pl.ds(pl.multiple_of(DEPTH + 128 * g, 128), wide)]
        high, low = a_ref[k, :wide, :], a_ref[k, wide:, :]
        picked = (
            jnp.dot(ut_high, high, preferred_element_type=F32)
            + jnp.dot(ut_high, low, preferred_element_type=F32)
            + jnp.dot(ut_low, high, preferred_element_type=F32)
        )
        return [jnp.sum(picked[256 * c : 256 * c + 256] * wz, axis=0, keepdims=True) for c in range(3)]

    def two(p, carry):
        chunks = [order_ref[2 * p + k] if outer else 2 * p + k for k in range(2)]
        both = [(j, tables(j), k) for k, j in enumerate(chunks)]
        for j, table, k in both:
            lanes = pl.ds(pl.multiple_of(256 * j, 256), 256)
            first = 0 if outer else span_ref[2 * j] // 3
            for c, value in enumerate(window(first, *table, k)):
                sorted_ref[c : c + 1, lanes] += value
        if outer:
            return carry
        for j, table, k in both:
            lanes = pl.ds(pl.multiple_of(256 * j, 256), 256)
            first, high_x = span_ref[2 * j] // 3, span_ref[2 * j + 1]

            def more(w, carry, table=table, k=k, lanes=lanes, first=first):
                for c, value in enumerate(window(first + REACH * w, *table, k)):
                    sorted_ref[c : c + 1, lanes] += value
                return carry

            lax.fori_loop(1, (high_x + 4 - 3 * first + 3 * REACH - 1) // (3 * REACH), more, 0)
        return carry

    lax.fori_loop(0, (n + 1) // 2, two, 0)


DEPTH = 128 * (GROUPS + REACH)


def advance(planes, old, grid_ref, fresh_ref, owned, ut_ref, at, depth, known=(True, True, True)):
    for h in range(2):
        half_over = 0.5 / old(6 + h)
        for c in range(3):
            j = 2 * c + h
            value = old(j) + grid_ref[j, planes] * half_over
            for i, x in owned:
                fresh_ref[j, x] = value[i, :CY]
            kept = [value[i] if known[i] else jnp.zeros((ROWS, 128), F32) for i in range(3)]
            high, low = split(jnp.concatenate(kept + [jnp.zeros((8, 128), F32)], axis=0).T)
            rows = slice(128 * j, 128 * j + 128)
            ut_ref[rows, pl.ds(at, 128)] = high
            ut_ref[rows, pl.ds(depth + at, 128)] = low


def own_plane(u_ref, rho_ref, rim_ref, j, e):
    lanes = slice(128 * (j % 2), 128 * (j % 2) + 128)
    inner = u_ref[j // 2, e - 1, :, lanes] if j < 6 else rho_ref[e - 1, :, lanes]
    return jnp.concatenate([inner, rim_ref[j, e]], axis=0)


def middle_kernel(
    count_ref, span_ref, list_ref, u_ref, rho_ref, below_ref, above_ref, grid_ref,
    fresh_ref, rim_ref, sorted_ref, ut_ref, a_ref, wx_ref,
):
    count = count_ref[0]
    for j in range(8):
        rim_ref[j] = jnp.full((PLANES, 8, 128), 0.0 if j < 6 else 1.0, F32)
        rim_ref[j, 1:33, 7, :] = below_ref[CX * j : CX * (j + 1), :]
        rim_ref[j, 1:33, 0, :] = above_ref[2 * CX * j : 2 * CX * j + CX, :]
        rim_ref[j, 1:33, 1, :] = above_ref[2 * CX * j + CX : 2 * CX * (j + 1), :]
    for part in range(2):
        for g, groups in ((0, 1), (11, 1 + REACH)):
            start = DEPTH * part + 128 * g
            ut_ref[:, start : start + 128 * groups] = jnp.zeros((768, 128 * groups), BF16)
    sorted_ref[...] = jnp.zeros(sorted_ref.shape, F32)

    def old(g):
        return lambda j: jnp.stack([own_plane(u_ref, rho_ref, rim_ref, j, 3 * g + i) for i in range(3)])

    def group(g, carry):
        advance(
            pl.ds(3 * g, 3), old(g), grid_ref, fresh_ref, [(i, 3 * g + i - 1) for i in range(3)],
            ut_ref, pl.multiple_of(128 * g, 128), DEPTH,
        )
        return carry

    lax.fori_loop(1, 10, group, 0)
    advance(
        pl.ds(30, 3), old(10), grid_ref, fresh_ref, [(0, 29), (1, 30)], ut_ref, 1280, DEPTH, (True, True, False)
    )
    interpolate(list_ref, span_ref, None, 2 * ((count + 3) // 4), ut_ref, a_ref, wx_ref, sorted_ref)


def middle(count, span, markers, u_old, density, below, above, grid):
    return pl.pallas_call(
        middle_kernel,
        out_shape=[
            jax.ShapeDtypeStruct((6, CX, CY, 128), F32),
            jax.ShapeDtypeStruct((8, PLANES, 8, 128), F32),
            jax.ShapeDtypeStruct((8, 128 * TILES + 256), F32),
        ],
        in_specs=[SMEM, SMEM] + [VMEM] * 6,
        out_specs=[VMEM] * 3,
        compiler_params=pltpu.CompilerParams(vmem_limit_bytes=24 * MIB),
        scratch_shapes=[
            pltpu.VMEM((768, 2 * DEPTH), BF16),
            pltpu.VMEM((2, 2 * 128 * REACH, 256), BF16),
            pltpu.VMEM((2, 16, 256), F32),
        ],
        cost_estimate=pl.CostEstimate(flops=6_000_000_000, bytes_accessed=6_000_000, transcendentals=0),
        name="middle",
    )(count, span, markers, u_old, density, below, above, grid)


def finish_kernel(
    count_ref, span_ref, list_ref, pos_ref, u_ref, rho_ref, rim_ref, left_ref, right_ref,
    grid_in, fresh_in, sorted_in,
    out_ref, vel_ref, grid_ref, fresh_ref, sorted_ref, ut_ref, a_ref, wx_ref, order_ref, out_sem,
):
    count = count_ref[0]
    lo, ro = 8 * ROWS, 16 * ROWS
    high = [scalar(left_ref[lo + COUNTS + n : lo + COUNTS + n + 1, :]) for n in (1, 2)]
    spread_edges(
        [
            (left_ref, lo, jnp.minimum(high[0] // 128, TILES - 1), (high[1] + 127) // 128, -1, 0),
            (right_ref, ro, 0, tiles_of(right_ref, ro), 1, 0),
        ],
        grid_ref,
    )
    for j in range(6):
        for ref, base, e in ((left_ref, lo + LIST, 0), (right_ref, ro + LIST, 32)):
            for dy, first in ((-1, -1), (1, CY - 1)):
                for i in range(3):
                    at = base + patch_row(j, dy, i)
                    grid_ref[j, e : e + 3, (first + i) % ROWS, :] += ref[at : at + 3, :]

    def plane(j, e):
        if e == 0:
            return left_ref[ROWS * j : ROWS * (j + 1), :]
        if e in (33, 34):
            return right_ref[ROWS * (2 * j + e - 33) : ROWS * (2 * j + e - 32), :]
        if e == 35:
            return jnp.full((ROWS, 128), 0.0 if j < 6 else 1.0, F32)
        return own_plane(u_ref, rho_ref, rim_ref, j, e)

    for n, g in enumerate(OUTER):
        known = [e < 3 or e > CX - 1 for e in range(3 * g, 3 * g + 3)]
        advance(
            pl.ds(3 * g, 3), lambda j, g=g: jnp.stack([plane(j, 3 * g + i) for i in range(3)]), grid_ref, fresh_ref,
            [(i, 3 * g + i - 1) for i in range(3) if known[i] and 1 <= 3 * g + i <= CX],
            ut_ref, 128 * n, 128 * len(OUTER), known,
        )
    outs = []
    for c in range(3):
        for h in range(2):
            outs.append(
                pltpu.make_async_copy(
                    fresh_ref.at[2 * c + h], out_ref.at[c, :, :, pl.ds(128 * h, 128)], out_sem.at[2 * c + h]
                )
            )
    for copy in outs:
        copy.start()
    n = outer_chunks(span_ref, (count + 1) // 2, order_ref)
    interpolate(list_ref, span_ref, order_ref, n, ut_ref, a_ref, wx_ref, sorted_ref)

    parts = jnp.concatenate([p.astype(F32) for p in split3(sorted_ref[:, : 128 * TILES])], axis=0).astype(BF16)
    place = lax.broadcasted_iota(jnp.int32, (2048, 128), 0).astype(F32)
    vel_ref[...] = jnp.zeros(vel_ref.shape, F32)

    def back(p, carry):
        for t in (4 * p, 4 * p + 2):
            pick = jnp.concatenate(
                [jnp.where(place == pos_ref[pl.ds(t + h, 1), :], 1.0, 0.0).astype(BF16) for h in range(2)], axis=1
            )
            sums = jnp.dot(parts, pick, preferred_element_type=F32)
            sums = sums[0:8] + sums[8:16] + sums[16:24]
            for h in range(2):
                for c in range(3):
                    vel_ref[c, pl.ds(t + h, 1), :] = sums[c : c + 1, 128 * h : 128 * h + 128]
        return carry

    lax.fori_loop(0, (count + 3) // 4, back, 0)
    for copy in outs:
        copy.wait()


def finish(count, span, markers, pos, u_old, density, rim, left, right, grid, fresh, sorted_list):
    slots = pos.shape[0]
    return pl.pallas_call(
        finish_kernel,
        out_shape=[
            jax.ShapeDtypeStruct(u_old.shape, F32),
            jax.ShapeDtypeStruct((3, slots, 128), F32),
            jax.ShapeDtypeStruct(grid.shape, F32),
            jax.ShapeDtypeStruct(fresh.shape, F32),
            jax.ShapeDtypeStruct(sorted_list.shape, F32),
        ],
        in_specs=[SMEM, SMEM] + [VMEM] * 10,
        out_specs=[HBM] + [VMEM] * 4,
        input_output_aliases={9: 2, 10: 3, 11: 4},
        compiler_params=pltpu.CompilerParams(vmem_limit_bytes=24 * MIB),
        scratch_shapes=[
            pltpu.VMEM((768, 2 * 128 * len(OUTER)), BF16),
            pltpu.VMEM((2, 2 * 128 * len(OUTER), 256), BF16),
            pltpu.VMEM((2, ROWS, 256), F32),
            pltpu.SMEM((TILES,), jnp.int32),
            pltpu.SemaphoreType.DMA((6,)),
        ],
        cost_estimate=pl.CostEstimate(flops=6_000_000_000, bytes_accessed=12_000_000, transcendentals=0),
        name="finish",
    )(count, span, markers, pos, u_old, density, rim, left, right, grid, fresh, sorted_list)[:2]


def shift(value, axis, steps):
    count = lax.axis_size(axis)
    return lax.ppermute(value, axis, [(i, (i + steps) % count) for i in range(count)])


def on_device(u_old, density, offsets, forces, base_x, base_y, base_z, tile_count):
    arrays = (offsets, forces, base_x, base_y, base_z)
    to_next, to_previous, payload = pack_y(tile_count, arrays, u_old, density)
    below = shift(to_next, "gy", 1)
    above = shift(to_previous, "gy", -1)
    markers, pos, span = sort(tile_count, payload)
    grid = spread(tile_count, span, markers)
    to_next, to_previous, grid = pack_x(u_old, density, below, above, markers, grid)
    left = shift(to_next, "gx", 1)
    right = shift(to_previous, "gx", -1)
    fresh, rim, sorted_list = middle(
        tile_count, span, markers, u_old, density, below, above, grid
    )
    return finish(
        tile_count, span, markers, pos, u_old, density, rim, left, right, grid, fresh, sorted_list
    )


def solution(mesh):
    in_specs = (
        P(None, "gx", "gy", None),
        P("gx", "gy", None),
        P(None, ("gx", "gy"), None),
        P(None, ("gx", "gy"), None),
        P(("gx", "gy"), None),
        P(("gx", "gy"), None),
        P(("gx", "gy"), None),
        P(("gx", "gy")),
    )
    out_specs = (P(None, "gx", "gy", None), P(None, ("gx", "gy"), None))
    return jax.shard_map(
        on_device, mesh=mesh, in_specs=in_specs, out_specs=out_specs, check_vma=False
    )
```

```python
import jax
import jax.numpy as jnp
from jax import lax
from jax.experimental import pallas as pl
from jax.experimental.pallas import tpu as pltpu
from jax.sharding import PartitionSpec as P


CX, CY, ROWS, PLANES = 32, 32, 40, 36
GROUPS = 12
WINDOW = 9
TALL = 368
REACH = 4
TILES = 16
DEEP, COUNTS = 8 * TILES, 9 * TILES
LIST = 9 * TILES + 8
PATCH = 6 * 24
F32, BF16 = jnp.float32, jnp.bfloat16
VMEM = pl.BlockSpec(memory_space=pltpu.VMEM)
SMEM = pl.BlockSpec(memory_space=pltpu.SMEM)
HBM = pl.BlockSpec(memory_space=pltpu.MemorySpace.HBM)
MIB = 2**20


def stencil(frac):
    root = jnp.sqrt(1.0 + 4.0 * frac - 4.0 * frac * frac)
    return [
        (3.0 - 2.0 * frac - root) / 8.0,
        (3.0 - 2.0 * frac + root) / 8.0,
        (1.0 + 2.0 * frac + root) / 8.0,
        (1.0 + 2.0 * frac - root) / 8.0,
    ]


def spread_four(rows, targets, weights):
    row = lax.broadcasted_iota(jnp.int32, (rows, targets[0].shape[1]), 0)
    total = jnp.zeros(row.shape, F32)
    for target, weight in zip(targets, weights):
        total = jnp.where(row == target, weight, total)
    return total


def split(value):
    high = value.astype(BF16)
    return high, (value - high.astype(F32)).astype(BF16)


def split3(value):
    high, rest = value.astype(BF16), value
    parts = [high]
    for _ in range(2):
        rest = rest - parts[-1].astype(F32)
        parts.append(rest.astype(BF16))
    return parts


def x_table(rows, base_x, first, weights):
    return spread_four(rows, [base_x + (a - first) for a in range(4)], weights)


def y_table(base_y, weights):
    targets = []
    for b in range(4):
        y = base_y + (b - 1)
        targets.append(jnp.where((y < -1) | (y > CY + 1), -1, jnp.where(y < 0, ROWS - 1, y)))
    return spread_four(ROWS, targets, weights)


def one_row(base, target, weights):
    total = jnp.zeros(base.shape, F32)
    for shift, weight in enumerate(weights):
        total = jnp.where(base + (shift - 1) == target, weight, total)
    return total


def z_table(base_z, weights):
    return spread_four(256, [(base_z + c - 1) & 255 for c in range(4)], weights)


def fill_payload(pay_ref, off_ref, force_ref, bx_ref, by_ref, bz_ref):
    for t in range(TILES):
        lanes = slice(128 * t, 128 * t + 128)
        for c in range(3):
            pay_ref[c : c + 1, lanes] = off_ref[c, t : t + 1, :]
            pay_ref[3 + c : 4 + c, lanes] = force_ref[c, t : t + 1, :]
        pay_ref[6:7, lanes] = bx_ref[t : t + 1, :].astype(F32)
        pay_ref[7:8, lanes] = by_ref[t : t + 1, :].astype(F32)
        pay_ref[14:15, lanes] = bz_ref[t : t + 1, :].astype(F32)
        pay_ref[15:16, lanes] = jnp.ones((1, 128), F32)


def payload_of(pay_ref):
    first, second, third = split3(pay_ref[0:8, :])
    row8 = lax.broadcasted_iota(jnp.int32, first.shape, 0)
    second = jnp.where(row8 < 6, second.astype(F32), pay_ref[8:16, :])
    return jnp.concatenate([first.astype(F32), second, third.astype(F32)], axis=0).astype(BF16)


def columns_of(rows, col_ref):
    columns = jnp.concatenate([rows, jnp.zeros((128 - TILES, 128), F32)], axis=0).T
    for t in range(TILES):
        col_ref[128 * t : 128 * t + 128, :] = jnp.broadcast_to(columns[:, t : t + 1], (128, 128))


def gather(payload, col_ref, j, start, list_ref, base):
    lane = lax.broadcasted_iota(jnp.int32, (128 * TILES, 128), 1).astype(F32)
    here = col_ref[...] - (start + 256 * j).astype(F32)
    pick = jnp.concatenate([jnp.where(here == lane + 128.0 * h, 1.0, 0.0).astype(BF16) for h in range(2)], axis=1)
    parts = jnp.dot(payload, pick, preferred_element_type=F32)
    row = lax.broadcasted_iota(jnp.int32, (8, 256), 0)
    fields = jnp.where(row < 6, parts[0:8] + parts[8:16] + parts[16:24], parts[0:8])
    for h in range(2):
        lanes = slice(128 * h, 128 * h + 128)
        list_ref[pl.ds(pl.multiple_of(base + 16 * j, 8) + 8 * h, 8), :] = fields[:, lanes]
        list_ref[pl.ds(base + DEEP + 2 * j + h, 1), :] = parts[14:15, lanes]
    return parts


def running():
    i0 = lax.broadcasted_iota(jnp.int32, (128, 256), 0)
    i1 = lax.broadcasted_iota(jnp.int32, (128, 256), 1)
    return jnp.where(i0 <= i1, 1.0, 0.0).astype(BF16)


def scalar(row):
    return jnp.max(row).astype(jnp.int32)


def decode(block, deep):
    weights = [stencil(block[c : c + 1]) for c in range(3)]
    bases = [row.astype(jnp.int32) for row in (block[6:7], block[7:8], deep)]
    return weights, [block[3 + c : 4 + c] for c in range(3)], bases


def chunk_of(list_ref, j):
    rows = pl.multiple_of(16 * j, 8)
    block = jnp.concatenate([list_ref[pl.ds(rows, 8), :], list_ref[pl.ds(rows + 8, 8), :]], axis=1)
    deep = jnp.concatenate([list_ref[pl.ds(DEEP + 2 * j + h, 1), :] for h in range(2)], axis=1)
    return decode(block, deep)


def pack_y_kernel(
    count_ref, off_hbm, force_hbm, bx_hbm, by_hbm, bz_hbm, u_ref, rho_ref, yn_ref, yp_ref, pay_ref,
    off_ref, force_ref, bx_ref, by_ref, bz_ref, slab, col_ref, sems,
):
    loads = [
        pltpu.make_async_copy(src, dst, sems.at[2, n])
        for n, (src, dst) in enumerate(
            zip((by_hbm, bx_hbm, bz_hbm, off_hbm, force_hbm), (by_ref, bx_ref, bz_ref, off_ref, force_ref))
        )
    ]
    for load in loads:
        load.start()
    copies = []
    for c in range(4):
        for h in range(2):
            j, lanes = 2 * c + h, pl.ds(128 * h, 128)
            for n in range(2):
                ys = pl.ds((CY - 8) * n, 8)
                src = u_ref.at[c, :, ys, lanes] if c < 3 else rho_ref.at[:, ys, lanes]
                copies.append(pltpu.make_async_copy(src, slab.at[n, j], sems.at[n, j]))
    for copy in copies:
        copy.start()
    count = count_ref[0]
    for load in loads:
        load.wait()
    tile = lax.broadcasted_iota(jnp.int32, (TILES, 128), 0)
    y = jnp.where(tile < count, by_ref[...], CY // 2)
    low, high = (y < 3).astype(F32), (y > CY - 4).astype(F32)
    counts = jnp.dot(jnp.concatenate([low, high], axis=0).astype(BF16), running(), preferred_element_type=F32)
    below = lax.broadcasted_iota(jnp.int32, (2 * TILES, 2 * TILES), 0)
    left = lax.broadcasted_iota(jnp.int32, (2 * TILES, 2 * TILES), 1)
    earlier = jnp.where((left < below) & ((left < TILES) == (below < TILES)), 1.0, 0.0).astype(BF16)
    before = jnp.dot(earlier, counts[:, 128:].astype(BF16), preferred_element_type=F32)
    place = counts[:, :128] + before - 1.0
    columns_of(low * (place[:TILES] + 1.0) + high * (place[TILES:] + 4097.0) - 1.0, col_ref)
    fill_payload(pay_ref, off_ref, force_ref, bx_ref, by_ref, bz_ref)
    payload = payload_of(pay_ref)
    ends = before + counts[:, 128:]
    for n, (ref, base, start) in enumerate(((yp_ref, 16 * CX, 0), (yn_ref, 8 * CX, 4096))):
        end = ends[TILES * n + TILES - 1 : TILES * n + TILES]
        size = scalar(end)

        def chunk(j, carry, ref=ref, base=base, start=start):
            gather(payload, col_ref, j, start, ref, base)
            return carry

        lax.fori_loop(0, jnp.maximum((size + 255) // 256, 1), chunk, 0)
        ref[base + COUNTS : base + COUNTS + 1, :] = end
    for copy in copies:
        copy.wait()
    for j in range(8):
        for r in range(2):
            yp_ref[(2 * j + r) * CX : (2 * j + r + 1) * CX, :] = slab[0, j, :, r, :]
        yn_ref[j * CX : (j + 1) * CX, :] = slab[1, j, :, 7, :]


def pack_y(count, arrays, u_old, density):
    return pl.pallas_call(
        pack_y_kernel,
        out_shape=[
            jax.ShapeDtypeStruct((8 * CX + LIST, 128), F32),
            jax.ShapeDtypeStruct((16 * CX + LIST, 128), F32),
            jax.ShapeDtypeStruct((16, 128 * TILES), F32),
        ],
        in_specs=[SMEM] + [HBM] * 7,
        out_specs=[VMEM] * 3,
        scratch_shapes=[
            pltpu.VMEM((3, TILES, 128), F32),
            pltpu.VMEM((3, TILES, 128), F32),
            pltpu.VMEM((TILES, 128), jnp.int32),
            pltpu.VMEM((TILES, 128), jnp.int32),
            pltpu.VMEM((TILES, 128), jnp.int32),
            pltpu.VMEM((2, 8, CX, 8, 128), F32),
            pltpu.VMEM((128 * TILES, 128), F32),
            pltpu.SemaphoreType.DMA((3, 8)),
        ],
        name="pack_y",
    )(count, *arrays, u_old, density)


def sort_kernel(count_ref, pay_ref, list_ref, pos_ref, span_ref, col_ref):
    count = count_ref[0]
    list_ref[...] = jnp.zeros(list_ref.shape, F32)
    key_row = lax.broadcasted_iota(jnp.int32, (CX, 128), 0)
    keys = [
        jnp.where(t < count, pay_ref[6:7, 128 * t : 128 * t + 128].astype(jnp.int32), 2 * CX) for t in range(TILES)
    ]
    same = [(key_row == k).astype(F32) for k in keys]
    less = [(k < key_row).astype(F32) for k in keys]
    counts = jnp.dot(jnp.concatenate(same, axis=0).astype(BF16), running(), preferred_element_type=F32)
    smaller = jnp.dot(sum(less).astype(BF16), jnp.ones((128, 128), BF16), preferred_element_type=F32)
    before = smaller
    for t in range(TILES):
        part = counts[CX * t : CX * t + CX]
        pos_ref[t : t + 1, :] = jnp.sum(same[t] * (part[:, :128] + before), axis=0, keepdims=True) - 1.0
        before = before + part[:, 128:]
    columns_of(pos_ref[...], col_ref)
    payload = payload_of(pay_ref)

    def chunks(p, carry):
        for j in (2 * p, 2 * p + 1):
            parts = gather(payload, col_ref, j, 0, list_ref, 0)
            there = parts[15:16] > 0.5
            span_ref[2 * j] = jnp.min(jnp.where(there, parts[6:7], CX - 1.0)).astype(jnp.int32)
            span_ref[2 * j + 1] = scalar(jnp.where(there, parts[6:7], 0.0))
        return carry

    lax.fori_loop(0, (count + 3) // 4, chunks, 0)
    list_ref[COUNTS : COUNTS + 1, :] = smaller[3:4]
    list_ref[COUNTS + 1 : COUNTS + 2, :] = smaller[CX - 3 : CX - 2]
    list_ref[COUNTS + 2 : COUNTS + 3, :] = jnp.full((1, 128), (128 * count).astype(F32))


def sort(count, payload):
    return pl.pallas_call(
        sort_kernel,
        out_shape=[
            jax.ShapeDtypeStruct((LIST, 128), F32),
            jax.ShapeDtypeStruct((TILES, 128), F32),
            jax.ShapeDtypeStruct((TILES,), jnp.int32),
        ],
        in_specs=[SMEM, VMEM],
        out_specs=[VMEM, VMEM, SMEM],
        compiler_params=pltpu.CompilerParams(vmem_limit_bytes=8 * MIB),
        scratch_shapes=[pltpu.VMEM((128 * TILES, 128), F32)],
        cost_estimate=pl.CostEstimate(flops=3_000_000_000, bytes_accessed=400_000, transcendentals=0),
        name="sort",
    )(count, payload)


def spread_list(list_ref, pairs, span_ref, grid_ref, a_ref, b_ref, wx_ref):
    def tables(j, k):
        (weight_x, weight_y, weight_z), forces, (base_x, base_y, base_z) = chunk_of(list_ref, j)
        wy, wz = y_table(base_y, weight_y), z_table(base_z, weight_z)
        for c in range(3):
            high, low = split(wz * forces[c])
            b_ref[k, 0, 256 * c : 256 * c + 256, :] = high
            b_ref[k, 1, 256 * c : 256 * c + 256, :] = low
        return weight_x, base_x, wy

    def window(first, weight_x, base_x, wy, k):
        wx_ref[k] = x_table(16, base_x, first, weight_x)
        rows = [wx_ref[k, e : e + 1, :] * wy for e in range(WINDOW)]
        high, low = split(jnp.concatenate(rows + [jnp.zeros((TALL - WINDOW * ROWS, 256), F32)], axis=0))
        a_ref[k, :TALL, :] = high
        a_ref[k, TALL:, :] = low
        across = (((1,), (1,)), ((), ()))
        both = lax.dot_general(a_ref[k], b_ref[k, 0], across, preferred_element_type=F32)
        rest = lax.dot_general(a_ref[k, :TALL, :], b_ref[k, 1], across, preferred_element_type=F32)
        sums = (both[:TALL] + rest + both[TALL:])[: WINDOW * ROWS]
        for j in range(6):
            grid_ref[j, pl.ds(first, WINDOW)] += sums[:, 128 * j : 128 * j + 128].reshape(
                WINDOW, ROWS, 128
            )

    def two(p, carry):
        both = [(tables(2 * p + k, k), k) for k in range(2)]
        for table, k in both:
            window(span_ref[2 * (2 * p + k)], *table, k)
        for table, k in both:
            low_x, high_x = span_ref[2 * (2 * p + k)], span_ref[2 * (2 * p + k) + 1]

            def more(w, carry, table=table, k=k, low_x=low_x):
                window(low_x + WINDOW * w, *table, k)
                return carry

            lax.fori_loop(1, (high_x + 4 - low_x + WINDOW - 1) // WINDOW, more, 0)
        return carry

    lax.fori_loop(0, pairs, two, 0)


def spread_edges(edges, grid_ref, patches=None):
    for edge in edges:
        edge_tile(*edge[:3], *edge[4:], grid_ref, patches)
    for edge in edges:

        def more(t, carry, edge=edge):
            edge_tile(*edge[:2], t, *edge[4:], grid_ref, patches)
            return carry

        lax.fori_loop(edge[2] + 1, edge[3], more, 0)


def edge_tile(ref, base, t, dx, dy, grid_ref, patches):
    rows = pl.ds(pl.multiple_of(base + 8 * t, 8), 8)
    (weight_x, weight_y, weight_z), forces, (base_x, base_y, base_z) = decode(
        ref[rows, :], ref[pl.ds(base + DEEP + t, 1), :]
    )
    base_x, base_y = base_x + CX * dx, base_y + CY * dy
    wz = z_table(base_z, weight_z)
    if dx == 0:
        table = x_table(ROWS, base_x, 0, weight_x)
        cells = (-1, 0, 1) if dy < 0 else (CY - 1, CY, CY + 1)
        lines = [one_row(base_y, cell, weight_y) for cell in cells]
    else:
        table = y_table(base_y, weight_y)
        cells = (-1, 0, 1) if dx < 0 else (CX - 1, CX, CX + 1)
        lines = [one_row(base_x, cell, weight_x) for cell in cells]
    a_high, a_low = split(jnp.concatenate([table * line for line in lines], axis=0))
    b_high, b_low = split(jnp.concatenate([wz * force for force in forces], axis=0))
    sums = lax.dot_general(
        jnp.concatenate([a_high, a_low, a_high], axis=1),
        jnp.concatenate([b_high, b_high, b_low], axis=1),
        (((1,), (1,)), ((), ())),
        preferred_element_type=F32,
    )
    for j in range(6):
        part = sums[:, 128 * j : 128 * j + 128]
        if dx == 0:
            for i, cell in enumerate(cells):
                row = cell % ROWS
                grid_ref[j, 0:PLANES, row, :] += part[ROWS * i : ROWS * i + PLANES]
                for (patch, at), e in zip(patches, (32, 0)):
                    at = at + patch_row(j, dy, i)
                    patch[at : at + 3, :] += part[ROWS * i + e : ROWS * i + e + 3]
        else:
            grid_ref[j, cells[0] + 1 : cells[0] + 4] += part.reshape(3, ROWS, 128)


def tiles_of(ref, base):
    return (scalar(ref[base + COUNTS : base + COUNTS + 1, :]) + 127) // 128


def patch_row(j, dy, i):
    return 24 * j + (9 if dy > 0 else 0) + 3 * i


def spread_kernel(count_ref, span_ref, list_ref, grid_ref, a_ref, b_ref, wx_ref):
    for j in range(6):
        grid_ref[j] = jnp.zeros(grid_ref.shape[1:], F32)
    spread_list(list_ref, (count_ref[0] + 3) // 4, span_ref, grid_ref, a_ref, b_ref, wx_ref)


def spread(count, span, markers):
    return pl.pallas_call(
        spread_kernel,
        out_shape=jax.ShapeDtypeStruct((6, PLANES + WINDOW, ROWS, 128), F32),
        in_specs=[SMEM, SMEM, VMEM],
        out_specs=VMEM,
        compiler_params=pltpu.CompilerParams(vmem_limit_bytes=16 * MIB),
        scratch_shapes=[
            pltpu.VMEM((2, 2 * TALL, 256), BF16),
            pltpu.VMEM((2, 2, 768, 256), BF16),
            pltpu.VMEM((2, 16, 256), F32),
        ],
        cost_estimate=pl.CostEstimate(flops=6_000_000_000, bytes_accessed=6_000_000, transcendentals=0),
        name="spread",
    )(count, span, markers)


def pack_x_kernel(u_ref, rho_ref, below_ref, above_ref, list_ref, grid_in, xn_ref, xp_ref, grid_ref, sems):
    copies = []
    for c in range(4):
        for h in range(2):
            j, lanes = 2 * c + h, pl.ds(128 * h, 128)
            for n, (ref, base, x) in enumerate(
                ((xn_ref, ROWS * j, CX - 1), (xp_ref, 2 * ROWS * j, 0), (xp_ref, 2 * ROWS * j + ROWS, 1))
            ):
                src = u_ref.at[c, x, :, lanes] if c < 3 else rho_ref.at[x, :, lanes]
                copies.append(pltpu.make_async_copy(src, ref.at[pl.ds(base, CY)], sems.at[n, j]))
    for copy in copies:
        copy.start()
    for j in range(8):
        fill = jnp.full((8, 128), 0.0 if j < 6 else 1.0, F32)
        for ref, base, x in (
            (xn_ref, ROWS * j, CX - 1), (xp_ref, 2 * ROWS * j, 0), (xp_ref, 2 * ROWS * j + ROWS, 1)
        ):
            ref[base + CY : base + ROWS, :] = fill
            for r in range(2):
                row = (2 * j + r) * CX + x
                ref[base + CY + r : base + CY + r + 1, :] = above_ref[row : row + 1, :]
            ref[base + ROWS - 1 : base + ROWS, :] = below_ref[j * CX + x : j * CX + x + 1, :]
    patches = []
    for ref, base in ((xn_ref, 8 * ROWS), (xp_ref, 16 * ROWS)):
        ref[base : base + LIST, :] = list_ref[:LIST, :]
        ref[base + LIST : base + LIST + PATCH, :] = jnp.zeros((PATCH, 128), F32)
        patches.append((ref, base + LIST))
    spread_edges(
        [
            (below_ref, 8 * CX, 0, tiles_of(below_ref, 8 * CX), 0, -1),
            (above_ref, 16 * CX, 0, tiles_of(above_ref, 16 * CX), 0, 1),
        ],
        grid_ref,
        patches,
    )
    for copy in copies:
        copy.wait()


def pack_x(u_old, density, below, above, markers, grid):
    return pl.pallas_call(
        pack_x_kernel,
        out_shape=[
            jax.ShapeDtypeStruct((8 * ROWS + LIST + PATCH, 128), F32),
            jax.ShapeDtypeStruct((16 * ROWS + LIST + PATCH, 128), F32),
            jax.ShapeDtypeStruct(grid.shape, F32),
        ],
        in_specs=[HBM, HBM] + [VMEM] * 4,
        out_specs=[VMEM] * 3,
        input_output_aliases={5: 2},
        compiler_params=pltpu.CompilerParams(vmem_limit_bytes=16 * MIB),
        scratch_shapes=[pltpu.SemaphoreType.DMA((3, 8))],
        name="pack_x",
    )(u_old, density, below, above, markers, grid)


OUTER = (0, 10, 11)


def outer_chunks(span_ref, chunks, order_ref):
    def look(j, n):
        order_ref[n] = j
        return n + ((span_ref[2 * j] < 3) | (span_ref[2 * j + 1] > 28)).astype(jnp.int32)

    n = lax.fori_loop(0, chunks, look, 0)
    order_ref[n] = TILES // 2
    return n


def interpolate(list_ref, span_ref, order_ref, n, ut_ref, a_ref, wx_ref, sorted_ref):
    outer = order_ref is not None
    reach = len(OUTER) if outer else REACH
    wide = 128 * reach

    def tables(j):
        (weight_x, weight_y, weight_z), _, (base_x, base_y, base_z) = chunk_of(list_ref, j)
        return weight_x, base_x, y_table(base_y, weight_y), z_table(base_z, weight_z)

    def window(g, weight_x, base_x, wy, wz, k):
        wx_ref[k] = x_table(wx_ref.shape[1], base_x, 3 * g, weight_x)
        for i in range(reach):
            at = 3 * (OUTER[i] if outer else i)
            three = [wx_ref[k, e : e + 1, :] * wy for e in range(at, at + 3)]
            high, low = split(jnp.concatenate(three + [jnp.zeros((8, 256), F32)], axis=0))
            a_ref[k, 128 * i : 128 * i + 128, :] = high
            a_ref[k, wide + 128 * i : wide + 128 * i + 128, :] = low
        if outer:
            ut_high, ut_low = ut_ref[:, :wide], ut_ref[:, wide:]
        else:
            ut_high = ut_ref[:, pl.ds(pl.multiple_of(128 * g, 128), wide)]
            ut_low = ut_ref[:, pl.ds(pl.multiple_of(DEPTH + 128 * g, 128), wide)]
        high, low = a_ref[k, :wide, :], a_ref[k, wide:, :]
        picked = (
            jnp.dot(ut_high, high, preferred_element_type=F32)
            + jnp.dot(ut_high, low, preferred_element_type=F32)
            + jnp.dot(ut_low, high, preferred_element_type=F32)
        )
        return [jnp.sum(picked[256 * c : 256 * c + 256] * wz, axis=0, keepdims=True) for c in range(3)]

    def two(p, carry):
        chunks = [order_ref[2 * p + k] if outer else 2 * p + k for k in range(2)]
        both = [(j, tables(j), k) for k, j in enumerate(chunks)]
        for j, table, k in both:
            lanes = pl.ds(pl.multiple_of(256 * j, 256), 256)
            first = 0 if outer else span_ref[2 * j] // 3
            for c, value in enumerate(window(first, *table, k)):
                sorted_ref[c : c + 1, lanes] += value
        if outer:
            return carry
        for j, table, k in both:
            lanes = pl.ds(pl.multiple_of(256 * j, 256), 256)
            first, high_x = span_ref[2 * j] // 3, span_ref[2 * j + 1]

            def more(w, carry, table=table, k=k, lanes=lanes, first=first):
                for c, value in enumerate(window(first + REACH * w, *table, k)):
                    sorted_ref[c : c + 1, lanes] += value
                return carry

            lax.fori_loop(1, (high_x + 4 - 3 * first + 3 * REACH - 1) // (3 * REACH), more, 0)
        return carry

    lax.fori_loop(0, (n + 1) // 2, two, 0)


DEPTH = 128 * (GROUPS + REACH)


def advance(planes, old, grid_ref, fresh_ref, owned, ut_ref, at, depth, known=(True, True, True)):
    for h in range(2):
        half_over = 0.5 / old(6 + h)
        for c in range(3):
            j = 2 * c + h
            value = old(j) + grid_ref[j, planes] * half_over
            for i, x in owned:
                fresh_ref[j, x] = value[i, :CY]
            kept = [value[i] if known[i] else jnp.zeros((ROWS, 128), F32) for i in range(3)]
            high, low = split(jnp.concatenate(kept + [jnp.zeros((8, 128), F32)], axis=0).T)
            rows = slice(128 * j, 128 * j + 128)
            ut_ref[rows, pl.ds(at, 128)] = high
            ut_ref[rows, pl.ds(depth + at, 128)] = low


def own_plane(u_ref, rho_ref, rim_ref, j, e):
    lanes = slice(128 * (j % 2), 128 * (j % 2) + 128)
    inner = u_ref[j // 2, e - 1, :, lanes] if j < 6 else rho_ref[e - 1, :, lanes]
    return jnp.concatenate([inner, rim_ref[j, e]], axis=0)


def middle_kernel(
    u_ref, rho_ref, below_ref, above_ref, grid_ref, fresh_ref, rim_ref, ut_ref,
):
    for j in range(8):
        rim_ref[j] = jnp.full((PLANES, 8, 128), 0.0 if j < 6 else 1.0, F32)
        rim_ref[j, 1:33, 7, :] = below_ref[CX * j : CX * (j + 1), :]
        rim_ref[j, 1:33, 0, :] = above_ref[2 * CX * j : 2 * CX * j + CX, :]
        rim_ref[j, 1:33, 1, :] = above_ref[2 * CX * j + CX : 2 * CX * (j + 1), :]
    for part in range(2):
        for g, groups in ((0, 1), (11, 1 + REACH)):
            start = DEPTH * part + 128 * g
            ut_ref[:, start : start + 128 * groups] = jnp.zeros((768, 128 * groups), BF16)

    def old(g):
        return lambda j: jnp.stack([own_plane(u_ref, rho_ref, rim_ref, j, 3 * g + i) for i in range(3)])

    def group(g, carry):
        advance(
            pl.ds(3 * g, 3), old(g), grid_ref, fresh_ref, [(i, 3 * g + i - 1) for i in range(3)],
            ut_ref, pl.multiple_of(128 * g, 128), DEPTH,
        )
        return carry

    lax.fori_loop(1, 10, group, 0)
    advance(
        pl.ds(30, 3), old(10), grid_ref, fresh_ref, [(0, 29), (1, 30)], ut_ref, 1280, DEPTH, (True, True, False)
    )


def middle(u_old, density, below, above, grid):
    return pl.pallas_call(
        middle_kernel,
        out_shape=[
            jax.ShapeDtypeStruct((6, CX, CY, 128), F32),
            jax.ShapeDtypeStruct((8, PLANES, 8, 128), F32),
            jax.ShapeDtypeStruct((768, 2 * DEPTH), BF16),
        ],
        in_specs=[VMEM] * 5,
        out_specs=[VMEM] * 3,
        compiler_params=pltpu.CompilerParams(vmem_limit_bytes=24 * MIB),
        cost_estimate=pl.CostEstimate(flops=3_000_000_000, bytes_accessed=6_000_000, transcendentals=0),
        name="middle",
    )(u_old, density, below, above, grid)


def inner_kernel(count_ref, span_ref, list_ref, ut_ref, sorted_ref, a_ref, wx_ref):
    sorted_ref[...] = jnp.zeros(sorted_ref.shape, F32)
    interpolate(list_ref, span_ref, None, 2 * ((count_ref[0] + 3) // 4), ut_ref, a_ref, wx_ref, sorted_ref)


def inner(count, span, markers, ut):
    return pl.pallas_call(
        inner_kernel,
        out_shape=jax.ShapeDtypeStruct((8, 128 * TILES + 256), F32),
        in_specs=[SMEM, SMEM, VMEM, VMEM],
        out_specs=VMEM,
        compiler_params=pltpu.CompilerParams(vmem_limit_bytes=24 * MIB),
        scratch_shapes=[pltpu.VMEM((2, 2 * 128 * REACH, 256), BF16), pltpu.VMEM((2, 16, 256), F32)],
        cost_estimate=pl.CostEstimate(flops=6_000_000_000, bytes_accessed=6_000_000, transcendentals=0),
        name="inner",
    )(count, span, markers, ut)


def finish_kernel(
    count_ref, span_ref, list_ref, pos_ref, u_ref, rho_ref, rim_ref, left_ref, right_ref,
    grid_in, fresh_in, sorted_in,
    out_ref, vel_ref, grid_ref, fresh_ref, sorted_ref, ut_ref, a_ref, wx_ref, order_ref, out_sem,
):
    count = count_ref[0]
    lo, ro = 8 * ROWS, 16 * ROWS
    high = [scalar(left_ref[lo + COUNTS + n : lo + COUNTS + n + 1, :]) for n in (1, 2)]
    spread_edges(
        [
            (left_ref, lo, jnp.minimum(high[0] // 128, TILES - 1), (high[1] + 127) // 128, -1, 0),
            (right_ref, ro, 0, tiles_of(right_ref, ro), 1, 0),
        ],
        grid_ref,
    )
    for j in range(6):
        for ref, base, e in ((left_ref, lo + LIST, 0), (right_ref, ro + LIST, 32)):
            for dy, first in ((-1, -1), (1, CY - 1)):
                for i in range(3):
                    at = base + patch_row(j, dy, i)
                    grid_ref[j, e : e + 3, (first + i) % ROWS, :] += ref[at : at + 3, :]

    def plane(j, e):
        if e == 0:
            return left_ref[ROWS * j : ROWS * (j + 1), :]
        if e in (33, 34):
            return right_ref[ROWS * (2 * j + e - 33) : ROWS * (2 * j + e - 32), :]
        if e == 35:
            return jnp.full((ROWS, 128), 0.0 if j < 6 else 1.0, F32)
        return own_plane(u_ref, rho_ref, rim_ref, j, e)

    for n, g in enumerate(OUTER):
        known = [e < 3 or e > CX - 1 for e in range(3 * g, 3 * g + 3)]
        advance(
            pl.ds(3 * g, 3), lambda j, g=g: jnp.stack([plane(j, 3 * g + i) for i in range(3)]), grid_ref, fresh_ref,
            [(i, 3 * g + i - 1) for i in range(3) if known[i] and 1 <= 3 * g + i <= CX],
            ut_ref, 128 * n, 128 * len(OUTER), known,
        )
    outs = []
    for c in range(3):
        for h in range(2):
            outs.append(
                pltpu.make_async_copy(
                    fresh_ref.at[2 * c + h], out_ref.at[c, :, :, pl.ds(128 * h, 128)], out_sem.at[2 * c + h]
                )
            )
    for copy in outs:
        copy.start()
    n = outer_chunks(span_ref, (count + 1) // 2, order_ref)
    interpolate(list_ref, span_ref, order_ref, n, ut_ref, a_ref, wx_ref, sorted_ref)

    parts = jnp.concatenate([p.astype(F32) for p in split3(sorted_ref[:, : 128 * TILES])], axis=0).astype(BF16)
    place = lax.broadcasted_iota(jnp.int32, (2048, 128), 0).astype(F32)
    vel_ref[...] = jnp.zeros(vel_ref.shape, F32)

    def back(p, carry):
        for t in (4 * p, 4 * p + 2):
            pick = jnp.concatenate(
                [jnp.where(place == pos_ref[pl.ds(t + h, 1), :], 1.0, 0.0).astype(BF16) for h in range(2)], axis=1
            )
            sums = jnp.dot(parts, pick, preferred_element_type=F32)
            sums = sums[0:8] + sums[8:16] + sums[16:24]
            for h in range(2):
                for c in range(3):
                    vel_ref[c, pl.ds(t + h, 1), :] = sums[c : c + 1, 128 * h : 128 * h + 128]
        return carry

    lax.fori_loop(0, (count + 3) // 4, back, 0)
    for copy in outs:
        copy.wait()


def finish(count, span, markers, pos, u_old, density, rim, left, right, grid, fresh, sorted_list):
    slots = pos.shape[0]
    return pl.pallas_call(
        finish_kernel,
        out_shape=[
            jax.ShapeDtypeStruct(u_old.shape, F32),
            jax.ShapeDtypeStruct((3, slots, 128), F32),
            jax.ShapeDtypeStruct(grid.shape, F32),
            jax.ShapeDtypeStruct(fresh.shape, F32),
            jax.ShapeDtypeStruct(sorted_list.shape, F32),
        ],
        in_specs=[SMEM, SMEM] + [VMEM] * 10,
        out_specs=[HBM] + [VMEM] * 4,
        input_output_aliases={9: 2, 10: 3, 11: 4},
        compiler_params=pltpu.CompilerParams(vmem_limit_bytes=24 * MIB),
        scratch_shapes=[
            pltpu.VMEM((768, 2 * 128 * len(OUTER)), BF16),
            pltpu.VMEM((2, 2 * 128 * len(OUTER), 256), BF16),
            pltpu.VMEM((2, ROWS, 256), F32),
            pltpu.SMEM((TILES,), jnp.int32),
            pltpu.SemaphoreType.DMA((6,)),
        ],
        cost_estimate=pl.CostEstimate(flops=6_000_000_000, bytes_accessed=12_000_000, transcendentals=0),
        name="finish",
    )(count, span, markers, pos, u_old, density, rim, left, right, grid, fresh, sorted_list)[:2]


def shift(value, axis, steps):
    count = lax.axis_size(axis)
    return lax.ppermute(value, axis, [(i, (i + steps) % count) for i in range(count)])


def on_device(u_old, density, offsets, forces, base_x, base_y, base_z, tile_count):
    arrays = (offsets, forces, base_x, base_y, base_z)
    to_next, to_previous, payload = pack_y(tile_count, arrays, u_old, density)
    below = shift(to_next, "gy", 1)
    above = shift(to_previous, "gy", -1)
    markers, pos, span = sort(tile_count, payload)
    grid = spread(tile_count, span, markers)
    to_next, to_previous, grid = pack_x(u_old, density, below, above, markers, grid)
    left = shift(to_next, "gx", 1)
    fresh, rim, ut = middle(u_old, density, below, above, grid)
    right = shift(to_previous, "gx", -1)
    sorted_list = inner(tile_count, span, markers, ut)
    return finish(
        tile_count, span, markers, pos, u_old, density, rim, left, right, grid, fresh, sorted_list
    )


def solution(mesh):
    in_specs = (
        P(None, "gx", "gy", None),
        P("gx", "gy", None),
        P(None, ("gx", "gy"), None),
        P(None, ("gx", "gy"), None),
        P(("gx", "gy"), None),
        P(("gx", "gy"), None),
        P(("gx", "gy"), None),
        P(("gx", "gy")),
    )
    out_specs = (P(None, "gx", "gy", None), P(None, ("gx", "gy"), None))
    return jax.shard_map(
        on_device, mesh=mesh, in_specs=in_specs, out_specs=out_specs, check_vma=False
    )
```
